64 devices in a mesh: dp: 4 (over x, y), tp: 16 (over z, core).
Axes of the slice: x: 2, y: 2, z: 8, core: 2. Of those that a mesh axis runs over, the one named last changes fastest.
The devices are a block of a 4x4x8 slice.
Arguments:
- hidden: bfloat16 [2048, 4096], P('dp'), parts along dimension 0
- w_q: bfloat16 [4096, 4096], P(None, 'tp')
- w_k: bfloat16 [4096, 4096], P(None, 'tp')
- w_v: bfloat16 [4096, 4096], P(None, 'tp')
- w_o: bfloat16 [4096, 4096], P('tp')
- q_norm_w: float32 [4096], P('tp')
- k_norm_w: float32 [4096], P('tp')
- post_norm_w: float32 [4096], replicated
- k_cache: bfloat16 [2048, 16, 32, 128], P('dp', None, 'tp'), parts along dimension 0
- v_cache: bfloat16 [2048, 16, 32, 128], P('dp', None, 'tp'), parts along dimension 0
- positions: int32 [2048], P('dp'), parts along dimension 0
Outputs:
- output 1: bfloat16 [2048, 4096], P('dp'), parts along dimension 0
- output 2: bfloat16 [2048, 16, 32, 128], P('dp', None, 'tp'), parts along dimension 0
- output 3: bfloat16 [2048, 16, 32, 128], P('dp', None, 'tp'), parts along dimension 0
There are 4 independent parts. The reference program is written for one: setup_inputs(seed, part) draws one part's arguments, and reference() takes and returns one part's arrays. A program takes and returns all parts, laid end to end along the dimension named above; an argument that names none is the same for every part.
All inputs are finite; a program needn't handle non-finite values.
Results may differ from the reference program's by a relative error of at most 0.0138914.
Values are sent between devices in bfloat16 or wider.
A program may use at most 768 MiB of HBM per device.

```python
import jax
import jax.numpy as jnp
from jax import lax

BATCH = 512
CACHE_LEN = 16
HEADS = 32
HEAD_DIM = 128
WIDTH = HEADS * HEAD_DIM
NORM_EPS = 1e-6
ROPE_BASE = 500000.0


def setup_inputs(seed: int = 0, part: int = 0) -> dict:
    base_key = jax.random.key(seed)
    shared_keys = jax.random.split(base_key, 9)
    part_keys = jax.random.split(jax.random.fold_in(base_key, part), 6)
    fan_scale = WIDTH ** -0.5
    head_frac = jnp.arange(HEADS, dtype=jnp.float32) / max(HEADS - 1, 1)
    q_heads = jnp.exp(1.2 * (2.0 * head_frac - 1.0) + 0.2 * jax.random.normal(shared_keys[0], (HEADS,)))
    k_heads = jnp.exp(1.2 * (1.0 - 2.0 * head_frac) + 0.2 * jax.random.normal(shared_keys[1], (HEADS,)))
    q_cols = jnp.repeat(q_heads, HEAD_DIM)
    k_cols = jnp.repeat(k_heads, HEAD_DIM)
    w_q = (jax.random.normal(shared_keys[2], (WIDTH, WIDTH)) * fan_scale * q_cols[None, :]).astype(jnp.bfloat16)
    w_k = (jax.random.normal(shared_keys[3], (WIDTH, WIDTH)) * fan_scale * k_cols[None, :]).astype(jnp.bfloat16)
    w_v = (jax.random.normal(shared_keys[4], (WIDTH, WIDTH)) * fan_scale).astype(jnp.bfloat16)
    w_o = (jax.random.normal(shared_keys[5], (WIDTH, WIDTH)) * fan_scale).astype(jnp.bfloat16)
    q_norm_w = jax.random.uniform(shared_keys[6], (WIDTH,), minval=0.5, maxval=1.5).astype(jnp.float32)
    k_norm_w = jax.random.uniform(shared_keys[7], (WIDTH,), minval=0.5, maxval=1.5).astype(jnp.float32)
    post_norm_w = jax.random.uniform(shared_keys[8], (WIDTH,), minval=0.5, maxval=1.5).astype(jnp.float32)
    hidden = jax.random.normal(part_keys[0], (BATCH, WIDTH)).astype(jnp.bfloat16)
    k_cache = jax.random.normal(part_keys[1], (BATCH, CACHE_LEN, HEADS, HEAD_DIM)).astype(jnp.bfloat16)
    v_cache = jax.random.normal(part_keys[2], (BATCH, CACHE_LEN, HEADS, HEAD_DIM)).astype(jnp.bfloat16)
    slot_draw = jax.random.randint(part_keys[3], (BATCH,), 0, CACHE_LEN, dtype=jnp.int32)
    shift_bits = jax.random.randint(part_keys[4], (BATCH,), 0, 10, dtype=jnp.int32)
    longest = jax.random.randint(part_keys[5], (), 0, BATCH, dtype=jnp.int32)
    positions = jnp.where(jnp.arange(BATCH, dtype=jnp.int32) == longest, CACHE_LEN - 1, jnp.right_shift(slot_draw, shift_bits)).astype(jnp.int32)
    return dict(hidden=hidden, w_q=w_q, w_k=w_k, w_v=w_v, w_o=w_o, q_norm_w=q_norm_w, k_norm_w=k_norm_w, post_norm_w=post_norm_w, k_cache=k_cache, v_cache=v_cache, positions=positions)


def width_norm(vals, gain):
    wide = vals.astype(jnp.float32)
    inv_rms = lax.rsqrt(jnp.mean(wide * wide, axis=-1, keepdims=True) + NORM_EPS)
    return wide * inv_rms * gain


def apply_rope(heads_val, positions):
    half = HEAD_DIM // 2
    inv_freq = ROPE_BASE ** (-2.0 * jnp.arange(half, dtype=jnp.float32) / HEAD_DIM)
    angles = positions.astype(jnp.float32)[:, None, None] * inv_freq[None, None, :]
    cos_tab = jnp.cos(angles)
    sin_tab = jnp.sin(angles)
    wide = heads_val.astype(jnp.float32)
    first = wide[..., :half]
    second = wide[..., half:]
    return jnp.concatenate([first * cos_tab - second * sin_tab, second * cos_tab + first * sin_tab], axis=-1).astype(jnp.bfloat16)


def attend_row(row_args):
    q_row, k_row, v_row, row_pos = row_args
    slot_ids = jnp.arange(CACHE_LEN)
    scores = jnp.einsum('hd,shd->hs', q_row.astype(jnp.float32), k_row.astype(jnp.float32)) * HEAD_DIM ** -0.5
    scores = jnp.where(slot_ids[None, :] <= row_pos, scores, -1e30)
    probs = jax.nn.softmax(scores, axis=-1).astype(jnp.bfloat16)
    return jnp.einsum('hs,shd->hd', probs.astype(jnp.float32), v_row.astype(jnp.float32)).astype(jnp.bfloat16)


def reference(hidden, w_q, w_k, w_v, w_o, q_norm_w, k_norm_w, post_norm_w, k_cache, v_cache, positions):
    n_rows = hidden.shape[0]
    q_full = jnp.dot(hidden, w_q, preferred_element_type=jnp.float32).astype(jnp.bfloat16)
    k_full = jnp.dot(hidden, w_k, preferred_element_type=jnp.float32).astype(jnp.bfloat16)
    v_full = jnp.dot(hidden, w_v, preferred_element_type=jnp.float32).astype(jnp.bfloat16)
    q_normed = width_norm(q_full, q_norm_w).astype(jnp.bfloat16).reshape(n_rows, HEADS, HEAD_DIM)
    k_normed = width_norm(k_full, k_norm_w).astype(jnp.bfloat16).reshape(n_rows, HEADS, HEAD_DIM)
    q_rot = apply_rope(q_normed, positions)
    k_rot = apply_rope(k_normed, positions)
    v_heads = v_full.reshape(n_rows, HEADS, HEAD_DIM)
    at_slot = (jnp.arange(CACHE_LEN)[None, :] == positions[:, None])[:, :, None, None]
    k_new = jnp.where(at_slot, k_rot[:, None], k_cache)
    v_new = jnp.where(at_slot, v_heads[:, None], v_cache)
    attn = lax.map(attend_row, (q_rot, k_new, v_new, positions))
    a_out = jnp.dot(attn.reshape(n_rows, WIDTH), w_o, preferred_element_type=jnp.float32)
    hidden_out = (hidden.astype(jnp.float32) + width_norm(a_out, post_norm_w)).astype(jnp.bfloat16)
    return hidden_out, k_new, v_new
```

```python
import functools

import jax
import jax.numpy as jnp
from jax import lax
from jax.experimental import pallas as pl
from jax.experimental.pallas import tpu as pltpu
from jax.sharding import PartitionSpec as P

NORM_EPS = 1e-6
ROPE_BASE = 500000.0
OUT_VMEM = True


def apply_rope(heads_val, positions):
    head_dim = heads_val.shape[-1]
    half = head_dim // 2
    inv_freq = ROPE_BASE ** (-2.0 * jnp.arange(half, dtype=jnp.float32) / head_dim)
    angles = positions.astype(jnp.float32)[:, None, None] * inv_freq[None, None, :]
    cos_tab = jnp.cos(angles)
    sin_tab = jnp.sin(angles)
    wide = heads_val.astype(jnp.float32)
    first = wide[..., :half]
    second = wide[..., half:]
    return jnp.concatenate([first * cos_tab - second * sin_tab, second * cos_tab + first * sin_tab], axis=-1).astype(jnp.bfloat16)


def write_slot(cache, new_vals, positions):
    slot_ids = jnp.arange(cache.shape[1], dtype=jnp.int32)
    at_slot = (slot_ids[None, :] == positions[:, None])[:, :, None, None]
    return jnp.where(at_slot, new_vals[:, None], cache)


def attend(q_rot, k_new, v_new, positions):
    slot_ids = jnp.arange(k_new.shape[1], dtype=jnp.int32)
    scores = jnp.einsum('bhd,bshd->bhs', q_rot, k_new, preferred_element_type=jnp.float32) * k_new.shape[3] ** -0.5
    valid = (slot_ids[None, :] <= positions[:, None])[:, None, :]
    scores = jnp.where(valid, scores, -1e30)
    probs = jax.nn.softmax(scores, axis=-1).astype(jnp.bfloat16)
    return jnp.einsum('bhs,bshd->bhd', probs, v_new, preferred_element_type=jnp.float32).astype(jnp.bfloat16)


MESH = pl.DeviceIdType.MESH
SUBS = 2
LAG = 2


def finish_kernel(n_tp, o_ref, w_ref, hid_ref, gain_ref, out_ref,
                  o_in, w_in, hid, share, rs_in, rs_out,
                  x_send, x_recv, h_sem, rs_send, rs_recv, ag_send, ag_recv, d2d_send, d2d_recv):
    nz = n_tp // 2
    t = lax.axis_index("tp")
    z, k = t // 2, lax.rem(t, 2)
    up, down, mate = lax.rem(t + 2, n_tp), lax.rem(t + n_tp - 2, n_tp), z * 2 + 1 - k
    n_rows, width = out_ref.shape
    half_rows = n_rows // 2
    rows = half_rows // nz
    sub = rows // SUBS
    half = width // 2
    far = nz // 2
    chunk_of = lambda j: lax.rem(z + nz + j, nz)
    out_row = lambda j, s: pl.multiple_of(k * half_rows + chunk_of(j) * rows + s * sub, sub)
    cols = (pl.ds(0, half), pl.ds(half, half))
    target = (up, down)
    long_half = (0, 1)

    barrier = pltpu.get_barrier_semaphore()
    for peer in (up, down, mate):
        pl.semaphore_signal(barrier, inc=1, device_id={"tp": peer}, device_id_type=MESH)
    hid_copy = pltpu.make_async_copy(hid_ref.at[pl.ds(pl.multiple_of(k * half_rows + z * rows, rows), rows), :], hid, h_sem)
    hid_copy.start()
    pl.semaphore_wait(barrier, 3)

    o_copy = pltpu.make_async_remote_copy(
        o_ref.at[pl.ds(pl.multiple_of((1 - k) * half_rows, half_rows), half_rows), :], o_in,
        x_send.at[0], x_recv.at[0], device_id={"tp": mate}, device_id_type=MESH)
    w_copy = pltpu.make_async_remote_copy(w_ref, w_in, x_send.at[1], x_recv.at[1], device_id={"tp": mate}, device_id_type=MESH)
    o_copy.start()
    w_copy.start()
    o_copy.wait_recv()
    w_copy.wait_recv()

    tile = min(1024, width)

    def make_share(j):
        own = o_ref[pl.ds(pl.multiple_of(k * half_rows + chunk_of(j) * rows, rows), rows), :]
        other = o_in[pl.ds(pl.multiple_of(chunk_of(j) * rows, rows), rows), :]

        def one(c, carry):
            at = pl.ds(pl.multiple_of(c * tile, tile), tile)
            share[j % nz, :, at] = (jnp.dot(own, w_ref[:, at], preferred_element_type=jnp.float32)
                                    + jnp.dot(other, w_in[:, at], preferred_element_type=jnp.float32))
            return carry

        lax.fori_loop(0, width // tile, one, 0)

    def hops(d, c):
        return far if c == long_half[d] else far - 1

    slots = {}
    for d in range(2):
        for c in range(2):
            for h in range(hops(d, c)):
                for s in range(SUBS):
                    slots[d, c, h, s] = len(slots)

    def rs_message(d, c, h, s):
        i = slots[d, c, h, s]
        return pltpu.make_async_remote_copy(
            rs_out.at[i], rs_in.at[i], rs_send.at[i], rs_recv.at[i], device_id={"tp": target[d]}, device_id_type=MESH)

    def piece(j, c, s):
        return share[j % nz, s * sub:(s + 1) * sub, c * half:(c + 1) * half]

    def rs_step(d, c, h, s):
        ahead = hops(d, c) - h
        j = ahead if d == 0 else -ahead
        value = piece(j, c, s)
        if h > 0:
            before = rs_message(d, c, h - 1, s)
            before.wait_recv()
            value = value + rs_in[slots[d, c, h - 1, s]].astype(jnp.float32)
        rs_out[slots[d, c, h, s]] = value.astype(jnp.bfloat16)
        rs_message(d, c, h, s).start()

    def ag_message(d, c, h, s):
        j = -h if d == 0 else h
        here = out_ref.at[pl.ds(out_row(j, s), sub), cols[c]]
        i = slots[d, c, h, s]
        return pltpu.make_async_remote_copy(
            here, here, ag_send.at[i], ag_recv.at[i], device_id={"tp": target[d]}, device_id_type=MESH)

    def ag_arrival(d, c, h, s):
        j = -(h + 1) if d == 0 else h + 1
        here = out_ref.at[pl.ds(out_row(j, s), sub), cols[c]]
        i = slots[d, c, h, s]
        return pltpu.make_async_remote_copy(
            here, here, ag_send.at[i], ag_recv.at[i], device_id={"tp": target[d]}, device_id_type=MESH)

    d2d = []

    def d2d_start(j, c, s):
        here = out_ref.at[pl.ds(out_row(j, s), sub), cols[c]]
        i = len(d2d)
        copy = pltpu.make_async_remote_copy(here, here, d2d_send.at[i], d2d_recv.at[i], device_id={"tp": mate}, device_id_type=MESH)
        copy.start()
        d2d.append((j, c, s))

    def finish(s):
        total = []
        for c in range(2):
            acc = piece(0, c, s)
            for d in range(2):
                last = hops(d, c) - 1
                rs_message(d, c, last, s).wait_recv()
                acc = acc + rs_in[slots[d, c, last, s]].astype(jnp.float32)
            share[0, s * sub:(s + 1) * sub, c * half:(c + 1) * half] = acc
            total.append(jnp.sum(acc * acc, axis=-1, keepdims=True))
        inv = lax.rsqrt((total[0] + total[1]) / width + NORM_EPS)
        for c in range(2):
            at = slice(c * half, (c + 1) * half)
            normed = share[0, s * sub:(s + 1) * sub, at] * inv * gain_ref[:, at]
            out_ref[pl.ds(out_row(0, s), sub), at] = (hid[s * sub:(s + 1) * sub, at].astype(jnp.float32) + normed).astype(jnp.bfloat16)
        for d in range(2):
            for c in (long_half[d], 1 - long_half[d]):
                ag_message(d, c, 0, s).start()
        for c in range(2):
            d2d_start(0, c, s)

    def ag_step(h, s):
        for c in range(2):
            for d in range(2):
                if h - 1 < hops(d, c):
                    ag_arrival(d, c, h - 1, s).wait_recv()
                    if h < hops(d, c):
                        ag_message(d, c, h, s).start()
                    d2d_start(-h if d == 0 else h, c, s)

    def stage(g, s):
        if g < far:
            for longer in (True, False):
                for d in range(2):
                    c = long_half[d] if longer else 1 - long_half[d]
                    if g < hops(d, c):
                        if g == 0 and s == 0:
                            j = hops(d, c) if d == 0 else -hops(d, c)
                            if j % nz not in made:
                                make_share(j)
                                made.add(j % nz)
                        rs_step(d, c, g, s)
            if g == 0 and s == 0:
                for j in sorted(range(nz), key=lambda j: -min(j, nz - j)):
                    if j not in made:
                        make_share(j)
                        made.add(j)
        elif g == far:
            if s == 0:
                hid_copy.wait()
            finish(s)
        else:
            ag_step(g - far, s)

    made = set()
    last_stage = 2 * far
    for slot in range(last_stage + 1 + LAG * (SUBS - 1)):
        for s in range(SUBS):
            g = slot - LAG * s
            if 0 <= g <= last_stage:
                stage(g, s)

    o_copy.wait_send()
    w_copy.wait_send()
    for (d, c, h, s) in slots:
        rs_message(d, c, h, s).wait_send()
        ag_message(d, c, h, s).wait_send()
    for i, (j, c, s) in enumerate(d2d):
        here = out_ref.at[pl.ds(out_row(j, s), sub), cols[c]]
        there = out_ref.at[pl.ds(pl.multiple_of((1 - k) * half_rows + chunk_of(j) * rows + s * sub, sub), sub), cols[c]]
        copy = pltpu.make_async_remote_copy(here, there, d2d_send.at[i], d2d_recv.at[i], device_id={"tp": mate}, device_id_type=MESH)
        copy.wait_send()
        copy.wait_recv()


def finish_call(n_tp, attn, w_o, hidden, gain):
    n_rows, width = hidden.shape
    depth = w_o.shape[0]
    nz = n_tp // 2
    half_rows, rows = n_rows // 2, n_rows // n_tp
    sub = rows // SUBS
    n_msg = 2 * SUBS * (nz - 1)
    vmem = pl.BlockSpec(memory_space=pltpu.VMEM)
    return pl.pallas_call(
        functools.partial(finish_kernel, n_tp),
        name="finish",
        out_shape=pltpu.VMEM((n_rows, width), jnp.bfloat16) if OUT_VMEM else jax.ShapeDtypeStruct((n_rows, width), jnp.bfloat16),
        in_specs=[vmem, vmem, pl.BlockSpec(memory_space=pl.ANY), vmem],
        out_specs=vmem,
        scratch_shapes=[
            pltpu.VMEM((half_rows, depth), jnp.bfloat16),
            pltpu.VMEM((depth, width), jnp.bfloat16),
            pltpu.VMEM((rows, width), jnp.bfloat16),
            pltpu.VMEM((nz, rows, width), jnp.float32),
            pltpu.VMEM((n_msg, sub, width // 2), jnp.bfloat16),
            pltpu.VMEM((n_msg, sub, width // 2), jnp.bfloat16),
            pltpu.SemaphoreType.DMA((2,)),
            pltpu.SemaphoreType.DMA((2,)),
            pltpu.SemaphoreType.DMA,
            pltpu.SemaphoreType.DMA((n_msg,)),
            pltpu.SemaphoreType.DMA((n_msg,)),
            pltpu.SemaphoreType.DMA((n_msg,)),
            pltpu.SemaphoreType.DMA((n_msg,)),
            pltpu.SemaphoreType.DMA((2 * SUBS * nz,)),
            pltpu.SemaphoreType.DMA((2 * SUBS * nz,)),
        ],
        compiler_params=pltpu.CompilerParams(collective_id=0, has_side_effects=True, vmem_limit_bytes=40 * 2**20),
    )(attn, w_o, hidden, gain)


def solution(mesh):
    def local_step(hidden, w_q, w_k, w_v, w_o, q_norm_w, k_norm_w, post_norm_w, k_cache, v_cache, positions):
        n_rows, width = hidden.shape
        local_heads, head_dim = k_cache.shape[2], k_cache.shape[3]
        q_local = jnp.dot(hidden, w_q, preferred_element_type=jnp.float32).astype(jnp.bfloat16).astype(jnp.float32)
        k_local = jnp.dot(hidden, w_k, preferred_element_type=jnp.float32).astype(jnp.bfloat16).astype(jnp.float32)
        v_local = jnp.dot(hidden, w_v, preferred_element_type=jnp.float32).astype(jnp.bfloat16)
        energy = jnp.stack([jnp.sum(q_local * q_local, axis=-1), jnp.sum(k_local * k_local, axis=-1)])
        energy = lax.psum(energy, 'tp')
        inv_rms = lax.rsqrt(energy / width + NORM_EPS)
        q_normed = (q_local * inv_rms[0][:, None] * q_norm_w).astype(jnp.bfloat16).reshape(n_rows, local_heads, head_dim)
        k_normed = (k_local * inv_rms[1][:, None] * k_norm_w).astype(jnp.bfloat16).reshape(n_rows, local_heads, head_dim)
        q_rot = apply_rope(q_normed, positions)
        k_rot = apply_rope(k_normed, positions)
        k_new = write_slot(k_cache, k_rot, positions)
        v_new = write_slot(v_cache, v_local.reshape(n_rows, local_heads, head_dim), positions)
        attn = attend(q_rot, k_new, v_new, positions)
        hidden_out = finish_call(mesh.shape['tp'], attn.reshape(n_rows, local_heads * head_dim), w_o, hidden, post_norm_w[None, :])
        return hidden_out, k_new, v_new

    cache_spec = P('dp', None, 'tp', None)
    return jax.shard_map(local_step, mesh=mesh, in_specs=(P('dp', None), P(None, 'tp'), P(None, 'tp'), P(None, 'tp'), P('tp', None), P('tp'), P('tp'), P(None), cache_spec, cache_spec, P('dp')), out_specs=(P('dp', None), cache_spec, cache_spec), check_vma=False)
```

```python
import functools

import jax
import jax.numpy as jnp
from jax import lax
from jax.experimental import pallas as pl
from jax.experimental.pallas import tpu as pltpu
from jax.sharding import PartitionSpec as P

NORM_EPS = 1e-6
ROPE_BASE = 500000.0
OUT_VMEM = True


def apply_rope(heads_val, positions):
    head_dim = heads_val.shape[-1]
    half = head_dim // 2
    inv_freq = ROPE_BASE ** (-2.0 * jnp.arange(half, dtype=jnp.float32) / head_dim)
    angles = positions.astype(jnp.float32)[:, None, None] * inv_freq[None, None, :]
    cos_tab = jnp.cos(angles)
    sin_tab = jnp.sin(angles)
    wide = heads_val.astype(jnp.float32)
    first = wide[..., :half]
    second = wide[..., half:]
    return jnp.concatenate([first * cos_tab - second * sin_tab, second * cos_tab + first * sin_tab], axis=-1).astype(jnp.bfloat16)


ROW_BLOCK = 64
GROUP = 8


def attend_kernel(slots, heads, pos_ref, q_ref, k_ref, v_ref, posb_ref, kc_ref, vc_ref, o_ref, kn_ref, vn_ref, kf, vf):
    block = q_ref.shape[0]
    dim = q_ref.shape[1] // heads
    lines = slots * heads
    step = pl.program_id(0)
    kf[...] = k_ref[...].astype(jnp.float32)
    vf[...] = v_ref[...].astype(jnp.float32)
    line = lax.broadcasted_iota(jnp.int32, (lines // 2, dim), 0)
    first = lax.rem(line, heads) == 0
    slot_of = [(line // heads + part * (slots // 2)).astype(jnp.float32).astype(jnp.bfloat16) for part in range(2)]

    def insert(r):
        p = jnp.full((lines // 2, dim), pos_ref[step * block + r].astype(jnp.float32)).astype(jnp.bfloat16)
        for src, old, new in ((kf, kc_ref, kn_ref), (vf, vc_ref, vn_ref)):
            h0 = jnp.broadcast_to(src[pl.ds(r, 1), 0:dim], (lines // 2, dim))
            h1 = jnp.broadcast_to(src[pl.ds(r, 1), dim:2 * dim], (lines // 2, dim))
            fresh = jnp.where(first, h0, h1).astype(jnp.bfloat16)
            for part in range(2):
                at = pl.ds(r * lines + part * (lines // 2), lines // 2)
                new[at, :] = jnp.where(slot_of[part] == p, fresh, old[at, :])

    for r in range(block):
        insert(r)

    n_groups = block // GROUP
    wide = GROUP * lines
    m = lax.broadcasted_iota(jnp.int32, (heads * GROUP, wide), 0)
    n = lax.broadcasted_iota(jnp.int32, (heads * GROUP, wide), 1)
    own = (lax.rem(m, GROUP) == n // lines) & (m // GROUP == lax.rem(n, heads))
    slot = jnp.where(own, (lax.rem(n, lines) // heads).astype(jnp.float32), 1e9)
    scores = []
    for g in range(n_groups):
        rows = slice(g * GROUP, (g + 1) * GROUP)
        q = jnp.concatenate([q_ref[rows, h * dim:(h + 1) * dim] for h in range(heads)], axis=0)
        keys = kn_ref[g * wide:(g + 1) * wide, :]
        s = lax.dot_general(q, keys, (((1,), (1,)), ((), ())), preferred_element_type=jnp.float32) * dim ** -0.5
        at = jnp.concatenate([posb_ref[rows, :]] * heads, axis=0)
        at = jnp.concatenate([at] * (wide // at.shape[1]), axis=1)
        scores.append(jnp.where(slot <= at, s, -1e30))
    for g in range(n_groups):
        s = scores[g]
        e = jnp.exp(s - jnp.max(s, axis=-1, keepdims=True))
        probs = (e / jnp.sum(e, axis=-1, keepdims=True)).astype(jnp.bfloat16)
        o = jnp.dot(probs, vn_ref[g * wide:(g + 1) * wide, :], preferred_element_type=jnp.float32).astype(jnp.bfloat16)
        for h in range(heads):
            o_ref[g * GROUP:(g + 1) * GROUP, h * dim:(h + 1) * dim] = o[h * GROUP:(h + 1) * GROUP]


def attend_call(q, k, v, posb, positions, k_cache, v_cache):
    n_rows, slots, heads, dim = k_cache.shape
    lines = slots * heads
    flat = (n_rows * lines, dim)
    block = ROW_BLOCK
    row_spec = pl.BlockSpec((block, heads * dim), lambda i, pos: (i, 0))
    cache_spec = pl.BlockSpec((block * lines, dim), lambda i, pos: (i, 0))
    o, k_new, v_new = pl.pallas_call(
        functools.partial(attend_kernel, slots, heads),
        name="attend",
        out_shape=[jax.ShapeDtypeStruct((n_rows, heads * dim), jnp.bfloat16),
                   jax.ShapeDtypeStruct(flat, jnp.bfloat16), jax.ShapeDtypeStruct(flat, jnp.bfloat16)],
        grid_spec=pltpu.PrefetchScalarGridSpec(
            num_scalar_prefetch=1,
            grid=(n_rows // block,),
            in_specs=[row_spec, row_spec, row_spec, pl.BlockSpec((block, dim), lambda i, pos: (i, 0)), cache_spec, cache_spec],
            out_specs=[row_spec, cache_spec, cache_spec],
            scratch_shapes=[pltpu.VMEM((block, heads * dim), jnp.float32), pltpu.VMEM((block, heads * dim), jnp.float32)],
        ),
        compiler_params=pltpu.CompilerParams(vmem_limit_bytes=24 * 2**20),
    )(positions, q, k, v, posb, k_cache.reshape(flat), v_cache.reshape(flat))
    return o, k_new.reshape(k_cache.shape), v_new.reshape(v_cache.shape)


MESH = pl.DeviceIdType.MESH
SUBS = 2
LAG = 2


def finish_kernel(n_tp, o_ref, w_ref, hid_ref, gain_ref, out_ref,
                  o_in, w_in, hid, share, rs_in, rs_out,
                  x_send, x_recv, h_sem, rs_send, rs_recv, ag_send, ag_recv, d2d_send, d2d_recv):
    nz = n_tp // 2
    t = lax.axis_index("tp")
    z, k = t // 2, lax.rem(t, 2)
    up, down, mate = lax.rem(t + 2, n_tp), lax.rem(t + n_tp - 2, n_tp), z * 2 + 1 - k
    n_rows, width = out_ref.shape
    half_rows = n_rows // 2
    rows = half_rows // nz
    sub = rows // SUBS
    half = width // 2
    far = nz // 2
    chunk_of = lambda j: lax.rem(z + nz + j, nz)
    out_row = lambda j, s: pl.multiple_of(k * half_rows + chunk_of(j) * rows + s * sub, sub)
    cols = (pl.ds(0, half), pl.ds(half, half))
    target = (up, down)
    long_half = (0, 1)

    barrier = pltpu.get_barrier_semaphore()
    for peer in (up, down, mate):
        pl.semaphore_signal(barrier, inc=1, device_id={"tp": peer}, device_id_type=MESH)
    hid_copy = pltpu.make_async_copy(hid_ref.at[pl.ds(pl.multiple_of(k * half_rows + z * rows, rows), rows), :], hid, h_sem)
    hid_copy.start()
    pl.semaphore_wait(barrier, 3)

    o_copy = pltpu.make_async_remote_copy(
        o_ref.at[pl.ds(pl.multiple_of((1 - k) * half_rows, half_rows), half_rows), :], o_in,
        x_send.at[0], x_recv.at[0], device_id={"tp": mate}, device_id_type=MESH)
    w_copy = pltpu.make_async_remote_copy(w_ref, w_in, x_send.at[1], x_recv.at[1], device_id={"tp": mate}, device_id_type=MESH)
    o_copy.start()
    w_copy.start()
    o_copy.wait_recv()
    w_copy.wait_recv()

    tile = min(1024, width)

    def make_share(j):
        own = o_ref[pl.ds(pl.multiple_of(k * half_rows + chunk_of(j) * rows, rows), rows), :]
        other = o_in[pl.ds(pl.multiple_of(chunk_of(j) * rows, rows), rows), :]

        def one(c, carry):
            at = pl.ds(pl.multiple_of(c * tile, tile), tile)
            share[j % nz, :, at] = (jnp.dot(own, w_ref[:, at], preferred_element_type=jnp.float32)
                                    + jnp.dot(other, w_in[:, at], preferred_element_type=jnp.float32))
            return carry

        lax.fori_loop(0, width // tile, one, 0)

    def hops(d, c):
        return far if c == long_half[d] else far - 1

    slots = {}
    for d in range(2):
        for c in range(2):
            for h in range(hops(d, c)):
                for s in range(SUBS):
                    slots[d, c, h, s] = len(slots)

    def rs_message(d, c, h, s):
        i = slots[d, c, h, s]
        return pltpu.make_async_remote_copy(
            rs_out.at[i], rs_in.at[i], rs_send.at[i], rs_recv.at[i], device_id={"tp": target[d]}, device_id_type=MESH)

    def piece(j, c, s):
        return share[j % nz, s * sub:(s + 1) * sub, c * half:(c + 1) * half]

    def rs_step(d, c, h, s):
        ahead = hops(d, c) - h
        j = ahead if d == 0 else -ahead
        value = piece(j, c, s)
        if h > 0:
            before = rs_message(d, c, h - 1, s)
            before.wait_recv()
            value = value + rs_in[slots[d, c, h - 1, s]].astype(jnp.float32)
        rs_out[slots[d, c, h, s]] = value.astype(jnp.bfloat16)
        rs_message(d, c, h, s).start()

    def ag_message(d, c, h, s):
        j = -h if d == 0 else h
        here = out_ref.at[pl.ds(out_row(j, s), sub), cols[c]]
        i = slots[d, c, h, s]
        return pltpu.make_async_remote_copy(
            here, here, ag_send.at[i], ag_recv.at[i], device_id={"tp": target[d]}, device_id_type=MESH)

    def ag_arrival(d, c, h, s):
        j = -(h + 1) if d == 0 else h + 1
        here = out_ref.at[pl.ds(out_row(j, s), sub), cols[c]]
        i = slots[d, c, h, s]
        return pltpu.make_async_remote_copy(
            here, here, ag_send.at[i], ag_recv.at[i], device_id={"tp": target[d]}, device_id_type=MESH)

    d2d = []

    def d2d_start(j, c, s):
        here = out_ref.at[pl.ds(out_row(j, s), sub), cols[c]]
        i = len(d2d)
        copy = pltpu.make_async_remote_copy(here, here, d2d_send.at[i], d2d_recv.at[i], device_id={"tp": mate}, device_id_type=MESH)
        copy.start()
        d2d.append((j, c, s))

    def finish(s):
        total = []
        for c in range(2):
            acc = piece(0, c, s)
            for d in range(2):
                last = hops(d, c) - 1
                rs_message(d, c, last, s).wait_recv()
                acc = acc + rs_in[slots[d, c, last, s]].astype(jnp.float32)
            share[0, s * sub:(s + 1) * sub, c * half:(c + 1) * half] = acc
            total.append(jnp.sum(acc * acc, axis=-1, keepdims=True))
        inv = lax.rsqrt((total[0] + total[1]) / width + NORM_EPS)
        for c in range(2):
            at = slice(c * half, (c + 1) * half)
            normed = share[0, s * sub:(s + 1) * sub, at] * inv * gain_ref[:, at]
            out_ref[pl.ds(out_row(0, s), sub), at] = (hid[s * sub:(s + 1) * sub, at].astype(jnp.float32) + normed).astype(jnp.bfloat16)
        for d in range(2):
            for c in (long_half[d], 1 - long_half[d]):
                ag_message(d, c, 0, s).start()
        for c in range(2):
            d2d_start(0, c, s)

    def ag_step(h, s):
        for c in range(2):
            for d in range(2):
                if h - 1 < hops(d, c):
                    ag_arrival(d, c, h - 1, s).wait_recv()
                    if h < hops(d, c):
                        ag_message(d, c, h, s).start()
                    d2d_start(-h if d == 0 else h, c, s)

    def stage(g, s):
        if g < far:
            for longer in (True, False):
                for d in range(2):
                    c = long_half[d] if longer else 1 - long_half[d]
                    if g < hops(d, c):
                        if g == 0 and s == 0:
                            j = hops(d, c) if d == 0 else -hops(d, c)
                            if j % nz not in made:
                                make_share(j)
                                made.add(j % nz)
                        rs_step(d, c, g, s)
            if g == 0 and s == 0:
                for j in sorted(range(nz), key=lambda j: -min(j, nz - j)):
                    if j not in made:
                        make_share(j)
                        made.add(j)
        elif g == far:
            if s == 0:
                hid_copy.wait()
            finish(s)
        else:
            ag_step(g - far, s)

    made = set()
    last_stage = 2 * far
    for slot in range(last_stage + 1 + LAG * (SUBS - 1)):
        for s in range(SUBS):
            g = slot - LAG * s
            if 0 <= g <= last_stage:
                stage(g, s)

    o_copy.wait_send()
    w_copy.wait_send()
    for (d, c, h, s) in slots:
        rs_message(d, c, h, s).wait_send()
        ag_message(d, c, h, s).wait_send()
    for i, (j, c, s) in enumerate(d2d):
        here = out_ref.at[pl.ds(out_row(j, s), sub), cols[c]]
        there = out_ref.at[pl.ds(pl.multiple_of((1 - k) * half_rows + chunk_of(j) * rows + s * sub, sub), sub), cols[c]]
        copy = pltpu.make_async_remote_copy(here, there, d2d_send.at[i], d2d_recv.at[i], device_id={"tp": mate}, device_id_type=MESH)
        copy.wait_send()
        copy.wait_recv()


def finish_call(n_tp, attn, w_o, hidden, gain):
    n_rows, width = hidden.shape
    depth = w_o.shape[0]
    nz = n_tp // 2
    half_rows, rows = n_rows // 2, n_rows // n_tp
    sub = rows // SUBS
    n_msg = 2 * SUBS * (nz - 1)
    vmem = pl.BlockSpec(memory_space=pltpu.VMEM)
    return pl.pallas_call(
        functools.partial(finish_kernel, n_tp),
        name="finish",
        out_shape=pltpu.VMEM((n_rows, width), jnp.bfloat16) if OUT_VMEM else jax.ShapeDtypeStruct((n_rows, width), jnp.bfloat16),
        in_specs=[vmem, vmem, pl.BlockSpec(memory_space=pl.ANY), vmem],
        out_specs=vmem,
        scratch_shapes=[
            pltpu.VMEM((half_rows, depth), jnp.bfloat16),
            pltpu.VMEM((depth, width), jnp.bfloat16),
            pltpu.VMEM((rows, width), jnp.bfloat16),
            pltpu.VMEM((nz, rows, width), jnp.float32),
            pltpu.VMEM((n_msg, sub, width // 2), jnp.bfloat16),
            pltpu.VMEM((n_msg, sub, width // 2), jnp.bfloat16),
            pltpu.SemaphoreType.DMA((2,)),
            pltpu.SemaphoreType.DMA((2,)),
            pltpu.SemaphoreType.DMA,
            pltpu.SemaphoreType.DMA((n_msg,)),
            pltpu.SemaphoreType.DMA((n_msg,)),
            pltpu.SemaphoreType.DMA((n_msg,)),
            pltpu.SemaphoreType.DMA((n_msg,)),
            pltpu.SemaphoreType.DMA((2 * SUBS * nz,)),
            pltpu.SemaphoreType.DMA((2 * SUBS * nz,)),
        ],
        compiler_params=pltpu.CompilerParams(collective_id=0, has_side_effects=True, vmem_limit_bytes=40 * 2**20),
    )(attn, w_o, hidden, gain)


def solution(mesh):
    def local_step(hidden, w_q, w_k, w_v, w_o, q_norm_w, k_norm_w, post_norm_w, k_cache, v_cache, positions):
        n_rows, width = hidden.shape
        local_heads, head_dim = k_cache.shape[2], k_cache.shape[3]
        q_local = jnp.dot(hidden, w_q, preferred_element_type=jnp.float32).astype(jnp.bfloat16).astype(jnp.float32)
        k_local = jnp.dot(hidden, w_k, preferred_element_type=jnp.float32).astype(jnp.bfloat16).astype(jnp.float32)
        v_local = jnp.dot(hidden, w_v, preferred_element_type=jnp.float32).astype(jnp.bfloat16)
        energy = jnp.stack([jnp.sum(q_local * q_local, axis=-1), jnp.sum(k_local * k_local, axis=-1)])
        energy = lax.psum(energy, 'tp')
        inv_rms = lax.rsqrt(energy / width + NORM_EPS)
        q_normed = (q_local * inv_rms[0][:, None] * q_norm_w).astype(jnp.bfloat16).reshape(n_rows, local_heads, head_dim)
        k_normed = (k_local * inv_rms[1][:, None] * k_norm_w).astype(jnp.bfloat16).reshape(n_rows, local_heads, head_dim)
        q_rot = apply_rope(q_normed, positions)
        k_rot = apply_rope(k_normed, positions)
        posb = jnp.broadcast_to(positions.astype(jnp.float32)[:, None], (n_rows, head_dim))
        attn, k_new, v_new = attend_call(q_rot.reshape(n_rows, -1), k_rot.reshape(n_rows, -1), v_local, posb, positions, k_cache, v_cache)
        hidden_out = finish_call(mesh.shape['tp'], attn, w_o, hidden, post_norm_w[None, :])
        return hidden_out, k_new, v_new

    cache_spec = P('dp', None, 'tp', None)
    return jax.shard_map(local_step, mesh=mesh, in_specs=(P('dp', None), P(None, 'tp'), P(None, 'tp'), P(None, 'tp'), P('tp', None), P('tp'), P('tp'), P(None), cache_spec, cache_spec, P('dp')), out_specs=(P('dp', None), cache_spec, cache_spec), check_vma=False)
```

```python
import functools

import jax
import jax.numpy as jnp
import numpy as np
from jax import lax
from jax.experimental import pallas as pl
from jax.experimental.pallas import tpu as pltpu
from jax.sharding import PartitionSpec as P

NORM_EPS = 1e-6
ROPE_BASE = 500000.0
OUT_VMEM = True


MESH = pl.DeviceIdType.MESH
DEPTH_CUTS = 4
TABLE_ROWS = 128


def rope_table(slots, dim):
    half = dim // 2
    inv_freq = np.float32(ROPE_BASE) ** (np.float32(-2.0) * np.arange(half, dtype=np.float32) / np.float32(dim))
    angles = (np.arange(slots, dtype=np.float32)[:, None] * inv_freq.astype(np.float32)[None, :]).astype(np.float64)
    cos_tab, sin_tab = np.cos(angles), np.sin(angles)
    rest = np.concatenate([cos_tab, cos_tab, -sin_tab, sin_tab], axis=1).astype(np.float32)
    out = np.zeros((TABLE_ROWS, 2 * dim), np.float32)
    for part in range(3):
        high = rest.astype(jnp.bfloat16).astype(np.float32)
        out[part * slots:(part + 1) * slots] = high
        rest = rest - high
    return jnp.asarray(out, dtype=jnp.bfloat16)


def project_kernel(n_tp, slots, dim, pos_ref, table_ref, qg_ref, kg_ref, hid_ref, wq_ref, wk_ref, wv_ref, wo_ref,
                   q_ref, k_ref, v_ref, posb_ref, wo_in,
                   hid, wqk, wv, acc, vacc, cosb, sinb, e_mine, e_in,
                   in_sem, v_sem, e_send, e_recv, w_sem):
    t = lax.axis_index("tp")
    mate = t + 1 - 2 * lax.rem(t, 2)
    n_rows, width = hid_ref.shape
    local = wq_ref.shape[1]
    heads = local // dim
    cut = width // DEPTH_CUTS
    barrier = pltpu.get_barrier_semaphore()
    for off in range(1, n_tp):
        pl.semaphore_signal(barrier, inc=1, device_id={"tp": lax.rem(t + off, n_tp)}, device_id_type=MESH)

    loads = []
    for c in range(DEPTH_CUTS):
        at = pl.ds(c * cut, cut)
        loads.append([
            pltpu.make_async_copy(hid_ref.at[:, at], hid.at[c], in_sem.at[c, 0]),
            pltpu.make_async_copy(wq_ref.at[at, :], wqk.at[c, :, pl.ds(0, local)], in_sem.at[c, 1]),
            pltpu.make_async_copy(wk_ref.at[at, :], wqk.at[c, :, pl.ds(local, local)], in_sem.at[c, 2])])
    v_loads = [pltpu.make_async_copy(wv_ref.at[pl.ds(c * cut, cut), :], wv.at[c], v_sem.at[c]) for c in range(DEPTH_CUTS)]
    for group in loads:
        for copy in group:
            copy.start()
    for copy in v_loads:
        copy.start()

    w_copy = pltpu.make_async_remote_copy(wo_ref, wo_in, w_sem.at[0], w_sem.at[1], device_id={"tp": mate}, device_id_type=MESH)
    for c in range(DEPTH_CUTS):
        for copy in loads[c]:
            copy.wait()
        part = jnp.dot(hid[c], wqk[c], preferred_element_type=jnp.float32)
        if c == 0:
            acc[...] = part
        else:
            acc[...] += part
        if c == DEPTH_CUTS - 2:
            pl.semaphore_wait(barrier, n_tp - 1)
            w_copy.start()

    lanes = e_mine.shape[1]
    blocks = n_rows // lanes
    ones = jnp.ones((8, local), jnp.bfloat16)
    nt = (((1,), (1,)), ((), ()))
    for i in range(2):
        rounded = acc[:, i * local:(i + 1) * local].astype(jnp.bfloat16).astype(jnp.float32)
        square = rounded * rounded
        high = square.astype(jnp.bfloat16)
        low = (square - high.astype(jnp.float32)).astype(jnp.bfloat16)
        energy = (lax.dot_general(ones, high, nt, preferred_element_type=jnp.float32)
                  + lax.dot_general(ones, low, nt, preferred_element_type=jnp.float32))
        for b in range(blocks):
            e_mine[i * blocks + b:i * blocks + b + 1, :] = energy[0:1, b * lanes:(b + 1) * lanes]
    sends = [pltpu.make_async_remote_copy(
        e_mine, e_in.at[off], e_send.at[off], e_recv.at[off],
        device_id={"tp": lax.rem(t + off, n_tp)}, device_id_type=MESH) for off in range(1, n_tp)]
    for copy in sends:
        copy.start()

    for c in range(DEPTH_CUTS):
        v_loads[c].wait()
        part = jnp.dot(hid[c], wv[c], preferred_element_type=jnp.float32)
        if c == 0:
            vacc[...] = part
        elif c < DEPTH_CUTS - 1:
            vacc[...] += part
        else:
            v_ref[...] = (vacc[...] + part).astype(jnp.bfloat16)
    lane = lax.broadcasted_iota(jnp.int32, (lanes, TABLE_ROWS), 1)
    which = jnp.where(lane < 3 * slots, lax.rem(lane, slots), -1).astype(jnp.float32)
    for b in range(blocks):
        at = slice(b * lanes, (b + 1) * lanes)
        column = jnp.broadcast_to(pos_ref[b:b + 1, :].astype(jnp.float32), (lanes, lanes)).T
        posb_ref[at, :] = column
        hot = jnp.where(which == column, 1.0, 0.0).astype(jnp.bfloat16)
        factors = jnp.dot(hot, table_ref[...], preferred_element_type=jnp.float32)
        cosb[at, :] = factors[:, :dim]
        sinb[at, :] = factors[:, dim:]

    total = e_mine[...]
    for i, copy in enumerate(sends):
        copy.wait_recv()
        total = total + e_in[i + 1]
    inv = lax.rsqrt(total / width + NORM_EPS)
    for b in range(blocks):
        at = slice(b * lanes, (b + 1) * lanes)
        for i, (gain, out) in enumerate(((qg_ref, q_ref), (kg_ref, k_ref))):
            scale = jnp.broadcast_to(inv[i * blocks + b:i * blocks + b + 1, :], (lanes, lanes)).T
            for h in range(heads):
                cols = slice(h * dim, (h + 1) * dim)
                x = acc[at, i * local + h * dim:i * local + (h + 1) * dim].astype(jnp.bfloat16).astype(jnp.float32)
                x = (x * scale * gain[:, cols]).astype(jnp.bfloat16).astype(jnp.float32)
                out[at, cols] = (x * cosb[at, :] + pltpu.roll(x, dim // 2, 1) * sinb[at, :]).astype(jnp.bfloat16)
    for copy in sends:
        copy.wait_send()
    w_copy.wait()


def project_call(n_tp, hidden, w_q, w_k, w_v, w_o, q_gain, k_gain, positions, slots, dim):
    n_rows, width = hidden.shape
    local = w_q.shape[1]
    lanes = 128
    cut = width // DEPTH_CUTS
    vmem, hbm = pl.BlockSpec(memory_space=pltpu.VMEM), pl.BlockSpec(memory_space=pltpu.HBM)
    return pl.pallas_call(
        functools.partial(project_kernel, n_tp, slots, dim),
        name="project",
        out_shape=[pltpu.VMEM((n_rows, local), jnp.bfloat16)] * 3
        + [pltpu.VMEM((n_rows, lanes), jnp.float32), pltpu.VMEM(w_o.shape, jnp.bfloat16)],
        in_specs=[vmem] * 4 + [hbm] * 5,
        out_specs=[vmem] * 5,
        scratch_shapes=[
            pltpu.VMEM((DEPTH_CUTS, n_rows, cut), jnp.bfloat16),
            pltpu.VMEM((DEPTH_CUTS, cut, 2 * local), jnp.bfloat16),
            pltpu.VMEM((DEPTH_CUTS, cut, local), jnp.bfloat16),
            pltpu.VMEM((n_rows, 2 * local), jnp.float32),
            pltpu.VMEM((n_rows, local), jnp.float32),
            pltpu.VMEM((n_rows, dim), jnp.float32),
            pltpu.VMEM((n_rows, dim), jnp.float32),
            pltpu.VMEM((2 * n_rows // lanes, lanes), jnp.float32),
            pltpu.VMEM((n_tp, 2 * n_rows // lanes, lanes), jnp.float32),
            pltpu.SemaphoreType.DMA((DEPTH_CUTS, 3)),
            pltpu.SemaphoreType.DMA((DEPTH_CUTS,)),
            pltpu.SemaphoreType.DMA((n_tp,)),
            pltpu.SemaphoreType.DMA((n_tp,)),
            pltpu.SemaphoreType.DMA((2,)),
        ],
        compiler_params=pltpu.CompilerParams(collective_id=1, has_side_effects=True, vmem_limit_bytes=24 * 2**20),
        cost_estimate=pl.CostEstimate(flops=6 * n_rows * width * local, bytes_accessed=2 * (n_rows * width + 3 * width * local), transcendentals=0),
    )(positions.reshape(n_rows // lanes, lanes), rope_table(slots, dim), q_gain, k_gain, hidden, w_q, w_k, w_v, w_o)


ROW_BLOCK = 64
GROUP = 8


def attend_kernel(slots, heads, pos_ref, q_ref, k_ref, v_ref, posb_ref, kc_ref, vc_ref, o_ref, kn_ref, vn_ref, kf, vf):
    block = q_ref.shape[0]
    dim = q_ref.shape[1] // heads
    lines = slots * heads
    step = pl.program_id(0)
    kf[...] = k_ref[...].astype(jnp.float32)
    vf[...] = v_ref[...].astype(jnp.float32)
    line = lax.broadcasted_iota(jnp.int32, (lines // 2, dim), 0)
    first = lax.rem(line, heads) == 0
    slot_of = [(line // heads + part * (slots // 2)).astype(jnp.float32).astype(jnp.bfloat16) for part in range(2)]

    def insert(r):
        p = jnp.full((lines // 2, dim), pos_ref[step * block + r].astype(jnp.float32)).astype(jnp.bfloat16)
        for src, old, new in ((kf, kc_ref, kn_ref), (vf, vc_ref, vn_ref)):
            h0 = jnp.broadcast_to(src[pl.ds(r, 1), 0:dim], (lines // 2, dim))
            h1 = jnp.broadcast_to(src[pl.ds(r, 1), dim:2 * dim], (lines // 2, dim))
            fresh = jnp.where(first, h0, h1).astype(jnp.bfloat16)
            for part in range(2):
                at = pl.ds(r * lines + part * (lines // 2), lines // 2)
                new[at, :] = jnp.where(slot_of[part] == p, fresh, old[at, :])

    for r in range(block):
        insert(r)

    n_groups = block // GROUP
    wide = GROUP * lines
    m = lax.broadcasted_iota(jnp.int32, (heads * GROUP, wide), 0)
    n = lax.broadcasted_iota(jnp.int32, (heads * GROUP, wide), 1)
    own = (lax.rem(m, GROUP) == n // lines) & (m // GROUP == lax.rem(n, heads))
    slot = jnp.where(own, (lax.rem(n, lines) // heads).astype(jnp.float32), 1e9)
    scores = []
    for g in range(n_groups):
        rows = slice(g * GROUP, (g + 1) * GROUP)
        q = jnp.concatenate([q_ref[rows, h * dim:(h + 1) * dim] for h in range(heads)], axis=0)
        keys = kn_ref[g * wide:(g + 1) * wide, :]
        s = lax.dot_general(q, keys, (((1,), (1,)), ((), ())), preferred_element_type=jnp.float32) * dim ** -0.5
        at = jnp.concatenate([posb_ref[rows, :]] * heads, axis=0)
        at = jnp.concatenate([at] * (wide // at.shape[1]), axis=1)
        scores.append(jnp.where(slot <= at, s, -1e30))
    for g in range(n_groups):
        s = scores[g]
        e = jnp.exp(s - jnp.max(s, axis=-1, keepdims=True))
        probs = (e / jnp.sum(e, axis=-1, keepdims=True)).astype(jnp.bfloat16)
        o = jnp.dot(probs, vn_ref[g * wide:(g + 1) * wide, :], preferred_element_type=jnp.float32).astype(jnp.bfloat16)
        for h in range(heads):
            o_ref[g * GROUP:(g + 1) * GROUP, h * dim:(h + 1) * dim] = o[h * GROUP:(h + 1) * GROUP]


def attend_call(q, k, v, posb, positions, k_cache, v_cache):
    n_rows, slots, heads, dim = k_cache.shape
    lines = slots * heads
    flat = (n_rows * lines, dim)
    block = ROW_BLOCK
    row_spec = pl.BlockSpec((block, heads * dim), lambda i, pos: (i, 0))
    cache_spec = pl.BlockSpec((block * lines, dim), lambda i, pos: (i, 0))
    o, k_new, v_new = pl.pallas_call(
        functools.partial(attend_kernel, slots, heads),
        name="attend",
        out_shape=[jax.ShapeDtypeStruct((n_rows, heads * dim), jnp.bfloat16),
                   jax.ShapeDtypeStruct(flat, jnp.bfloat16), jax.ShapeDtypeStruct(flat, jnp.bfloat16)],
        grid_spec=pltpu.PrefetchScalarGridSpec(
            num_scalar_prefetch=1,
            grid=(n_rows // block,),
            in_specs=[row_spec, row_spec, row_spec, pl.BlockSpec((block, dim), lambda i, pos: (i, 0)), cache_spec, cache_spec],
            out_specs=[row_spec, cache_spec, cache_spec],
            scratch_shapes=[pltpu.VMEM((block, heads * dim), jnp.float32), pltpu.VMEM((block, heads * dim), jnp.float32)],
        ),
        compiler_params=pltpu.CompilerParams(vmem_limit_bytes=24 * 2**20),
    )(positions, q, k, v, posb, k_cache.reshape(flat), v_cache.reshape(flat))
    return o, k_new.reshape(k_cache.shape), v_new.reshape(v_cache.shape)


SUBS = 2
LAG = 2


def finish_kernel(n_tp, o_ref, w_ref, w_in, hid_ref, gain_ref, out_ref,
                  o_in, hid, share, rs_in, rs_out,
                  x_send, x_recv, h_sem, rs_send, rs_recv, ag_send, ag_recv, d2d_send, d2d_recv):
    nz = n_tp // 2
    t = lax.axis_index("tp")
    z, k = t // 2, lax.rem(t, 2)
    up, down, mate = lax.rem(t + 2, n_tp), lax.rem(t + n_tp - 2, n_tp), z * 2 + 1 - k
    n_rows, width = out_ref.shape
    half_rows = n_rows // 2
    rows = half_rows // nz
    sub = rows // SUBS
    half = width // 2
    far = nz // 2
    chunk_of = lambda j: lax.rem(z + nz + j, nz)
    out_row = lambda j, s: pl.multiple_of(k * half_rows + chunk_of(j) * rows + s * sub, sub)
    cols = (pl.ds(0, half), pl.ds(half, half))
    target = (up, down)
    long_half = (0, 1)

    barrier = pltpu.get_barrier_semaphore()
    for peer in (up, down, mate):
        pl.semaphore_signal(barrier, inc=1, device_id={"tp": peer}, device_id_type=MESH)
    hid_copy = pltpu.make_async_copy(hid_ref.at[pl.ds(pl.multiple_of(k * half_rows + z * rows, rows), rows), :], hid, h_sem)
    hid_copy.start()
    pl.semaphore_wait(barrier, 3)

    o_copy = pltpu.make_async_remote_copy(
        o_ref.at[pl.ds(pl.multiple_of((1 - k) * half_rows, half_rows), half_rows), :], o_in,
        x_send, x_recv, device_id={"tp": mate}, device_id_type=MESH)
    o_copy.start()
    o_copy.wait_recv()

    tile = min(1024, width)

    def make_share(j):
        own = o_ref[pl.ds(pl.multiple_of(k * half_rows + chunk_of(j) * rows, rows), rows), :]
        other = o_in[pl.ds(pl.multiple_of(chunk_of(j) * rows, rows), rows), :]

        def one(c, carry):
            at = pl.ds(pl.multiple_of(c * tile, tile), tile)
            share[j % nz, :, at] = (jnp.dot(own, w_ref[:, at], preferred_element_type=jnp.float32)
                                    + jnp.dot(other, w_in[:, at], preferred_element_type=jnp.float32))
            return carry

        lax.fori_loop(0, width // tile, one, 0)

    def hops(d, c):
        return far if c == long_half[d] else far - 1

    slots = {}
    for d in range(2):
        for c in range(2):
            for h in range(hops(d, c)):
                for s in range(SUBS):
                    slots[d, c, h, s] = len(slots)

    def rs_message(d, c, h, s):
        i = slots[d, c, h, s]
        return pltpu.make_async_remote_copy(
            rs_out.at[i], rs_in.at[i], rs_send.at[i], rs_recv.at[i], device_id={"tp": target[d]}, device_id_type=MESH)

    def piece(j, c, s):
        return share[j % nz, s * sub:(s + 1) * sub, c * half:(c + 1) * half]

    def rs_step(d, c, h, s):
        ahead = hops(d, c) - h
        j = ahead if d == 0 else -ahead
        value = piece(j, c, s)
        if h > 0:
            before = rs_message(d, c, h - 1, s)
            before.wait_recv()
            value = value + rs_in[slots[d, c, h - 1, s]].astype(jnp.float32)
        rs_out[slots[d, c, h, s]] = value.astype(jnp.bfloat16)
        rs_message(d, c, h, s).start()

    def ag_message(d, c, h, s):
        j = -h if d == 0 else h
        here = out_ref.at[pl.ds(out_row(j, s), sub), cols[c]]
        i = slots[d, c, h, s]
        return pltpu.make_async_remote_copy(
            here, here, ag_send.at[i], ag_recv.at[i], device_id={"tp": target[d]}, device_id_type=MESH)

    def ag_arrival(d, c, h, s):
        j = -(h + 1) if d == 0 else h + 1
        here = out_ref.at[pl.ds(out_row(j, s), sub), cols[c]]
        i = slots[d, c, h, s]
        return pltpu.make_async_remote_copy(
            here, here, ag_send.at[i], ag_recv.at[i], device_id={"tp": target[d]}, device_id_type=MESH)

    d2d = []

    def d2d_start(j, c, s):
        here = out_ref.at[pl.ds(out_row(j, s), sub), cols[c]]
        i = len(d2d)
        copy = pltpu.make_async_remote_copy(here, here, d2d_send.at[i], d2d_recv.at[i], device_id={"tp": mate}, device_id_type=MESH)
        copy.start()
        d2d.append((j, c, s))

    def finish(s):
        total = []
        for c in range(2):
            acc = piece(0, c, s)
            for d in range(2):
                last = hops(d, c) - 1
                rs_message(d, c, last, s).wait_recv()
                acc = acc + rs_in[slots[d, c, last, s]].astype(jnp.float32)
            share[0, s * sub:(s + 1) * sub, c * half:(c + 1) * half] = acc
            total.append(jnp.sum(acc * acc, axis=-1, keepdims=True))
        inv = lax.rsqrt((total[0] + total[1]) / width + NORM_EPS)
        for c in range(2):
            at = slice(c * half, (c + 1) * half)
            normed = share[0, s * sub:(s + 1) * sub, at] * inv * gain_ref[:, at]
            out_ref[pl.ds(out_row(0, s), sub), at] = (hid[s * sub:(s + 1) * sub, at].astype(jnp.float32) + normed).astype(jnp.bfloat16)
        for d in range(2):
            for c in (long_half[d], 1 - long_half[d]):
                ag_message(d, c, 0, s).start()
        for c in range(2):
            d2d_start(0, c, s)

    def ag_step(h, s):
        for c in range(2):
            for d in range(2):
                if h - 1 < hops(d, c):
                    ag_arrival(d, c, h - 1, s).wait_recv()
                    if h < hops(d, c):
                        ag_message(d, c, h, s).start()
                    d2d_start(-h if d == 0 else h, c, s)

    def stage(g, s):
        if g < far:
            for longer in (True, False):
                for d in range(2):
                    c = long_half[d] if longer else 1 - long_half[d]
                    if g < hops(d, c):
                        if g == 0 and s == 0:
                            j = hops(d, c) if d == 0 else -hops(d, c)
                            if j % nz not in made:
                                make_share(j)
                                made.add(j % nz)
                        rs_step(d, c, g, s)
            if g == 0 and s == 0:
                for j in sorted(range(nz), key=lambda j: -min(j, nz - j)):
                    if j not in made:
                        make_share(j)
                        made.add(j)
        elif g == far:
            if s == 0:
                hid_copy.wait()
            finish(s)
        else:
            ag_step(g - far, s)

    made = set()
    last_stage = 2 * far
    for slot in range(last_stage + 1 + LAG * (SUBS - 1)):
        for s in range(SUBS):
            g = slot - LAG * s
            if 0 <= g <= last_stage:
                stage(g, s)

    o_copy.wait_send()
    for (d, c, h, s) in slots:
        rs_message(d, c, h, s).wait_send()
        ag_message(d, c, h, s).wait_send()
    for i, (j, c, s) in enumerate(d2d):
        here = out_ref.at[pl.ds(out_row(j, s), sub), cols[c]]
        there = out_ref.at[pl.ds(pl.multiple_of((1 - k) * half_rows + chunk_of(j) * rows + s * sub, sub), sub), cols[c]]
        copy = pltpu.make_async_remote_copy(here, there, d2d_send.at[i], d2d_recv.at[i], device_id={"tp": mate}, device_id_type=MESH)
        copy.wait_send()
        copy.wait_recv()


def finish_call(n_tp, attn, w_o, w_mate, hidden, gain):
    n_rows, width = hidden.shape
    depth = w_o.shape[0]
    nz = n_tp // 2
    half_rows, rows = n_rows // 2, n_rows // n_tp
    sub = rows // SUBS
    n_msg = 2 * SUBS * (nz - 1)
    vmem = pl.BlockSpec(memory_space=pltpu.VMEM)
    return pl.pallas_call(
        functools.partial(finish_kernel, n_tp),
        name="finish",
        out_shape=pltpu.VMEM((n_rows, width), jnp.bfloat16) if OUT_VMEM else jax.ShapeDtypeStruct((n_rows, width), jnp.bfloat16),
        in_specs=[vmem, vmem, vmem, pl.BlockSpec(memory_space=pltpu.HBM), vmem],
        out_specs=vmem,
        scratch_shapes=[
            pltpu.VMEM((half_rows, depth), jnp.bfloat16),
            pltpu.VMEM((rows, width), jnp.bfloat16),
            pltpu.VMEM((nz, rows, width), jnp.float32),
            pltpu.VMEM((n_msg, sub, width // 2), jnp.bfloat16),
            pltpu.VMEM((n_msg, sub, width // 2), jnp.bfloat16),
            pltpu.SemaphoreType.DMA,
            pltpu.SemaphoreType.DMA,
            pltpu.SemaphoreType.DMA,
            pltpu.SemaphoreType.DMA((n_msg,)),
            pltpu.SemaphoreType.DMA((n_msg,)),
            pltpu.SemaphoreType.DMA((n_msg,)),
            pltpu.SemaphoreType.DMA((n_msg,)),
            pltpu.SemaphoreType.DMA((2 * SUBS * nz,)),
            pltpu.SemaphoreType.DMA((2 * SUBS * nz,)),
        ],
        compiler_params=pltpu.CompilerParams(collective_id=0, has_side_effects=True, vmem_limit_bytes=40 * 2**20),
    )(attn, w_o, w_mate, hidden, gain)


def solution(mesh):
    def local_step(hidden, w_q, w_k, w_v, w_o, q_norm_w, k_norm_w, post_norm_w, k_cache, v_cache, positions):
        n_tp = mesh.shape["tp"]
        slots, head_dim = k_cache.shape[1], k_cache.shape[3]
        in_hbm = lambda x: pltpu.with_memory_space_constraint(x, pltpu.HBM)
        hidden = in_hbm(hidden)
        q_rot, k_rot, v_local, posb, w_mate = project_call(
            n_tp, hidden, in_hbm(w_q), in_hbm(w_k), in_hbm(w_v), in_hbm(w_o), q_norm_w[None, :], k_norm_w[None, :], positions, slots, head_dim)
        attn, k_new, v_new = attend_call(q_rot, k_rot, v_local, posb, positions, k_cache, v_cache)
        hidden_out = finish_call(n_tp, attn, w_o, w_mate, hidden, post_norm_w[None, :])
        return hidden_out, k_new, v_new

    cache_spec = P('dp', None, 'tp', None)
    return jax.shard_map(local_step, mesh=mesh, in_specs=(P('dp', None), P(None, 'tp'), P(None, 'tp'), P(None, 'tp'), P('tp', None), P('tp'), P('tp'), P(None), cache_spec, cache_spec, P('dp')), out_specs=(P('dp', None), cache_spec, cache_spec), check_vma=False)
```

```python
import functools

import jax
import jax.numpy as jnp
import numpy as np
from jax import lax
from jax.experimental import pallas as pl
from jax.experimental.pallas import tpu as pltpu
from jax.sharding import PartitionSpec as P

NORM_EPS = 1e-6
ROPE_BASE = 500000.0
OUT_VMEM = True


MESH = pl.DeviceIdType.MESH
DEPTH_CUTS = 4
TABLE_ROWS = 128


def rope_table(slots, dim):
    half = dim // 2
    inv_freq = np.float32(ROPE_BASE) ** (np.float32(-2.0) * np.arange(half, dtype=np.float32) / np.float32(dim))
    angles = (np.arange(slots, dtype=np.float32)[:, None] * inv_freq.astype(np.float32)[None, :]).astype(np.float64)
    cos_tab, sin_tab = np.cos(angles), np.sin(angles)
    rest = np.concatenate([cos_tab, cos_tab, -sin_tab, sin_tab], axis=1).astype(np.float32)
    out = np.zeros((TABLE_ROWS, 2 * dim), np.float32)
    for part in range(3):
        high = rest.astype(jnp.bfloat16).astype(np.float32)
        out[part * slots:(part + 1) * slots] = high
        rest = rest - high
    return jnp.asarray(out, dtype=jnp.bfloat16)


def project_kernel(n_tp, slots, dim, pos_hbm, table_hbm, qg_hbm, kg_hbm, hid_ref, wq_ref, wk_ref, wv_ref, wo_ref, kc_ref, vc_ref,
                   q_ref, k_ref, v_ref, posb_ref, wo_in, kc_out, vc_out,
                   pos_ref, table_ref, qg_ref, kg_ref, hid, wqk, wv, acc, vacc, cosb, sinb, e_mine, e_in,
                   in_sem, v_sem, e_send, e_recv, w_sem, s_sem, c_sem):
    t = lax.axis_index("tp")
    mate = t + 1 - 2 * lax.rem(t, 2)
    n_rows, width = hid_ref.shape
    local = wq_ref.shape[1]
    heads = local // dim
    cut = width // DEPTH_CUTS
    barrier = pltpu.get_barrier_semaphore()
    for off in range(1, n_tp):
        pl.semaphore_signal(barrier, inc=1, device_id={"tp": lax.rem(t + off, n_tp)}, device_id_type=MESH)

    loads = []
    for c in range(DEPTH_CUTS):
        at = pl.ds(c * cut, cut)
        loads.append([
            pltpu.make_async_copy(hid_ref.at[:, at], hid.at[c], in_sem.at[c, 0]),
            pltpu.make_async_copy(wq_ref.at[at, :], wqk.at[c, :, pl.ds(0, local)], in_sem.at[c, 1]),
            pltpu.make_async_copy(wk_ref.at[at, :], wqk.at[c, :, pl.ds(local, local)], in_sem.at[c, 2])])
    v_loads = [pltpu.make_async_copy(wv_ref.at[pl.ds(c * cut, cut), :], wv.at[c], v_sem.at[c]) for c in range(DEPTH_CUTS)]
    for group in loads:
        for copy in group:
            copy.start()
    small = [pltpu.make_async_copy(src, dst, s_sem.at[i]) for i, (src, dst) in enumerate(
        ((pos_hbm, pos_ref), (table_hbm, table_ref), (qg_hbm, qg_ref), (kg_hbm, kg_ref)))]
    caches = [pltpu.make_async_copy(src, dst, c_sem.at[i]) for i, (src, dst) in enumerate(((kc_ref, kc_out), (vc_ref, vc_out)))]
    for copy in v_loads + small + caches:
        copy.start()

    w_copy = pltpu.make_async_remote_copy(wo_ref, wo_in, w_sem.at[0], w_sem.at[1], device_id={"tp": mate}, device_id_type=MESH)
    for c in range(DEPTH_CUTS):
        for copy in loads[c]:
            copy.wait()
        part = jnp.dot(hid[c], wqk[c], preferred_element_type=jnp.float32)
        if c == 0:
            acc[...] = part
        else:
            acc[...] += part
        if c == DEPTH_CUTS - 2:
            pl.semaphore_wait(barrier, n_tp - 1)
            w_copy.start()

    lanes = e_mine.shape[1]
    blocks = n_rows // lanes
    ones = jnp.ones((8, local), jnp.bfloat16)
    nt = (((1,), (1,)), ((), ()))
    for i in range(2):
        rounded = acc[:, i * local:(i + 1) * local].astype(jnp.bfloat16).astype(jnp.float32)
        square = rounded * rounded
        high = square.astype(jnp.bfloat16)
        low = (square - high.astype(jnp.float32)).astype(jnp.bfloat16)
        energy = (lax.dot_general(ones, high, nt, preferred_element_type=jnp.float32)
                  + lax.dot_general(ones, low, nt, preferred_element_type=jnp.float32))
        for b in range(blocks):
            e_mine[i * blocks + b:i * blocks + b + 1, :] = energy[0:1, b * lanes:(b + 1) * lanes]
    sends = [pltpu.make_async_remote_copy(
        e_mine, e_in.at[off], e_send.at[off], e_recv.at[off],
        device_id={"tp": lax.rem(t + off, n_tp)}, device_id_type=MESH) for off in range(1, n_tp)]
    for copy in sends:
        copy.start()

    for c in range(DEPTH_CUTS):
        v_loads[c].wait()
        part = jnp.dot(hid[c], wv[c], preferred_element_type=jnp.float32)
        if c == 0:
            vacc[...] = part
        elif c < DEPTH_CUTS - 1:
            vacc[...] += part
        else:
            v_ref[...] = (vacc[...] + part).astype(jnp.bfloat16)
    for copy in small:
        copy.wait()
    lane = lax.broadcasted_iota(jnp.int32, (lanes, TABLE_ROWS), 1)
    which = jnp.where(lane < 3 * slots, lax.rem(lane, slots), -1).astype(jnp.float32)
    for b in range(blocks):
        at = slice(b * lanes, (b + 1) * lanes)
        column = jnp.broadcast_to(pos_ref[b:b + 1, :].astype(jnp.float32), (lanes, lanes)).T
        posb_ref[at, :] = column
        hot = jnp.where(which == column, 1.0, 0.0).astype(jnp.bfloat16)
        factors = jnp.dot(hot, table_ref[...], preferred_element_type=jnp.float32)
        cosb[at, :] = factors[:, :dim]
        sinb[at, :] = factors[:, dim:]

    total = e_mine[...]
    for i, copy in enumerate(sends):
        copy.wait_recv()
        total = total + e_in[i + 1]
    inv = lax.rsqrt(total / width + NORM_EPS)
    for b in range(blocks):
        at = slice(b * lanes, (b + 1) * lanes)
        for i, (gain, out) in enumerate(((qg_ref, q_ref), (kg_ref, k_ref))):
            scale = jnp.broadcast_to(inv[i * blocks + b:i * blocks + b + 1, :], (lanes, lanes)).T
            for h in range(heads):
                cols = slice(h * dim, (h + 1) * dim)
                x = acc[at, i * local + h * dim:i * local + (h + 1) * dim].astype(jnp.bfloat16).astype(jnp.float32)
                x = (x * scale * gain[:, cols]).astype(jnp.bfloat16).astype(jnp.float32)
                out[at, cols] = (x * cosb[at, :] + pltpu.roll(x, dim // 2, 1) * sinb[at, :]).astype(jnp.bfloat16)
    for copy in sends:
        copy.wait_send()
    w_copy.wait()
    for copy in caches:
        copy.wait()


def project_call(n_tp, hidden, w_q, w_k, w_v, w_o, q_gain, k_gain, positions, k_cache, v_cache):
    n_rows, width = hidden.shape
    local = w_q.shape[1]
    slots, dim = k_cache.shape[1], k_cache.shape[3]
    lanes = 128
    flat = (k_cache.size // dim, dim)
    in_hbm = lambda x: pltpu.with_memory_space_constraint(x, pltpu.HBM)
    cut = width // DEPTH_CUTS
    vmem, hbm = pl.BlockSpec(memory_space=pltpu.VMEM), pl.BlockSpec(memory_space=pltpu.HBM)
    return pl.pallas_call(
        functools.partial(project_kernel, n_tp, slots, dim),
        name="project",
        out_shape=[pltpu.VMEM((n_rows, local), jnp.bfloat16)] * 3
        + [pltpu.VMEM((n_rows, lanes), jnp.float32), pltpu.VMEM(w_o.shape, jnp.bfloat16)] + [pltpu.VMEM(flat, jnp.bfloat16)] * 2,
        in_specs=[hbm] * 11,
        out_specs=[vmem] * 7,
        scratch_shapes=[
            pltpu.VMEM((n_rows // lanes, lanes), jnp.int32),
            pltpu.VMEM((TABLE_ROWS, 2 * dim), jnp.bfloat16),
            pltpu.VMEM((1, local), jnp.float32),
            pltpu.VMEM((1, local), jnp.float32),
            pltpu.VMEM((DEPTH_CUTS, n_rows, cut), jnp.bfloat16),
            pltpu.VMEM((DEPTH_CUTS, cut, 2 * local), jnp.bfloat16),
            pltpu.VMEM((DEPTH_CUTS, cut, local), jnp.bfloat16),
            pltpu.VMEM((n_rows, 2 * local), jnp.float32),
            pltpu.VMEM((n_rows, local), jnp.float32),
            pltpu.VMEM((n_rows, dim), jnp.float32),
            pltpu.VMEM((n_rows, dim), jnp.float32),
            pltpu.VMEM((2 * n_rows // lanes, lanes), jnp.float32),
            pltpu.VMEM((n_tp, 2 * n_rows // lanes, lanes), jnp.float32),
            pltpu.SemaphoreType.DMA((DEPTH_CUTS, 3)),
            pltpu.SemaphoreType.DMA((DEPTH_CUTS,)),
            pltpu.SemaphoreType.DMA((n_tp,)),
            pltpu.SemaphoreType.DMA((n_tp,)),
            pltpu.SemaphoreType.DMA((2,)),
            pltpu.SemaphoreType.DMA((4,)),
            pltpu.SemaphoreType.DMA((2,)),
        ],
        compiler_params=pltpu.CompilerParams(collective_id=1, has_side_effects=True, vmem_limit_bytes=32 * 2**20),
        cost_estimate=pl.CostEstimate(flops=6 * n_rows * width * local, bytes_accessed=2 * (n_rows * width + 3 * width * local), transcendentals=0),
    )(*map(in_hbm, (positions.reshape(n_rows // lanes, lanes), rope_table(slots, dim), q_gain, k_gain, hidden, w_q, w_k, w_v, w_o,
                    k_cache.reshape(flat), v_cache.reshape(flat))))


ROW_BLOCK = 128
GROUP = 8


def attend_kernel(slots, heads, pos_ref, q_ref, k_ref, v_ref, posb_ref, kc_ref, vc_ref, o_ref, kn_ref, vn_ref, kf, vf):
    block = q_ref.shape[0]
    dim = q_ref.shape[1] // heads
    lines = slots * heads
    step = pl.program_id(0)
    kf[...] = k_ref[...].astype(jnp.float32)
    vf[...] = v_ref[...].astype(jnp.float32)
    line = lax.broadcasted_iota(jnp.int32, (lines // 2, dim), 0)
    first = lax.rem(line, heads) == 0
    slot_of = [(line // heads + part * (slots // 2)).astype(jnp.float32).astype(jnp.bfloat16) for part in range(2)]

    def insert(r):
        p = jnp.full((lines // 2, dim), pos_ref[step * block + r].astype(jnp.float32)).astype(jnp.bfloat16)
        for src, old, new in ((kf, kc_ref, kn_ref), (vf, vc_ref, vn_ref)):
            h0 = jnp.broadcast_to(src[pl.ds(r, 1), 0:dim], (lines // 2, dim))
            h1 = jnp.broadcast_to(src[pl.ds(r, 1), dim:2 * dim], (lines // 2, dim))
            fresh = jnp.where(first, h0, h1).astype(jnp.bfloat16)
            for part in range(2):
                at = pl.ds(r * lines + part * (lines // 2), lines // 2)
                new[at, :] = jnp.where(slot_of[part] == p, fresh, old[at, :])

    for r in range(block):
        insert(r)

    n_groups = block // GROUP
    wide = GROUP * lines
    m = lax.broadcasted_iota(jnp.int32, (heads * GROUP, wide), 0)
    n = lax.broadcasted_iota(jnp.int32, (heads * GROUP, wide), 1)
    own = (lax.rem(m, GROUP) == n // lines) & (m // GROUP == lax.rem(n, heads))
    slot = jnp.where(own, (lax.rem(n, lines) // heads).astype(jnp.float32), 1e9)
    scores = []
    for g in range(n_groups):
        rows = slice(g * GROUP, (g + 1) * GROUP)
        q = jnp.concatenate([q_ref[rows, h * dim:(h + 1) * dim] for h in range(heads)], axis=0)
        keys = kn_ref[g * wide:(g + 1) * wide, :]
        s = lax.dot_general(q, keys, (((1,), (1,)), ((), ())), preferred_element_type=jnp.float32) * dim ** -0.5
        at = jnp.concatenate([posb_ref[rows, :]] * heads, axis=0)
        at = jnp.concatenate([at] * (wide // at.shape[1]), axis=1)
        scores.append(jnp.where(slot <= at, s, -1e30))
    for g in range(n_groups):
        s = scores[g]
        e = jnp.exp(s - jnp.max(s, axis=-1, keepdims=True))
        probs = (e / jnp.sum(e, axis=-1, keepdims=True)).astype(jnp.bfloat16)
        o = jnp.dot(probs, vn_ref[g * wide:(g + 1) * wide, :], preferred_element_type=jnp.float32).astype(jnp.bfloat16)
        for h in range(heads):
            o_ref[g * GROUP:(g + 1) * GROUP, h * dim:(h + 1) * dim] = o[h * GROUP:(h + 1) * GROUP]


def attend_call(q, k, v, posb, positions, k_cache, v_cache, cache_shape):
    n_rows, slots, heads, dim = cache_shape
    lines = slots * heads
    flat = (n_rows * lines, dim)
    block = ROW_BLOCK
    row_spec = pl.BlockSpec((block, heads * dim), lambda i, pos: (i, 0))
    cache_spec = pl.BlockSpec((block * lines, dim), lambda i, pos: (i, 0))
    o, k_new, v_new = pl.pallas_call(
        functools.partial(attend_kernel, slots, heads),
        name="attend",
        out_shape=[jax.ShapeDtypeStruct((n_rows, heads * dim), jnp.bfloat16),
                   jax.ShapeDtypeStruct(flat, jnp.bfloat16), jax.ShapeDtypeStruct(flat, jnp.bfloat16)],
        grid_spec=pltpu.PrefetchScalarGridSpec(
            num_scalar_prefetch=1,
            grid=(n_rows // block,),
            in_specs=[row_spec, row_spec, row_spec, pl.BlockSpec((block, dim), lambda i, pos: (i, 0)), cache_spec, cache_spec],
            out_specs=[row_spec, cache_spec, cache_spec],
            scratch_shapes=[pltpu.VMEM((block, heads * dim), jnp.float32), pltpu.VMEM((block, heads * dim), jnp.float32)],
        ),
        compiler_params=pltpu.CompilerParams(vmem_limit_bytes=24 * 2**20),
    )(positions, q, k, v, posb, k_cache, v_cache)
    return o, k_new.reshape(cache_shape), v_new.reshape(cache_shape)


SUBS = 2
LAG = 0
SHARE_TILE = 2048


def finish_kernel(n_tp, o_ref, w_ref, w_in, hid_ref, gain_ref, out_ref,
                  o_in, lhs, lhs_in, hid, share, rs_in, rs_out,
                  x_send, x_recv, h_sem, rs_send, rs_recv, ag_send, ag_recv, d2d_send, d2d_recv):
    nz = n_tp // 2
    t = lax.axis_index("tp")
    z, k = t // 2, lax.rem(t, 2)
    up, down, mate = lax.rem(t + 2, n_tp), lax.rem(t + n_tp - 2, n_tp), z * 2 + 1 - k
    n_rows, width = out_ref.shape
    half_rows = n_rows // 2
    rows = half_rows // nz
    sub = rows // SUBS
    half = width // 2
    far = nz // 2
    chunk_of = lambda j: lax.rem(z + nz + j, nz)
    out_row = lambda j, s: pl.multiple_of(k * half_rows + chunk_of(j) * rows + s * sub, sub)
    cols = (pl.ds(0, half), pl.ds(half, half))
    target = (up, down)
    long_half = (0, 1)

    barrier = pltpu.get_barrier_semaphore()
    for peer in (up, down, mate):
        pl.semaphore_signal(barrier, inc=1, device_id={"tp": peer}, device_id_type=MESH)
    hid_copy = pltpu.make_async_copy(hid_ref.at[pl.ds(pl.multiple_of(k * half_rows + z * rows, rows), rows), :], hid, h_sem)
    hid_copy.start()
    pl.semaphore_wait(barrier, 3)

    o_copy = pltpu.make_async_remote_copy(
        o_ref.at[pl.ds(pl.multiple_of((1 - k) * half_rows, half_rows), half_rows), :], o_in,
        x_send, x_recv, device_id={"tp": mate}, device_id_type=MESH)
    o_copy.start()

    order = sorted(range(nz), key=lambda j: -min(j, nz - j))
    place = {j: i for i, j in enumerate(order)}
    for j in range(nz):
        at = slice(place[j] * rows, (place[j] + 1) * rows)
        lhs[at, :] = o_ref[pl.ds(pl.multiple_of(k * half_rows + chunk_of(j) * rows, rows), rows), :]
    o_copy.wait_recv()
    for j in range(nz):
        at = slice(place[j] * rows, (place[j] + 1) * rows)
        lhs_in[at, :] = o_in[pl.ds(pl.multiple_of(chunk_of(j) * rows, rows), rows), :]

    def make_shares(first, last):
        def one(c, carry):
            at = pl.ds(pl.multiple_of(c * SHARE_TILE, SHARE_TILE), SHARE_TILE)
            share[first * rows:last * rows, at] = (
                jnp.dot(lhs[first * rows:last * rows, :], w_ref[:, at], preferred_element_type=jnp.float32)
                + jnp.dot(lhs_in[first * rows:last * rows, :], w_in[:, at], preferred_element_type=jnp.float32))
            return carry

        lax.fori_loop(0, width // SHARE_TILE, one, 0)

    def hops(d, c):
        return far if c == long_half[d] else far - 1

    slots = {}
    for d in range(2):
        for c in range(2):
            for h in range(hops(d, c)):
                for s in range(SUBS):
                    slots[d, c, h, s] = len(slots)

    def rs_message(d, c, h, s):
        i = slots[d, c, h, s]
        return pltpu.make_async_remote_copy(
            rs_out.at[i], rs_in.at[i], rs_send.at[i], rs_recv.at[i], device_id={"tp": target[d]}, device_id_type=MESH)

    def piece(j, c, s):
        return share[place[j % nz] * rows + s * sub:place[j % nz] * rows + (s + 1) * sub, c * half:(c + 1) * half]

    def rs_step(d, c, h, s):
        ahead = hops(d, c) - h
        j = ahead if d == 0 else -ahead
        value = piece(j, c, s)
        if h > 0:
            before = rs_message(d, c, h - 1, s)
            before.wait_recv()
            value = value + rs_in[slots[d, c, h - 1, s]].astype(jnp.float32)
        rs_out[slots[d, c, h, s]] = value.astype(jnp.bfloat16)
        rs_message(d, c, h, s).start()

    def ag_message(d, c, h, s):
        j = -h if d == 0 else h
        here = out_ref.at[pl.ds(out_row(j, s), sub), cols[c]]
        i = slots[d, c, h, s]
        return pltpu.make_async_remote_copy(
            here, here, ag_send.at[i], ag_recv.at[i], device_id={"tp": target[d]}, device_id_type=MESH)

    def ag_arrival(d, c, h, s):
        j = -(h + 1) if d == 0 else h + 1
        here = out_ref.at[pl.ds(out_row(j, s), sub), cols[c]]
        i = slots[d, c, h, s]
        return pltpu.make_async_remote_copy(
            here, here, ag_send.at[i], ag_recv.at[i], device_id={"tp": target[d]}, device_id_type=MESH)

    d2d = []

    def d2d_start(j, c, s):
        here = out_ref.at[pl.ds(out_row(j, s), sub), cols[c]]
        i = len(d2d)
        copy = pltpu.make_async_remote_copy(here, here, d2d_send.at[i], d2d_recv.at[i], device_id={"tp": mate}, device_id_type=MESH)
        copy.start()
        d2d.append((j, c, s))

    def finish(s):
        total = []
        for c in range(2):
            acc = piece(0, c, s)
            for d in range(2):
                last = hops(d, c) - 1
                rs_message(d, c, last, s).wait_recv()
                acc = acc + rs_in[slots[d, c, last, s]].astype(jnp.float32)
            share[place[0] * rows + s * sub:place[0] * rows + (s + 1) * sub, c * half:(c + 1) * half] = acc
            total.append(jnp.sum(acc * acc, axis=-1, keepdims=True))
        inv = lax.rsqrt((total[0] + total[1]) / width + NORM_EPS)
        for c in range(2):
            at = slice(c * half, (c + 1) * half)
            normed = piece(0, c, s) * inv * gain_ref[:, at]
            out_ref[pl.ds(out_row(0, s), sub), at] = (hid[s * sub:(s + 1) * sub, at].astype(jnp.float32) + normed).astype(jnp.bfloat16)
        for d in range(2):
            for c in (long_half[d], 1 - long_half[d]):
                ag_message(d, c, 0, s).start()
        for c in range(2):
            d2d_start(0, c, s)

    def ag_step(h, s):
        for c in range(2):
            for d in range(2):
                if h - 1 < hops(d, c):
                    ag_arrival(d, c, h - 1, s).wait_recv()
                    if h < hops(d, c):
                        ag_message(d, c, h, s).start()
                    d2d_start(-h if d == 0 else h, c, s)

    def stage(g, s):
        if g < far:
            for longer in (True, False):
                for d in range(2):
                    c = long_half[d] if longer else 1 - long_half[d]
                    if g < hops(d, c):
                        rs_step(d, c, g, s)
        elif g == far:
            if s == 0:
                hid_copy.wait()
            finish(s)
        else:
            ag_step(g - far, s)

    make_shares(0, 3)
    last_stage = 2 * far
    for slot in range(last_stage + 1 + LAG * (SUBS - 1)):
        if slot == 1:
            make_shares(3, nz)
        for s in range(SUBS):
            g = slot - LAG * s
            if 0 <= g <= last_stage:
                stage(g, s)

    o_copy.wait_send()
    for (d, c, h, s) in slots:
        rs_message(d, c, h, s).wait_send()
        ag_message(d, c, h, s).wait_send()
    for i, (j, c, s) in enumerate(d2d):
        here = out_ref.at[pl.ds(out_row(j, s), sub), cols[c]]
        there = out_ref.at[pl.ds(pl.multiple_of((1 - k) * half_rows + chunk_of(j) * rows + s * sub, sub), sub), cols[c]]
        copy = pltpu.make_async_remote_copy(here, there, d2d_send.at[i], d2d_recv.at[i], device_id={"tp": mate}, device_id_type=MESH)
        copy.wait_send()
        copy.wait_recv()


def finish_call(n_tp, attn, w_o, w_mate, hidden, gain):
    n_rows, width = hidden.shape
    depth = w_o.shape[0]
    nz = n_tp // 2
    half_rows, rows = n_rows // 2, n_rows // n_tp
    sub = rows // SUBS
    n_msg = 2 * SUBS * (nz - 1)
    vmem = pl.BlockSpec(memory_space=pltpu.VMEM)
    return pl.pallas_call(
        functools.partial(finish_kernel, n_tp),
        name="finish",
        out_shape=pltpu.VMEM((n_rows, width), jnp.bfloat16) if OUT_VMEM else jax.ShapeDtypeStruct((n_rows, width), jnp.bfloat16),
        in_specs=[vmem, vmem, vmem, pl.BlockSpec(memory_space=pltpu.HBM), vmem],
        out_specs=vmem,
        scratch_shapes=[
            pltpu.VMEM((half_rows, depth), jnp.bfloat16),
            pltpu.VMEM((half_rows, depth), jnp.bfloat16),
            pltpu.VMEM((half_rows, depth), jnp.bfloat16),
            pltpu.VMEM((rows, width), jnp.bfloat16),
            pltpu.VMEM((half_rows, width), jnp.float32),
            pltpu.VMEM((n_msg, sub, width // 2), jnp.bfloat16),
            pltpu.VMEM((n_msg, sub, width // 2), jnp.bfloat16),
            pltpu.SemaphoreType.DMA,
            pltpu.SemaphoreType.DMA,
            pltpu.SemaphoreType.DMA,
            pltpu.SemaphoreType.DMA((n_msg,)),
            pltpu.SemaphoreType.DMA((n_msg,)),
            pltpu.SemaphoreType.DMA((n_msg,)),
            pltpu.SemaphoreType.DMA((n_msg,)),
            pltpu.SemaphoreType.DMA((2 * SUBS * nz,)),
            pltpu.SemaphoreType.DMA((2 * SUBS * nz,)),
        ],
        compiler_params=pltpu.CompilerParams(collective_id=0, has_side_effects=True, vmem_limit_bytes=40 * 2**20),
    )(attn, w_o, w_mate, pltpu.with_memory_space_constraint(hidden, pltpu.HBM), gain)


def solution(mesh):
    def local_step(hidden, w_q, w_k, w_v, w_o, q_norm_w, k_norm_w, post_norm_w, k_cache, v_cache, positions):
        n_tp = mesh.shape["tp"]
        q_rot, k_rot, v_local, posb, w_mate, k_near, v_near = project_call(
            n_tp, hidden, w_q, w_k, w_v, w_o, q_norm_w[None, :], k_norm_w[None, :], positions, k_cache, v_cache)
        attn, k_new, v_new = attend_call(q_rot, k_rot, v_local, posb, positions, k_near, v_near, k_cache.shape)
        hidden_out = finish_call(n_tp, attn, w_o, w_mate, hidden, post_norm_w[None, :])
        return hidden_out, k_new, v_new

    cache_spec = P('dp', None, 'tp', None)
    return jax.shard_map(local_step, mesh=mesh, in_specs=(P('dp', None), P(None, 'tp'), P(None, 'tp'), P(None, 'tp'), P('tp', None), P('tp'), P('tp'), P(None), cache_spec, cache_spec, P('dp')), out_specs=(P('dp', None), cache_spec, cache_spec), check_vma=False)
```

```python
import functools

import jax
import jax.numpy as jnp
import numpy as np
from jax import lax
from jax.experimental import pallas as pl
from jax.experimental.pallas import tpu as pltpu
from jax.sharding import PartitionSpec as P

NORM_EPS = 1e-6
ROPE_BASE = 500000.0
OUT_VMEM = True


MESH = pl.DeviceIdType.MESH
DEPTH_CUTS = 4
TABLE_ROWS = 128


def rope_table(slots, dim):
    half = dim // 2
    inv_freq = np.float32(ROPE_BASE) ** (np.float32(-2.0) * np.arange(half, dtype=np.float32) / np.float32(dim))
    angles = (np.arange(slots, dtype=np.float32)[:, None] * inv_freq.astype(np.float32)[None, :]).astype(np.float64)
    cos_tab, sin_tab = np.cos(angles), np.sin(angles)
    rest = np.concatenate([cos_tab, cos_tab, -sin_tab, sin_tab], axis=1).astype(np.float32)
    out = np.zeros((TABLE_ROWS, 2 * dim), np.float32)
    for part in range(3):
        high = rest.astype(jnp.bfloat16).astype(np.float32)
        out[part * slots:(part + 1) * slots] = high
        rest = rest - high
    return jnp.asarray(out, dtype=jnp.bfloat16)


def inserter(slots, heads, dim):
    assert heads == 2
    part_lines = slots * heads // 2
    line = lax.broadcasted_iota(jnp.int32, (part_lines, dim), 0)
    first = lax.rem(line, heads) == 0
    slot_of = [(line // heads + part * (slots // 2)).astype(jnp.float32).astype(jnp.bfloat16) for part in range(2)]

    def insert(posb_ref, fresh_ref, start, count, old, new):
        spots = [pl.ds(pl.multiple_of((start + r) * 2 * part_lines, 2 * part_lines) + part * part_lines, part_lines)
                 for r in range(count) for part in range(2)]
        before = [old[at, :] for at in spots]
        for r in range(count):
            row = pl.ds(start + r, 1)
            p = jnp.broadcast_to(posb_ref[row, :], (part_lines, dim)).astype(jnp.bfloat16)
            h0 = jnp.broadcast_to(fresh_ref[0, row, :], (part_lines, dim))
            h1 = jnp.broadcast_to(fresh_ref[1, row, :], (part_lines, dim))
            fresh = jnp.where(first, h0, h1).astype(jnp.bfloat16)
            for part in range(2):
                new[spots[2 * r + part], :] = jnp.where(slot_of[part] == p, fresh, before[2 * r + part])

    return insert


def project_kernel(n_tp, slots, dim, pos_hbm, table_hbm, qg_hbm, kg_hbm, hid_ref, wq_ref, wk_ref, wv_ref, wo_ref, kc_ref, vc_ref,
                   q_ref, k_ref, posb_ref, wo_own, wo_in, kc_out, vc_out,
                   pos_ref, table_ref, qg_ref, kg_ref, hid, wqk, wv, vc_in, acc, vacc, cosb, sinb, e_mine, e_in,
                   in_sem, v_sem, e_send, e_recv, w_sem, s_sem, c_sem):
    t = lax.axis_index("tp")
    mate = t + 1 - 2 * lax.rem(t, 2)
    n_rows, width = hid_ref.shape
    local = wq_ref.shape[1]
    heads = local // dim
    cut = width // DEPTH_CUTS
    barrier = pltpu.get_barrier_semaphore()
    for off in range(1, n_tp):
        pl.semaphore_signal(barrier, inc=1, device_id={"tp": lax.rem(t + off, n_tp)}, device_id_type=MESH)

    loads = []
    for c in range(DEPTH_CUTS):
        at = pl.ds(c * cut, cut)
        loads.append([
            pltpu.make_async_copy(hid_ref.at[:, at], hid.at[c], in_sem.at[c, 0]),
            pltpu.make_async_copy(wq_ref.at[at, :], wqk.at[c, :, pl.ds(0, local)], in_sem.at[c, 1]),
            pltpu.make_async_copy(wk_ref.at[at, :], wqk.at[c, :, pl.ds(local, local)], in_sem.at[c, 2])])
    v_loads = [pltpu.make_async_copy(wv_ref.at[pl.ds(c * cut, cut), :], wv.at[c], v_sem.at[c]) for c in range(DEPTH_CUTS)]
    for group in loads:
        for copy in group:
            copy.start()
    small = [pltpu.make_async_copy(src, dst, s_sem.at[i]) for i, (src, dst) in enumerate(
        ((pos_hbm, pos_ref), (table_hbm, table_ref), (qg_hbm, qg_ref), (kg_hbm, kg_ref)))]
    caches = [pltpu.make_async_copy(src, dst, c_sem.at[i]) for i, (src, dst) in enumerate(((kc_ref, kc_out), (vc_ref, vc_in), (wo_ref, wo_own)))]
    for copy in v_loads + small + [caches[2], caches[1], caches[0]]:
        copy.start()

    w_copy = pltpu.make_async_remote_copy(wo_own, wo_in, w_sem.at[0], w_sem.at[1], device_id={"tp": mate}, device_id_type=MESH)
    for c in range(DEPTH_CUTS):
        for copy in loads[c]:
            copy.wait()
        part = jnp.dot(hid[c], wqk[c], preferred_element_type=jnp.float32)
        if c == 0:
            acc[...] = part
        else:
            acc[...] += part

    lanes = e_mine.shape[1]
    blocks = n_rows // lanes
    ones = jnp.ones((8, local), jnp.bfloat16)
    nt = (((1,), (1,)), ((), ()))
    for i in range(2):
        rounded = acc[:, i * local:(i + 1) * local].astype(jnp.bfloat16).astype(jnp.float32)
        square = rounded * rounded
        high = square.astype(jnp.bfloat16)
        low = (square - high.astype(jnp.float32)).astype(jnp.bfloat16)
        energy = (lax.dot_general(ones, high, nt, preferred_element_type=jnp.float32)
                  + lax.dot_general(ones, low, nt, preferred_element_type=jnp.float32))
        for b in range(blocks):
            e_mine[i * blocks + b:i * blocks + b + 1, :] = energy[0:1, b * lanes:(b + 1) * lanes]
    pl.semaphore_wait(barrier, n_tp - 1)
    sends = [pltpu.make_async_remote_copy(
        e_mine, e_in.at[off], e_send.at[off], e_recv.at[off],
        device_id={"tp": lax.rem(t + off, n_tp)}, device_id_type=MESH) for off in range(1, n_tp)]
    for copy in sends:
        copy.start()
    caches[2].wait()
    w_copy.start()

    for c in range(DEPTH_CUTS):
        v_loads[c].wait()
        part = jnp.dot(hid[c], wv[c], preferred_element_type=jnp.float32)
        for h in range(heads):
            if c == 0:
                vacc[h] = part[:, h * dim:(h + 1) * dim]
            else:
                vacc[h] += part[:, h * dim:(h + 1) * dim]
    for copy in small:
        copy.wait()
    lane = lax.broadcasted_iota(jnp.int32, (lanes, TABLE_ROWS), 1)
    which = jnp.where(lane < 3 * slots, lax.rem(lane, slots), -1).astype(jnp.float32)
    for b in range(blocks):
        at = slice(b * lanes, (b + 1) * lanes)
        column = jnp.broadcast_to(pos_ref[b:b + 1, :].astype(jnp.float32), (lanes, lanes)).T
        posb_ref[at, :] = column
        hot = jnp.where(which == column, 1.0, 0.0).astype(jnp.bfloat16)
        factors = jnp.dot(hot, table_ref[...], preferred_element_type=jnp.float32)
        cosb[at, :] = factors[:, :dim]
        sinb[at, :] = factors[:, dim:]
    caches[1].wait()
    insert = inserter(slots, heads, dim)

    def insert_rows(i, carry):
        insert(posb_ref, vacc, i * INSERT_UNROLL, INSERT_UNROLL, vc_in, vc_out)
        return carry

    lax.fori_loop(0, n_rows // INSERT_UNROLL, insert_rows, 0)

    total = e_mine[...]
    for i, copy in enumerate(sends):
        copy.wait_recv()
        total = total + e_in[i + 1]
    inv = lax.rsqrt(total / width + NORM_EPS)
    for b in range(blocks):
        at = slice(b * lanes, (b + 1) * lanes)
        for i, (gain, out) in enumerate(((qg_ref, q_ref), (kg_ref, k_ref))):
            scale = jnp.broadcast_to(inv[i * blocks + b:i * blocks + b + 1, :], (lanes, lanes)).T
            for h in range(heads):
                cols = slice(h * dim, (h + 1) * dim)
                x = acc[at, i * local + h * dim:i * local + (h + 1) * dim].astype(jnp.bfloat16).astype(jnp.float32)
                x = (x * scale * gain[:, cols]).astype(jnp.bfloat16).astype(jnp.float32)
                x = (x * cosb[at, :] + pltpu.roll(x, dim // 2, 1) * sinb[at, :]).astype(jnp.bfloat16)
                if i == 0:
                    out[at, cols] = x
                else:
                    out[h, at, :] = x.astype(jnp.float32)
    for copy in sends:
        copy.wait_send()
    w_copy.wait()
    caches[0].wait()


def project_call(n_tp, hidden, w_q, w_k, w_v, w_o, q_gain, k_gain, positions, k_cache, v_cache):
    n_rows, width = hidden.shape
    local = w_q.shape[1]
    slots, dim = k_cache.shape[1], k_cache.shape[3]
    lanes = 128
    flat = (k_cache.size // dim, dim)
    in_hbm = lambda x: pltpu.with_memory_space_constraint(x, pltpu.HBM)
    cut = width // DEPTH_CUTS
    vmem, hbm = pl.BlockSpec(memory_space=pltpu.VMEM), pl.BlockSpec(memory_space=pltpu.HBM)
    return pl.pallas_call(
        functools.partial(project_kernel, n_tp, slots, dim),
        name="project",
        out_shape=[pltpu.VMEM((n_rows, local), jnp.bfloat16), pltpu.VMEM((local // dim, n_rows, dim), jnp.float32)]
        + [pltpu.VMEM((n_rows, lanes), jnp.float32), pltpu.VMEM(w_o.shape, jnp.bfloat16), pltpu.VMEM(w_o.shape, jnp.bfloat16)] + [pltpu.VMEM(flat, jnp.bfloat16)] * 2,
        in_specs=[hbm] * 11,
        out_specs=[vmem] * 7,
        scratch_shapes=[
            pltpu.VMEM((n_rows // lanes, lanes), jnp.int32),
            pltpu.VMEM((TABLE_ROWS, 2 * dim), jnp.bfloat16),
            pltpu.VMEM((1, local), jnp.float32),
            pltpu.VMEM((1, local), jnp.float32),
            pltpu.VMEM((DEPTH_CUTS, n_rows, cut), jnp.bfloat16),
            pltpu.VMEM((DEPTH_CUTS, cut, 2 * local), jnp.bfloat16),
            pltpu.VMEM((DEPTH_CUTS, cut, local), jnp.bfloat16),
            pltpu.VMEM(flat, jnp.bfloat16),
            pltpu.VMEM((n_rows, 2 * local), jnp.float32),
            pltpu.VMEM((local // dim, n_rows, dim), jnp.float32),
            pltpu.VMEM((n_rows, dim), jnp.float32),
            pltpu.VMEM((n_rows, dim), jnp.float32),
            pltpu.VMEM((2 * n_rows // lanes, lanes), jnp.float32),
            pltpu.VMEM((n_tp, 2 * n_rows // lanes, lanes), jnp.float32),
            pltpu.SemaphoreType.DMA((DEPTH_CUTS, 3)),
            pltpu.SemaphoreType.DMA((DEPTH_CUTS,)),
            pltpu.SemaphoreType.DMA((n_tp,)),
            pltpu.SemaphoreType.DMA((n_tp,)),
            pltpu.SemaphoreType.DMA((2,)),
            pltpu.SemaphoreType.DMA((4,)),
            pltpu.SemaphoreType.DMA((3,)),
        ],
        compiler_params=pltpu.CompilerParams(collective_id=1, has_side_effects=True, vmem_limit_bytes=40 * 2**20),
        cost_estimate=pl.CostEstimate(flops=6 * n_rows * width * local, bytes_accessed=2 * (n_rows * width + 3 * width * local), transcendentals=0),
    )(*map(in_hbm, (positions.reshape(n_rows // lanes, lanes), rope_table(slots, dim), q_gain, k_gain, hidden, w_q, w_k, w_v, w_o,
                    k_cache.reshape(flat), v_cache.reshape(flat))))


ROW_BLOCK = 256
INSERT_UNROLL = 16
GROUP = 8


def attend_kernel(slots, heads, q_ref, k_ref, posb_ref, kc_ref, vn_ref, o_ref, k_out, v_out, kn, k_sem, v_sem):
    n_rows = q_ref.shape[0]
    dim = q_ref.shape[1] // heads
    lines = slots * heads
    block = ROW_BLOCK
    v_copy = pltpu.make_async_copy(vn_ref, v_out, v_sem)
    v_copy.start()
    insert = inserter(slots, heads, dim)
    n_groups = block // GROUP
    wide = GROUP * lines
    m = lax.broadcasted_iota(jnp.int32, (heads * GROUP, wide), 0)
    n = lax.broadcasted_iota(jnp.int32, (heads * GROUP, wide), 1)
    own = (lax.rem(m, GROUP) == n // lines) & (m // GROUP == lax.rem(n, heads))
    slot = jnp.where(own, (lax.rem(n, lines) // heads).astype(jnp.float32), 1e9)

    def k_copy(i):
        at = pl.ds(pl.multiple_of(i * block * lines, block * lines), block * lines)
        return pltpu.make_async_copy(kn.at[at, :], k_out.at[at, :], k_sem.at[i])

    def fill(i, carry):
        for r in range(0, block, INSERT_UNROLL):
            insert(posb_ref, k_ref, i * block + r, INSERT_UNROLL, kc_ref, kn)
        k_copy(i).start()
        return carry

    lax.fori_loop(0, n_rows // block, fill, 0)

    def one(i, carry):
        scores = []
        for g in range(n_groups):
            rows = pl.ds(pl.multiple_of(i * block + g * GROUP, GROUP), GROUP)
            keys = kn[pl.ds(pl.multiple_of((i * n_groups + g) * wide, wide), wide), :]
            q = jnp.concatenate([q_ref[rows, h * dim:(h + 1) * dim] for h in range(heads)], axis=0)
            s = lax.dot_general(q, keys, (((1,), (1,)), ((), ())), preferred_element_type=jnp.float32) * dim ** -0.5
            at = jnp.concatenate([posb_ref[rows, :]] * heads, axis=0)
            at = jnp.concatenate([at] * (wide // at.shape[1]), axis=1)
            scores.append(jnp.where(slot <= at, s, -1e30))
        for g in range(n_groups):
            rows = pl.ds(pl.multiple_of(i * block + g * GROUP, GROUP), GROUP)
            values = vn_ref[pl.ds(pl.multiple_of((i * n_groups + g) * wide, wide), wide), :]
            s = scores[g]
            e = jnp.exp(s - jnp.max(s, axis=-1, keepdims=True))
            probs = (e / jnp.sum(e, axis=-1, keepdims=True)).astype(jnp.bfloat16)
            o = jnp.dot(probs, values, preferred_element_type=jnp.float32).astype(jnp.bfloat16)
            for h in range(heads):
                o_ref[rows, h * dim:(h + 1) * dim] = o[h * GROUP:(h + 1) * GROUP]
        return carry

    lax.fori_loop(0, n_rows // block, one, 0)
    for i in range(n_rows // block):
        k_copy(i).wait()
    v_copy.wait()


def attend_call(q, k, posb, k_cache, v_new, cache_shape):
    n_rows, slots, heads, dim = cache_shape
    flat = (n_rows * slots * heads, dim)
    vmem, hbm = pl.BlockSpec(memory_space=pltpu.VMEM), pl.BlockSpec(memory_space=pltpu.HBM)
    o, k_out, v_out = pl.pallas_call(
        functools.partial(attend_kernel, slots, heads),
        name="attend",
        out_shape=[pltpu.VMEM((n_rows, heads * dim), jnp.bfloat16),
                   pltpu.HBM(flat, jnp.bfloat16), pltpu.HBM(flat, jnp.bfloat16)],
        in_specs=[vmem] * 5,
        out_specs=[vmem, hbm, hbm],
        scratch_shapes=[pltpu.VMEM(flat, jnp.bfloat16), pltpu.SemaphoreType.DMA((n_rows // ROW_BLOCK,)), pltpu.SemaphoreType.DMA],
        compiler_params=pltpu.CompilerParams(vmem_limit_bytes=24 * 2**20),
    )(q, k, posb, k_cache, v_new)
    return o, k_out.reshape(cache_shape), v_out.reshape(cache_shape)


SUBS = 2
LAG = 0
SHARE_TILE = 2048


def finish_kernel(n_tp, o_ref, w_ref, w_in, hid_ref, gain_ref, out_ref,
                  o_in, lhs, lhs_in, hid, share, rs_in, rs_out,
                  x_send, x_recv, h_sem, rs_send, rs_recv, ag_send, ag_recv, d2d_send, d2d_recv):
    nz = n_tp // 2
    t = lax.axis_index("tp")
    z, k = t // 2, lax.rem(t, 2)
    up, down, mate = lax.rem(t + 2, n_tp), lax.rem(t + n_tp - 2, n_tp), z * 2 + 1 - k
    n_rows, width = out_ref.shape
    half_rows = n_rows // 2
    rows = half_rows // nz
    sub = rows // SUBS
    half = width // 2
    far = nz // 2
    chunk_of = lambda j: lax.rem(z + nz + j, nz)
    out_row = lambda j, s: pl.multiple_of(k * half_rows + chunk_of(j) * rows + s * sub, sub)
    cols = (pl.ds(0, half), pl.ds(half, half))
    target = (up, down)
    long_half = (0, 1)

    barrier = pltpu.get_barrier_semaphore()
    for peer in (up, down, mate):
        pl.semaphore_signal(barrier, inc=1, device_id={"tp": peer}, device_id_type=MESH)
    hid_copy = pltpu.make_async_copy(hid_ref.at[pl.ds(pl.multiple_of(k * half_rows + z * rows, rows), rows), :], hid, h_sem)
    hid_copy.start()
    pl.semaphore_wait(barrier, 3)

    o_copy = pltpu.make_async_remote_copy(
        o_ref.at[pl.ds(pl.multiple_of((1 - k) * half_rows, half_rows), half_rows), :], o_in,
        x_send, x_recv, device_id={"tp": mate}, device_id_type=MESH)
    o_copy.start()

    order = sorted(range(nz), key=lambda j: -min(j, nz - j))
    place = {j: i for i, j in enumerate(order)}
    for j in range(nz):
        at = slice(place[j] * rows, (place[j] + 1) * rows)
        lhs[at, :] = o_ref[pl.ds(pl.multiple_of(k * half_rows + chunk_of(j) * rows, rows), rows), :]

    def add_shares(first, last, lhs_ref, weight, fresh):
        def one(c, carry):
            at = pl.ds(pl.multiple_of(c * SHARE_TILE, SHARE_TILE), SHARE_TILE)
            part = jnp.dot(lhs_ref[first * rows:last * rows, :], weight[:, at], preferred_element_type=jnp.float32)
            if fresh:
                share[first * rows:last * rows, at] = part
            else:
                share[first * rows:last * rows, at] += part
            return carry

        lax.fori_loop(0, width // SHARE_TILE, one, 0)

    add_shares(0, nz, lhs, w_ref, True)
    o_copy.wait_recv()
    for j in range(nz):
        at = slice(place[j] * rows, (place[j] + 1) * rows)
        lhs_in[at, :] = o_in[pl.ds(pl.multiple_of(chunk_of(j) * rows, rows), rows), :]

    def hops(d, c):
        return far if c == long_half[d] else far - 1

    slots = {}
    for d in range(2):
        for c in range(2):
            for h in range(hops(d, c)):
                for s in range(SUBS):
                    slots[d, c, h, s] = len(slots)

    def rs_message(d, c, h, s):
        i = slots[d, c, h, s]
        return pltpu.make_async_remote_copy(
            rs_out.at[i], rs_in.at[i], rs_send.at[i], rs_recv.at[i], device_id={"tp": target[d]}, device_id_type=MESH)

    def piece(j, c, s):
        return share[place[j % nz] * rows + s * sub:place[j % nz] * rows + (s + 1) * sub, c * half:(c + 1) * half]

    def rs_step(d, c, h, s):
        ahead = hops(d, c) - h
        j = ahead if d == 0 else -ahead
        value = piece(j, c, s)
        if h > 0:
            before = rs_message(d, c, h - 1, s)
            before.wait_recv()
            value = value + rs_in[slots[d, c, h - 1, s]].astype(jnp.float32)
        rs_out[slots[d, c, h, s]] = value.astype(jnp.bfloat16)
        rs_message(d, c, h, s).start()

    def ag_message(d, c, h, s):
        j = -h if d == 0 else h
        here = out_ref.at[pl.ds(out_row(j, s), sub), cols[c]]
        i = slots[d, c, h, s]
        return pltpu.make_async_remote_copy(
            here, here, ag_send.at[i], ag_recv.at[i], device_id={"tp": target[d]}, device_id_type=MESH)

    def ag_arrival(d, c, h, s):
        j = -(h + 1) if d == 0 else h + 1
        here = out_ref.at[pl.ds(out_row(j, s), sub), cols[c]]
        i = slots[d, c, h, s]
        return pltpu.make_async_remote_copy(
            here, here, ag_send.at[i], ag_recv.at[i], device_id={"tp": target[d]}, device_id_type=MESH)

    d2d = []

    def d2d_start(j, c, s):
        here = out_ref.at[pl.ds(out_row(j, s), sub), cols[c]]
        i = len(d2d)
        copy = pltpu.make_async_remote_copy(here, here, d2d_send.at[i], d2d_recv.at[i], device_id={"tp": mate}, device_id_type=MESH)
        copy.start()
        d2d.append((j, c, s))

    def finish(s):
        total = []
        for c in range(2):
            acc = piece(0, c, s)
            for d in range(2):
                last = hops(d, c) - 1
                rs_message(d, c, last, s).wait_recv()
                acc = acc + rs_in[slots[d, c, last, s]].astype(jnp.float32)
            share[place[0] * rows + s * sub:place[0] * rows + (s + 1) * sub, c * half:(c + 1) * half] = acc
            total.append(jnp.sum(acc * acc, axis=-1, keepdims=True))
        inv = lax.rsqrt((total[0] + total[1]) / width + NORM_EPS)
        for c in range(2):
            at = slice(c * half, (c + 1) * half)
            normed = piece(0, c, s) * inv * gain_ref[:, at]
            out_ref[pl.ds(out_row(0, s), sub), at] = (hid[s * sub:(s + 1) * sub, at].astype(jnp.float32) + normed).astype(jnp.bfloat16)
        for d in range(2):
            for c in (long_half[d], 1 - long_half[d]):
                ag_message(d, c, 0, s).start()
        for c in range(2):
            d2d_start(0, c, s)

    def ag_step(h, s):
        for c in range(2):
            for d in range(2):
                if h - 1 < hops(d, c):
                    ag_arrival(d, c, h - 1, s).wait_recv()
                    if h < hops(d, c):
                        ag_message(d, c, h, s).start()
                    d2d_start(-h if d == 0 else h, c, s)

    def stage(g, s):
        if g < far:
            for longer in (True, False):
                for d in range(2):
                    c = long_half[d] if longer else 1 - long_half[d]
                    if g < hops(d, c):
                        rs_step(d, c, g, s)
        elif g == far:
            if s == 0:
                hid_copy.wait()
            finish(s)
        else:
            ag_step(g - far, s)

    add_shares(0, 3, lhs_in, w_in, False)
    last_stage = 2 * far
    for slot in range(last_stage + 1 + LAG * (SUBS - 1)):
        if slot == 1:
            add_shares(3, nz, lhs_in, w_in, False)
        for s in range(SUBS):
            g = slot - LAG * s
            if 0 <= g <= last_stage:
                stage(g, s)

    o_copy.wait_send()
    for (d, c, h, s) in slots:
        rs_message(d, c, h, s).wait_send()
        ag_message(d, c, h, s).wait_send()
    for i, (j, c, s) in enumerate(d2d):
        here = out_ref.at[pl.ds(out_row(j, s), sub), cols[c]]
        there = out_ref.at[pl.ds(pl.multiple_of((1 - k) * half_rows + chunk_of(j) * rows + s * sub, sub), sub), cols[c]]
        copy = pltpu.make_async_remote_copy(here, there, d2d_send.at[i], d2d_recv.at[i], device_id={"tp": mate}, device_id_type=MESH)
        copy.wait_send()
        copy.wait_recv()


def finish_call(n_tp, attn, w_own, w_mate, hidden, gain):
    n_rows, width = hidden.shape
    depth = w_own.shape[0]
    nz = n_tp // 2
    half_rows, rows = n_rows // 2, n_rows // n_tp
    sub = rows // SUBS
    n_msg = 2 * SUBS * (nz - 1)
    vmem = pl.BlockSpec(memory_space=pltpu.VMEM)
    return pl.pallas_call(
        functools.partial(finish_kernel, n_tp),
        name="finish",
        out_shape=pltpu.VMEM((n_rows, width), jnp.bfloat16) if OUT_VMEM else jax.ShapeDtypeStruct((n_rows, width), jnp.bfloat16),
        in_specs=[vmem, vmem, vmem, pl.BlockSpec(memory_space=pltpu.HBM), vmem],
        out_specs=vmem,
        scratch_shapes=[
            pltpu.VMEM((half_rows, depth), jnp.bfloat16),
            pltpu.VMEM((half_rows, depth), jnp.bfloat16),
            pltpu.VMEM((half_rows, depth), jnp.bfloat16),
            pltpu.VMEM((rows, width), jnp.bfloat16),
            pltpu.VMEM((half_rows, width), jnp.float32),
            pltpu.VMEM((n_msg, sub, width // 2), jnp.bfloat16),
            pltpu.VMEM((n_msg, sub, width // 2), jnp.bfloat16),
            pltpu.SemaphoreType.DMA,
            pltpu.SemaphoreType.DMA,
            pltpu.SemaphoreType.DMA,
            pltpu.SemaphoreType.DMA((n_msg,)),
            pltpu.SemaphoreType.DMA((n_msg,)),
            pltpu.SemaphoreType.DMA((n_msg,)),
            pltpu.SemaphoreType.DMA((n_msg,)),
            pltpu.SemaphoreType.DMA((2 * SUBS * nz,)),
            pltpu.SemaphoreType.DMA((2 * SUBS * nz,)),
        ],
        compiler_params=pltpu.CompilerParams(collective_id=0, has_side_effects=True, vmem_limit_bytes=40 * 2**20),
    )(attn, w_own, w_mate, pltpu.with_memory_space_constraint(hidden, pltpu.HBM), gain)


def solution(mesh):
    def local_step(hidden, w_q, w_k, w_v, w_o, q_norm_w, k_norm_w, post_norm_w, k_cache, v_cache, positions):
        n_tp = mesh.shape["tp"]
        q_rot, k_rot, posb, w_own, w_mate, k_near, v_near = project_call(
            n_tp, hidden, w_q, w_k, w_v, w_o, q_norm_w[None, :], k_norm_w[None, :], positions, k_cache, v_cache)
        attn, k_new, v_new = attend_call(q_rot, k_rot, posb, k_near, v_near, k_cache.shape)
        hidden_out = finish_call(n_tp, attn, w_own, w_mate, hidden, post_norm_w[None, :])
        return hidden_out, k_new, v_new

    cache_spec = P('dp', None, 'tp', None)
    return jax.shard_map(local_step, mesh=mesh, in_specs=(P('dp', None), P(None, 'tp'), P(None, 'tp'), P(None, 'tp'), P('tp', None), P('tp'), P('tp'), P(None), cache_spec, cache_spec, P('dp')), out_specs=(P('dp', None), cache_spec, cache_spec), check_vma=False)
```

```python
import functools

import jax
import jax.numpy as jnp
import numpy as np
from jax import lax
from jax.experimental import pallas as pl
from jax.experimental.pallas import tpu as pltpu
from jax.sharding import PartitionSpec as P

NORM_EPS = 1e-6
ROPE_BASE = 500000.0
OUT_VMEM = True


MESH = pl.DeviceIdType.MESH
DEPTH_CUTS = 4
IN_FLIGHT = 3
TABLE_ROWS = 128


def rope_table(slots, dim):
    half = dim // 2
    inv_freq = np.float32(ROPE_BASE) ** (np.float32(-2.0) * np.arange(half, dtype=np.float32) / np.float32(dim))
    angles = (np.arange(slots, dtype=np.float32)[:, None] * inv_freq.astype(np.float32)[None, :]).astype(np.float64)
    cos_tab, sin_tab = np.cos(angles), np.sin(angles)
    rest = np.concatenate([cos_tab, cos_tab, -sin_tab, sin_tab], axis=1).astype(np.float32)
    out = np.zeros((TABLE_ROWS, 2 * dim), np.float32)
    for part in range(3):
        high = rest.astype(jnp.bfloat16).astype(np.float32)
        out[part * slots:(part + 1) * slots] = high
        rest = rest - high
    return jnp.asarray(out, dtype=jnp.bfloat16)


def inserter(slots, heads, dim):
    assert heads == 2
    part_lines = slots * heads // 2
    line = lax.broadcasted_iota(jnp.int32, (part_lines, dim), 0)
    first = lax.rem(line, heads) == 0
    slot_of = [(line // heads + part * (slots // 2)).astype(jnp.float32).astype(jnp.bfloat16) for part in range(2)]

    def insert(posb_ref, fresh_ref, start, count, old, new):
        rows = pl.ds(pl.multiple_of(start, count), count)
        lines = pl.ds(pl.multiple_of(start * 2 * part_lines, count * 2 * part_lines), count * 2 * part_lines)
        posb_ref, fresh_ref, old, new = posb_ref.at[rows, :], fresh_ref.at[:, rows, :], old.at[lines, :], new.at[lines, :]
        for r in range(count):
            p = jnp.broadcast_to(posb_ref[r:r + 1, :], (part_lines, dim)).astype(jnp.bfloat16)
            h0 = jnp.broadcast_to(fresh_ref[0, r:r + 1, :], (part_lines, dim))
            h1 = jnp.broadcast_to(fresh_ref[1, r:r + 1, :], (part_lines, dim))
            fresh = jnp.where(first, h0, h1).astype(jnp.bfloat16)
            for part in range(2):
                at = slice((2 * r + part) * part_lines, (2 * r + part + 1) * part_lines)
                new[at, :] = jnp.where(slot_of[part] == p, fresh, old[at, :])

    return insert


def project_kernel(n_tp, slots, dim, pos_hbm, table_hbm, qg_hbm, kg_hbm, hid_ref, wq_ref, wk_ref, wv_ref, wo_ref, kc_ref, vc_ref,
                   q_ref, k_ref, posb_ref, wo_own, wo_in, kc_out, vc_out,
                   pos_ref, table_ref, qg_ref, kg_ref, hid, wqk, wv, vc_in, acc, vacc, cosb, sinb, e_mine, e_in,
                   in_sem, v_sem, e_send, e_recv, w_sem, s_sem, c_sem):
    t = lax.axis_index("tp")
    mate = t + 1 - 2 * lax.rem(t, 2)
    n_rows, width = hid_ref.shape
    local = wq_ref.shape[1]
    heads = local // dim
    cut = width // DEPTH_CUTS
    barrier = pltpu.get_barrier_semaphore()
    for off in range(1, n_tp):
        pl.semaphore_signal(barrier, inc=1, device_id={"tp": lax.rem(t + off, n_tp)}, device_id_type=MESH)

    loads = []
    for c in range(DEPTH_CUTS):
        at = pl.ds(c * cut, cut)
        loads.append([
            pltpu.make_async_copy(hid_ref.at[:, at], hid.at[c], in_sem.at[c, 0]),
            pltpu.make_async_copy(wq_ref.at[at, :], wqk.at[c, :, pl.ds(0, local)], in_sem.at[c, 1]),
            pltpu.make_async_copy(wk_ref.at[at, :], wqk.at[c, :, pl.ds(local, local)], in_sem.at[c, 2])])
    v_loads = [pltpu.make_async_copy(wv_ref.at[pl.ds(c * cut, cut), :], wv.at[c], v_sem.at[c]) for c in range(DEPTH_CUTS)]
    small = [pltpu.make_async_copy(src, dst, s_sem.at[i]) for i, (src, dst) in enumerate(
        ((pos_hbm, pos_ref), (table_hbm, table_ref), (qg_hbm, qg_ref), (kg_hbm, kg_ref)))]
    caches = [pltpu.make_async_copy(src, dst, c_sem.at[i]) for i, (src, dst) in enumerate(((kc_ref, kc_out), (vc_ref, vc_in), (wo_ref, wo_own)))]
    queue = loads + [v_loads, small, [caches[2]], [caches[1]], [caches[0]]]

    def issue(count):
        for group in queue[:count]:
            for copy in group:
                copy.start()
        del queue[:count]

    issue(IN_FLIGHT)
    w_copy = pltpu.make_async_remote_copy(wo_own, wo_in, w_sem.at[0], w_sem.at[1], device_id={"tp": mate}, device_id_type=MESH)
    lanes = e_mine.shape[1]
    blocks = n_rows // lanes
    def tables():
        for copy in small:
            copy.wait()
        lane = lax.broadcasted_iota(jnp.int32, (lanes, TABLE_ROWS), 1)
        which = jnp.where(lane < 3 * slots, lax.rem(lane, slots), -1).astype(jnp.float32)
        for b in range(blocks):
            at = slice(b * lanes, (b + 1) * lanes)
            column = jnp.broadcast_to(pos_ref[b:b + 1, :].astype(jnp.float32), (lanes, lanes)).T
            posb_ref[at, :] = column
            hot = jnp.where(which == column, 1.0, 0.0).astype(jnp.bfloat16)
            factors = jnp.dot(hot, table_ref[...], preferred_element_type=jnp.float32)
            cosb[at, :] = factors[:, :dim]
            sinb[at, :] = factors[:, dim:]

    for c in range(DEPTH_CUTS):
        for copy in loads[c]:
            copy.wait()
        issue(1)
        part = jnp.dot(hid[c], wqk[c], preferred_element_type=jnp.float32)
        if c == 0:
            acc[...] = part
        else:
            acc[...] += part

    ones = jnp.ones((8, local), jnp.bfloat16)
    nt = (((1,), (1,)), ((), ()))
    for i in range(2):
        rounded = acc[:, i * local:(i + 1) * local].astype(jnp.bfloat16).astype(jnp.float32)
        square = rounded * rounded
        high = square.astype(jnp.bfloat16)
        low = (square - high.astype(jnp.float32)).astype(jnp.bfloat16)
        energy = (lax.dot_general(ones, high, nt, preferred_element_type=jnp.float32)
                  + lax.dot_general(ones, low, nt, preferred_element_type=jnp.float32))
        for b in range(blocks):
            e_mine[i * blocks + b:i * blocks + b + 1, :] = energy[0:1, b * lanes:(b + 1) * lanes]
    issue(len(queue))
    pl.semaphore_wait(barrier, n_tp - 1)
    sends = [pltpu.make_async_remote_copy(
        e_mine, e_in.at[off], e_send.at[off], e_recv.at[off],
        device_id={"tp": lax.rem(t + off, n_tp)}, device_id_type=MESH) for off in range(1, n_tp)]
    for copy in sends:
        copy.start()
    caches[2].wait()
    w_copy.start()
    tables()

    for c in range(DEPTH_CUTS):
        v_loads[c].wait()
        part = jnp.dot(hid[c], wv[c], preferred_element_type=jnp.float32)
        for h in range(heads):
            if c == 0:
                vacc[h] = part[:, h * dim:(h + 1) * dim]
            else:
                vacc[h] += part[:, h * dim:(h + 1) * dim]
    caches[1].wait()
    insert = inserter(slots, heads, dim)

    def insert_rows(i, carry):
        insert(posb_ref, vacc, i * INSERT_UNROLL, INSERT_UNROLL, vc_in, vc_out)
        return carry

    lax.fori_loop(0, n_rows // INSERT_UNROLL, insert_rows, 0)

    total = e_mine[...]
    for i, copy in enumerate(sends):
        copy.wait_recv()
        total = total + e_in[i + 1]
    inv = lax.rsqrt(total / width + NORM_EPS)
    for b in range(blocks):
        at = slice(b * lanes, (b + 1) * lanes)
        for i, (gain, out) in enumerate(((qg_ref, q_ref), (kg_ref, k_ref))):
            scale = jnp.broadcast_to(inv[i * blocks + b:i * blocks + b + 1, :], (lanes, lanes)).T
            for h in range(heads):
                cols = slice(h * dim, (h + 1) * dim)
                x = acc[at, i * local + h * dim:i * local + (h + 1) * dim].astype(jnp.bfloat16).astype(jnp.float32)
                x = (x * scale * gain[:, cols]).astype(jnp.bfloat16).astype(jnp.float32)
                x = (x * cosb[at, :] + pltpu.roll(x, dim // 2, 1) * sinb[at, :]).astype(jnp.bfloat16)
                if i == 0:
                    out[at, cols] = x
                else:
                    out[h, at, :] = x.astype(jnp.float32)
    for copy in sends:
        copy.wait_send()
    w_copy.wait()
    caches[0].wait()


def project_call(n_tp, hidden, w_q, w_k, w_v, w_o, q_gain, k_gain, positions, k_cache, v_cache):
    n_rows, width = hidden.shape
    local = w_q.shape[1]
    slots, dim = k_cache.shape[1], k_cache.shape[3]
    lanes = 128
    flat = (k_cache.size // dim, dim)
    in_hbm = lambda x: pltpu.with_memory_space_constraint(x, pltpu.HBM)
    cut = width // DEPTH_CUTS
    vmem, hbm = pl.BlockSpec(memory_space=pltpu.VMEM), pl.BlockSpec(memory_space=pltpu.HBM)
    return pl.pallas_call(
        functools.partial(project_kernel, n_tp, slots, dim),
        name="project",
        out_shape=[pltpu.VMEM((n_rows, local), jnp.bfloat16), pltpu.VMEM((local // dim, n_rows, dim), jnp.float32)]
        + [pltpu.VMEM((n_rows, lanes), jnp.float32), pltpu.VMEM(w_o.shape, jnp.bfloat16), pltpu.VMEM(w_o.shape, jnp.bfloat16)] + [pltpu.VMEM(flat, jnp.bfloat16)] * 2,
        in_specs=[hbm] * 11,
        out_specs=[vmem] * 7,
        scratch_shapes=[
            pltpu.VMEM((n_rows // lanes, lanes), jnp.int32),
            pltpu.VMEM((TABLE_ROWS, 2 * dim), jnp.bfloat16),
            pltpu.VMEM((1, local), jnp.float32),
            pltpu.VMEM((1, local), jnp.float32),
            pltpu.VMEM((DEPTH_CUTS, n_rows, cut), jnp.bfloat16),
            pltpu.VMEM((DEPTH_CUTS, cut, 2 * local), jnp.bfloat16),
            pltpu.VMEM((DEPTH_CUTS, cut, local), jnp.bfloat16),
            pltpu.VMEM(flat, jnp.bfloat16),
            pltpu.VMEM((n_rows, 2 * local), jnp.float32),
            pltpu.VMEM((local // dim, n_rows, dim), jnp.float32),
            pltpu.VMEM((n_rows, dim), jnp.float32),
            pltpu.VMEM((n_rows, dim), jnp.float32),
            pltpu.VMEM((2 * n_rows // lanes, lanes), jnp.float32),
            pltpu.VMEM((n_tp, 2 * n_rows // lanes, lanes), jnp.float32),
            pltpu.SemaphoreType.DMA((DEPTH_CUTS, 3)),
            pltpu.SemaphoreType.DMA((DEPTH_CUTS,)),
            pltpu.SemaphoreType.DMA((n_tp,)),
            pltpu.SemaphoreType.DMA((n_tp,)),
            pltpu.SemaphoreType.DMA((2,)),
            pltpu.SemaphoreType.DMA((4,)),
            pltpu.SemaphoreType.DMA((3,)),
        ],
        compiler_params=pltpu.CompilerParams(collective_id=1, has_side_effects=True, vmem_limit_bytes=40 * 2**20),
        cost_estimate=pl.CostEstimate(flops=6 * n_rows * width * local, bytes_accessed=2 * (n_rows * width + 3 * width * local), transcendentals=0),
    )(*map(in_hbm, (positions.reshape(n_rows // lanes, lanes), rope_table(slots, dim), q_gain, k_gain, hidden, w_q, w_k, w_v, w_o,
                    k_cache.reshape(flat), v_cache.reshape(flat))))


ROW_BLOCK = 256
INSERT_UNROLL = 16
GROUP = 8


def attend_kernel(slots, heads, q_ref, k_ref, posb_ref, kc_ref, vn_ref, o_ref, k_out, v_out, kn, k_sem, v_sem):
    n_rows = q_ref.shape[0]
    dim = q_ref.shape[1] // heads
    lines = slots * heads
    block = ROW_BLOCK
    v_copy = pltpu.make_async_copy(vn_ref, v_out, v_sem)
    v_copy.start()
    insert = inserter(slots, heads, dim)
    n_groups = block // GROUP
    wide = GROUP * lines
    m = lax.broadcasted_iota(jnp.int32, (heads * GROUP, wide), 0)
    n = lax.broadcasted_iota(jnp.int32, (heads * GROUP, wide), 1)
    own = (lax.rem(m, GROUP) == n // lines) & (m // GROUP == lax.rem(n, heads))
    slot = jnp.where(own, (lax.rem(n, lines) // heads).astype(jnp.float32), 1e9)

    def k_copy(i):
        at = pl.ds(pl.multiple_of(i * block * lines, block * lines), block * lines)
        return pltpu.make_async_copy(kn.at[at, :], k_out.at[at, :], k_sem.at[i])

    def fill(i, carry):
        for r in range(0, block, INSERT_UNROLL):
            insert(posb_ref, k_ref, i * block + r, INSERT_UNROLL, kc_ref, kn)
        k_copy(i).start()
        return carry

    lax.fori_loop(0, n_rows // block, fill, 0)

    def one(i, carry):
        scores = []
        for g in range(n_groups):
            rows = pl.ds(pl.multiple_of(i * block + g * GROUP, GROUP), GROUP)
            keys = kn[pl.ds(pl.multiple_of((i * n_groups + g) * wide, wide), wide), :]
            q = jnp.concatenate([q_ref[rows, h * dim:(h + 1) * dim] for h in range(heads)], axis=0)
            s = lax.dot_general(q, keys, (((1,), (1,)), ((), ())), preferred_element_type=jnp.float32) * dim ** -0.5
            at = jnp.concatenate([posb_ref[rows, :]] * heads, axis=0)
            at = jnp.concatenate([at] * (wide // at.shape[1]), axis=1)
            scores.append(jnp.where(slot <= at, s, -1e30))
        for g in range(n_groups):
            rows = pl.ds(pl.multiple_of(i * block + g * GROUP, GROUP), GROUP)
            values = vn_ref[pl.ds(pl.multiple_of((i * n_groups + g) * wide, wide), wide), :]
            s = scores[g]
            e = jnp.exp(s - jnp.max(s, axis=-1, keepdims=True))
            probs = (e / jnp.sum(e, axis=-1, keepdims=True)).astype(jnp.bfloat16)
            o = jnp.dot(probs, values, preferred_element_type=jnp.float32).astype(jnp.bfloat16)
            for h in range(heads):
                o_ref[rows, h * dim:(h + 1) * dim] = o[h * GROUP:(h + 1) * GROUP]
        return carry

    lax.fori_loop(0, n_rows // block, one, 0)
    for i in range(n_rows // block):
        k_copy(i).wait()
    v_copy.wait()


def attend_call(q, k, posb, k_cache, v_new, cache_shape):
    n_rows, slots, heads, dim = cache_shape
    flat = (n_rows * slots * heads, dim)
    vmem, hbm = pl.BlockSpec(memory_space=pltpu.VMEM), pl.BlockSpec(memory_space=pltpu.HBM)
    o, k_out, v_out = pl.pallas_call(
        functools.partial(attend_kernel, slots, heads),
        name="attend",
        out_shape=[pltpu.VMEM((n_rows, heads * dim), jnp.bfloat16),
                   pltpu.HBM(flat, jnp.bfloat16), pltpu.HBM(flat, jnp.bfloat16)],
        in_specs=[vmem] * 5,
        out_specs=[vmem, hbm, hbm],
        scratch_shapes=[pltpu.VMEM(flat, jnp.bfloat16), pltpu.SemaphoreType.DMA((n_rows // ROW_BLOCK,)), pltpu.SemaphoreType.DMA],
        compiler_params=pltpu.CompilerParams(vmem_limit_bytes=24 * 2**20),
    )(q, k, posb, k_cache, v_new)
    return o, k_out.reshape(cache_shape), v_out.reshape(cache_shape)


SUBS = 2
LAG = 0
RS_PLAN = 2
AG_PLAN = 0
SHARE_TILE = 2048


def rs_plan_of(far):
    if RS_PLAN == 0:
        return [[(t, "L")] + ([(t + 1, "S")] if t + 1 < far else []) for t in range(far)]
    if RS_PLAN == 1:
        return [[(0, "L")]] + [[(t, "F")] for t in range(1, far)]
    return [[(0, "L"), (1, "S")], [(1, "L")]] + [[(t, "F")] for t in range(2, far)]


def ag_plan_of(far):
    if AG_PLAN == 0:
        return [[(t, "L")] + ([(t, "S")] if t + 1 < far else []) for t in range(far)]
    return [[(t, "F")] for t in range(far - 1)] + [[(far - 1, "L")]]


def finish_kernel(n_tp, o_ref, w_ref, w_in, hid_ref, gain_ref, out_ref,
                  o_in, lhs, lhs_in, hid, share, rs_in, rs_out,
                  x_send, x_recv, h_sem, rs_send, rs_recv, ag_send, ag_recv, d2d_send, d2d_recv):
    nz = n_tp // 2
    t = lax.axis_index("tp")
    z, k = t // 2, lax.rem(t, 2)
    up, down, mate = lax.rem(t + 2, n_tp), lax.rem(t + n_tp - 2, n_tp), z * 2 + 1 - k
    n_rows, width = out_ref.shape
    half_rows = n_rows // 2
    rows = half_rows // nz
    sub = rows // SUBS
    half = width // 2
    far = nz // 2
    chunk_of = lambda j: lax.rem(z + nz + j, nz)
    out_row = lambda j, s: pl.multiple_of(k * half_rows + chunk_of(j) * rows + s * sub, sub)
    cols = (pl.ds(0, half), pl.ds(half, half))
    target = (up, down)
    long_half = (0, 1)

    barrier = pltpu.get_barrier_semaphore()
    for peer in (up, down, mate):
        pl.semaphore_signal(barrier, inc=1, device_id={"tp": peer}, device_id_type=MESH)
    hid_copy = pltpu.make_async_copy(hid_ref.at[pl.ds(pl.multiple_of(k * half_rows + z * rows, rows), rows), :], hid, h_sem)
    hid_copy.start()
    pl.semaphore_wait(barrier, 3)

    o_copy = pltpu.make_async_remote_copy(
        o_ref.at[pl.ds(pl.multiple_of((1 - k) * half_rows, half_rows), half_rows), :], o_in,
        x_send, x_recv, device_id={"tp": mate}, device_id_type=MESH)
    o_copy.start()

    order = sorted(range(nz), key=lambda j: -min(j, nz - j))
    place = {j: i for i, j in enumerate(order)}
    for j in range(nz):
        at = slice(place[j] * rows, (place[j] + 1) * rows)
        lhs[at, :] = o_ref[pl.ds(pl.multiple_of(k * half_rows + chunk_of(j) * rows, rows), rows), :]

    def add_shares(first, last, lhs_ref, weight, fresh):
        def one(c, carry):
            at = pl.ds(pl.multiple_of(c * SHARE_TILE, SHARE_TILE), SHARE_TILE)
            part = jnp.dot(lhs_ref[first * rows:last * rows, :], weight[:, at], preferred_element_type=jnp.float32)
            if fresh:
                share[first * rows:last * rows, at] = part
            else:
                share[first * rows:last * rows, at] += part
            return carry

        lax.fori_loop(0, width // SHARE_TILE, one, 0)

    add_shares(0, nz, lhs, w_ref, True)
    o_copy.wait_recv()
    for j in range(nz):
        at = slice(place[j] * rows, (place[j] + 1) * rows)
        lhs_in[at, :] = o_in[pl.ds(pl.multiple_of(chunk_of(j) * rows, rows), rows), :]

    def halves(d, kind):
        return {"L": (d,), "S": (1 - d,), "F": (0, 1)}[kind]

    def span(d, kind):
        return pl.ds(0, width) if kind == "F" else pl.ds(halves(d, kind)[0] * half, half)

    rs_plan, ag_plan = rs_plan_of(far), ag_plan_of(far)
    slots = {}
    for stage_list in rs_plan:
        for g, kind in stage_list:
            for d in range(2):
                for s in range(SUBS):
                    slots[d, g, kind, s] = len(slots)
    ag_slots = {}
    for stage_list in ag_plan:
        for g, kind in stage_list:
            for d in range(2):
                for s in range(SUBS):
                    ag_slots[d, g, kind, s] = len(ag_slots)

    def page(d, g, s):
        return (d * far + g) * SUBS + s

    def rs_message(d, g, kind, s):
        i = slots[d, g, kind, s]
        at = span(d, kind)
        return pltpu.make_async_remote_copy(
            rs_out.at[page(d, g, s), :, at], rs_in.at[page(d, g, s), :, at], rs_send.at[i], rs_recv.at[i],
            device_id={"tp": target[d]}, device_id_type=MESH)

    def piece(j, c, s):
        return share[place[j % nz] * rows + s * sub:place[j % nz] * rows + (s + 1) * sub, c * half:(c + 1) * half]

    arrived = set()

    def received(d, g, c, s):
        for kind in ("L", "S", "F"):
            if (d, g, kind, s) in slots and c in halves(d, kind) and (d, g, kind, s) not in arrived:
                rs_message(d, g, kind, s).wait_recv()
                arrived.add((d, g, kind, s))
        return rs_in[page(d, g, s), :, c * half:(c + 1) * half].astype(jnp.float32)

    def rs_step(d, g, kind, s):
        j = far - g if d == 0 else g - far
        for c in halves(d, kind):
            value = piece(j, c, s)
            if g > (0 if c == d else 1):
                value = value + received(d, g - 1, c, s)
            rs_out[page(d, g, s), :, c * half:(c + 1) * half] = value.astype(jnp.bfloat16)
        rs_message(d, g, kind, s).start()

    def ag_message(d, g, kind, s, behind):
        here = out_ref.at[pl.ds(out_row(-behind if d == 0 else behind, s), sub), span(d, kind)]
        i = ag_slots[d, g, kind, s]
        return pltpu.make_async_remote_copy(
            here, here, ag_send.at[i], ag_recv.at[i], device_id={"tp": target[d]}, device_id_type=MESH)

    d2d = []

    def d2d_start(j, at, s):
        here = out_ref.at[pl.ds(out_row(j, s), sub), at]
        i = len(d2d)
        copy = pltpu.make_async_remote_copy(here, here, d2d_send.at[i], d2d_recv.at[i], device_id={"tp": mate}, device_id_type=MESH)
        copy.start()
        d2d.append((j, at, s))

    def finish(s):
        total = []
        for c in range(2):
            acc = piece(0, c, s)
            for d in range(2):
                acc = acc + received(d, far - 1, c, s)
            share[place[0] * rows + s * sub:place[0] * rows + (s + 1) * sub, c * half:(c + 1) * half] = acc
            total.append(jnp.sum(acc * acc, axis=-1, keepdims=True))
        inv = lax.rsqrt((total[0] + total[1]) / width + NORM_EPS)
        for c in range(2):
            at = slice(c * half, (c + 1) * half)
            normed = piece(0, c, s) * inv * gain_ref[:, at]
            out_ref[pl.ds(out_row(0, s), sub), at] = (hid[s * sub:(s + 1) * sub, at].astype(jnp.float32) + normed).astype(jnp.bfloat16)
        for g, kind in ag_plan[0]:
            for d in range(2):
                ag_message(d, g, kind, s, 0).start()
        d2d_start(0, pl.ds(0, width), s)

    def ag_step(t, s):
        for g, kind in ag_plan[t - 1]:
            for d in range(2):
                ag_message(d, g, kind, s, g + 1).wait_recv()
                if t < len(ag_plan):
                    for g_next, kind_next in ag_plan[t]:
                        if kind_next == kind or (kind == "F" and kind_next == "L"):
                            ag_message(d, g_next, kind_next, s, g + 1).start()
                d2d_start(-(g + 1) if d == 0 else g + 1, span(d, kind), s)

    def stage(t, s):
        if t < far:
            for g, kind in rs_plan[t]:
                for d in range(2):
                    rs_step(d, g, kind, s)
        elif t == far:
            if s == 0:
                hid_copy.wait()
            finish(s)
        else:
            ag_step(t - far, s)

    add_shares(0, 3, lhs_in, w_in, False)
    last_stage = far + len(ag_plan)
    for slot in range(last_stage + 1 + LAG * (SUBS - 1)):
        if slot == 1:
            add_shares(3, nz, lhs_in, w_in, False)
        for s in range(SUBS):
            t = slot - LAG * s
            if 0 <= t <= last_stage:
                stage(t, s)

    o_copy.wait_send()
    for d, g, kind, s in slots:
        rs_message(d, g, kind, s).wait_send()
    for d, g, kind, s in ag_slots:
        ag_message(d, g, kind, s, g).wait_send()
    for i, (j, at, s) in enumerate(d2d):
        here = out_ref.at[pl.ds(out_row(j, s), sub), at]
        there = out_ref.at[pl.ds(pl.multiple_of((1 - k) * half_rows + chunk_of(j) * rows + s * sub, sub), sub), at]
        copy = pltpu.make_async_remote_copy(here, there, d2d_send.at[i], d2d_recv.at[i], device_id={"tp": mate}, device_id_type=MESH)
        copy.wait_send()
        copy.wait_recv()


def finish_call(n_tp, attn, w_own, w_mate, hidden, gain):
    n_rows, width = hidden.shape
    depth = w_own.shape[0]
    nz = n_tp // 2
    half_rows, rows = n_rows // 2, n_rows // n_tp
    sub = rows // SUBS
    n_msg = 2 * SUBS * (nz - 1)
    vmem = pl.BlockSpec(memory_space=pltpu.VMEM)
    return pl.pallas_call(
        functools.partial(finish_kernel, n_tp),
        name="finish",
        out_shape=pltpu.VMEM((n_rows, width), jnp.bfloat16) if OUT_VMEM else jax.ShapeDtypeStruct((n_rows, width), jnp.bfloat16),
        in_specs=[vmem, vmem, vmem, pl.BlockSpec(memory_space=pltpu.HBM), vmem],
        out_specs=vmem,
        scratch_shapes=[
            pltpu.VMEM((half_rows, depth), jnp.bfloat16),
            pltpu.VMEM((half_rows, depth), jnp.bfloat16),
            pltpu.VMEM((half_rows, depth), jnp.bfloat16),
            pltpu.VMEM((rows, width), jnp.bfloat16),
            pltpu.VMEM((half_rows, width), jnp.float32),
            pltpu.VMEM((nz * SUBS, sub, width), jnp.bfloat16),
            pltpu.VMEM((nz * SUBS, sub, width), jnp.bfloat16),
            pltpu.SemaphoreType.DMA,
            pltpu.SemaphoreType.DMA,
            pltpu.SemaphoreType.DMA,
            pltpu.SemaphoreType.DMA((n_msg,)),
            pltpu.SemaphoreType.DMA((n_msg,)),
            pltpu.SemaphoreType.DMA((n_msg,)),
            pltpu.SemaphoreType.DMA((n_msg,)),
            pltpu.SemaphoreType.DMA((2 * SUBS * nz,)),
            pltpu.SemaphoreType.DMA((2 * SUBS * nz,)),
        ],
        compiler_params=pltpu.CompilerParams(collective_id=0, has_side_effects=True, vmem_limit_bytes=40 * 2**20),
    )(attn, w_own, w_mate, pltpu.with_memory_space_constraint(hidden, pltpu.HBM), gain)


def solution(mesh):
    def local_step(hidden, w_q, w_k, w_v, w_o, q_norm_w, k_norm_w, post_norm_w, k_cache, v_cache, positions):
        n_tp = mesh.shape["tp"]
        q_rot, k_rot, posb, w_own, w_mate, k_near, v_near = project_call(
            n_tp, hidden, w_q, w_k, w_v, w_o, q_norm_w[None, :], k_norm_w[None, :], positions, k_cache, v_cache)
        attn, k_new, v_new = attend_call(q_rot, k_rot, posb, k_near, v_near, k_cache.shape)
        hidden_out = finish_call(n_tp, attn, w_own, w_mate, hidden, post_norm_w[None, :])
        return hidden_out, k_new, v_new

    cache_spec = P('dp', None, 'tp', None)
    return jax.shard_map(local_step, mesh=mesh, in_specs=(P('dp', None), P(None, 'tp'), P(None, 'tp'), P(None, 'tp'), P('tp', None), P('tp'), P('tp'), P(None), cache_spec, cache_spec, P('dp')), out_specs=(P('dp', None), cache_spec, cache_spec), check_vma=False)
```

```python
import functools

import jax
import jax.numpy as jnp
import numpy as np
from jax import lax
from jax.experimental import pallas as pl
from jax.experimental.pallas import tpu as pltpu
from jax.sharding import PartitionSpec as P

NORM_EPS = 1e-6
ROPE_BASE = 500000.0
OUT_VMEM = True


MESH = pl.DeviceIdType.MESH
DEPTH_CUTS = 4
IN_FLIGHT = 4
TABLE_ROWS = 128


def rope_table(slots, dim):
    half = dim // 2
    inv_freq = np.float32(ROPE_BASE) ** (np.float32(-2.0) * np.arange(half, dtype=np.float32) / np.float32(dim))
    angles = (np.arange(slots, dtype=np.float32)[:, None] * inv_freq.astype(np.float32)[None, :]).astype(np.float64)
    cos_tab, sin_tab = np.cos(angles), np.sin(angles)
    rest = np.concatenate([cos_tab, cos_tab, -sin_tab, sin_tab], axis=1).astype(np.float32)
    out = np.zeros((TABLE_ROWS, 2 * dim), np.float32)
    for part in range(3):
        high = rest.astype(jnp.bfloat16).astype(np.float32)
        out[part * slots:(part + 1) * slots] = high
        rest = rest - high
    return jnp.asarray(out, dtype=jnp.bfloat16)


def inserter(slots, heads, dim):
    assert heads == 2
    part_lines = slots * heads // 2
    line = lax.broadcasted_iota(jnp.int32, (part_lines, dim), 0)
    first = lax.rem(line, heads) == 0
    slot_of = [(line // heads + part * (slots // 2)).astype(jnp.float32).astype(jnp.bfloat16) for part in range(2)]

    def insert(posb_ref, fresh_ref, start, count, old, new):
        rows = pl.ds(pl.multiple_of(start, count), count)
        lines = pl.ds(pl.multiple_of(start * 2 * part_lines, count * 2 * part_lines), count * 2 * part_lines)
        posb_ref, fresh_ref, old, new = posb_ref.at[rows, :], fresh_ref.at[:, rows, :], old.at[lines, :], new.at[lines, :]
        for r in range(count):
            p = jnp.broadcast_to(posb_ref[r:r + 1, :], (part_lines, dim)).astype(jnp.bfloat16)
            h0 = jnp.broadcast_to(fresh_ref[0, r:r + 1, :], (part_lines, dim))
            h1 = jnp.broadcast_to(fresh_ref[1, r:r + 1, :], (part_lines, dim))
            fresh = jnp.where(first, h0, h1).astype(jnp.bfloat16)
            for part in range(2):
                at = slice((2 * r + part) * part_lines, (2 * r + part + 1) * part_lines)
                new[at, :] = jnp.where(slot_of[part] == p, fresh, old[at, :])

    return insert


def project_kernel(n_tp, slots, dim, pos_hbm, table_hbm, qg_hbm, kg_hbm, hid_ref, wq_ref, wk_ref, wv_ref, wo_ref, kc_ref, vc_ref,
                   q_ref, k_ref, posb_ref, wo_own, wo_in, kc_out, vc_out,
                   pos_ref, table_ref, qg_ref, kg_ref, hid, wqk, wv, vc_in, acc, vacc, cosb, sinb, e_mine, e_in,
                   in_sem, v_sem, e_send, e_recv, w_sem, s_sem, c_sem):
    t = lax.axis_index("tp")
    mate = t + 1 - 2 * lax.rem(t, 2)
    n_rows, width = hid_ref.shape
    local = wq_ref.shape[1]
    heads = local // dim
    cut = width // DEPTH_CUTS
    barrier = pltpu.get_barrier_semaphore()
    for off in range(1, n_tp):
        pl.semaphore_signal(barrier, inc=1, device_id={"tp": lax.rem(t + off, n_tp)}, device_id_type=MESH)

    loads = []
    for c in range(DEPTH_CUTS):
        at = pl.ds(c * cut, cut)
        loads.append([
            pltpu.make_async_copy(hid_ref.at[:, at], hid.at[c], in_sem.at[c, 0]),
            pltpu.make_async_copy(wq_ref.at[at, :], wqk.at[c, :, pl.ds(0, local)], in_sem.at[c, 1]),
            pltpu.make_async_copy(wk_ref.at[at, :], wqk.at[c, :, pl.ds(local, local)], in_sem.at[c, 2])])
    v_loads = [pltpu.make_async_copy(wv_ref.at[pl.ds(c * cut, cut), :], wv.at[c], v_sem.at[c]) for c in range(DEPTH_CUTS)]
    small = [pltpu.make_async_copy(src, dst, s_sem.at[i]) for i, (src, dst) in enumerate(
        ((pos_hbm, pos_ref), (table_hbm, table_ref), (qg_hbm, qg_ref), (kg_hbm, kg_ref)))]
    caches = [pltpu.make_async_copy(src, dst, c_sem.at[i]) for i, (src, dst) in enumerate(((kc_ref, kc_out), (vc_ref, vc_in), (wo_ref, wo_own)))]
    queue = loads + [v_loads, small, [caches[2]], [caches[1]], [caches[0]]]

    def issue(count):
        for group in queue[:count]:
            for copy in group:
                copy.start()
        del queue[:count]

    issue(IN_FLIGHT)
    w_copy = pltpu.make_async_remote_copy(wo_own, wo_in, w_sem.at[0], w_sem.at[1], device_id={"tp": mate}, device_id_type=MESH)
    lanes = e_mine.shape[1]
    blocks = n_rows // lanes
    def tables():
        for copy in small:
            copy.wait()
        lane = lax.broadcasted_iota(jnp.int32, (lanes, TABLE_ROWS), 1)
        which = jnp.where(lane < 3 * slots, lax.rem(lane, slots), -1).astype(jnp.float32)
        for b in range(blocks):
            at = slice(b * lanes, (b + 1) * lanes)
            column = jnp.broadcast_to(pos_ref[b:b + 1, :].astype(jnp.float32), (lanes, lanes)).T
            posb_ref[at, :] = column
            hot = jnp.where(which == column, 1.0, 0.0).astype(jnp.bfloat16)
            factors = jnp.dot(hot, table_ref[...], preferred_element_type=jnp.float32)
            cosb[at, :] = factors[:, :dim]
            sinb[at, :] = factors[:, dim:]

    for c in range(DEPTH_CUTS):
        for copy in loads[c]:
            copy.wait()
        issue(1)
        part = jnp.dot(hid[c], wqk[c], preferred_element_type=jnp.float32)
        if c == 0:
            acc[...] = part
        else:
            acc[...] += part

    ones = jnp.ones((8, local), jnp.bfloat16)
    nt = (((1,), (1,)), ((), ()))
    for i in range(2):
        rounded = acc[:, i * local:(i + 1) * local].astype(jnp.bfloat16).astype(jnp.float32)
        square = rounded * rounded
        high = square.astype(jnp.bfloat16)
        low = (square - high.astype(jnp.float32)).astype(jnp.bfloat16)
        energy = (lax.dot_general(ones, high, nt, preferred_element_type=jnp.float32)
                  + lax.dot_general(ones, low, nt, preferred_element_type=jnp.float32))
        for b in range(blocks):
            e_mine[i * blocks + b:i * blocks + b + 1, :] = energy[0:1, b * lanes:(b + 1) * lanes]
    issue(len(queue))
    pl.semaphore_wait(barrier, n_tp - 1)
    sends = [pltpu.make_async_remote_copy(
        e_mine, e_in.at[off], e_send.at[off], e_recv.at[off],
        device_id={"tp": lax.rem(t + off, n_tp)}, device_id_type=MESH) for off in range(1, n_tp)]
    for copy in sends:
        copy.start()
    caches[2].wait()
    w_copy.start()
    tables()

    for c in range(DEPTH_CUTS):
        v_loads[c].wait()
        part = jnp.dot(hid[c], wv[c], preferred_element_type=jnp.float32)
        for h in range(heads):
            if c == 0:
                vacc[h] = part[:, h * dim:(h + 1) * dim]
            else:
                vacc[h] += part[:, h * dim:(h + 1) * dim]
    caches[1].wait()
    insert = inserter(slots, heads, dim)

    def insert_rows(i, carry):
        insert(posb_ref, vacc, i * INSERT_UNROLL, INSERT_UNROLL, vc_in, vc_out)
        return carry

    lax.fori_loop(0, n_rows // INSERT_UNROLL, insert_rows, 0)

    total = e_mine[...]
    for i, copy in enumerate(sends):
        copy.wait_recv()
        total = total + e_in[i + 1]
    inv = lax.rsqrt(total / width + NORM_EPS)
    for b in range(blocks):
        at = slice(b * lanes, (b + 1) * lanes)
        for i, (gain, out) in enumerate(((qg_ref, q_ref), (kg_ref, k_ref))):
            scale = jnp.broadcast_to(inv[i * blocks + b:i * blocks + b + 1, :], (lanes, lanes)).T
            for h in range(heads):
                cols = slice(h * dim, (h + 1) * dim)
                x = acc[at, i * local + h * dim:i * local + (h + 1) * dim].astype(jnp.bfloat16).astype(jnp.float32)
                x = (x * scale * gain[:, cols]).astype(jnp.bfloat16).astype(jnp.float32)
                x = (x * cosb[at, :] + pltpu.roll(x, dim // 2, 1) * sinb[at, :]).astype(jnp.bfloat16)
                if i == 0:
                    out[at, cols] = x
                else:
                    out[h, at, :] = x.astype(jnp.float32)
    for copy in sends:
        copy.wait_send()
    w_copy.wait()
    caches[0].wait()


def project_call(n_tp, hidden, w_q, w_k, w_v, w_o, q_gain, k_gain, positions, k_cache, v_cache):
    n_rows, width = hidden.shape
    local = w_q.shape[1]
    slots, dim = k_cache.shape[1], k_cache.shape[3]
    lanes = 128
    flat = (k_cache.size // dim, dim)
    in_hbm = lambda x: pltpu.with_memory_space_constraint(x, pltpu.HBM)
    cut = width // DEPTH_CUTS
    vmem, hbm = pl.BlockSpec(memory_space=pltpu.VMEM), pl.BlockSpec(memory_space=pltpu.HBM)
    return pl.pallas_call(
        functools.partial(project_kernel, n_tp, slots, dim),
        name="project",
        out_shape=[pltpu.VMEM((n_rows, local), jnp.bfloat16), pltpu.VMEM((local // dim, n_rows, dim), jnp.float32)]
        + [pltpu.VMEM((n_rows, lanes), jnp.float32), pltpu.VMEM(w_o.shape, jnp.bfloat16), pltpu.VMEM(w_o.shape, jnp.bfloat16)] + [pltpu.VMEM(flat, jnp.bfloat16)] * 2,
        in_specs=[hbm] * 11,
        out_specs=[vmem] * 7,
        scratch_shapes=[
            pltpu.VMEM((n_rows // lanes, lanes), jnp.int32),
            pltpu.VMEM((TABLE_ROWS, 2 * dim), jnp.bfloat16),
            pltpu.VMEM((1, local), jnp.float32),
            pltpu.VMEM((1, local), jnp.float32),
            pltpu.VMEM((DEPTH_CUTS, n_rows, cut), jnp.bfloat16),
            pltpu.VMEM((DEPTH_CUTS, cut, 2 * local), jnp.bfloat16),
            pltpu.VMEM((DEPTH_CUTS, cut, local), jnp.bfloat16),
            pltpu.VMEM(flat, jnp.bfloat16),
            pltpu.VMEM((n_rows, 2 * local), jnp.float32),
            pltpu.VMEM((local // dim, n_rows, dim), jnp.float32),
            pltpu.VMEM((n_rows, dim), jnp.float32),
            pltpu.VMEM((n_rows, dim), jnp.float32),
            pltpu.VMEM((2 * n_rows // lanes, lanes), jnp.float32),
            pltpu.VMEM((n_tp, 2 * n_rows // lanes, lanes), jnp.float32),
            pltpu.SemaphoreType.DMA((DEPTH_CUTS, 3)),
            pltpu.SemaphoreType.DMA((DEPTH_CUTS,)),
            pltpu.SemaphoreType.DMA((n_tp,)),
            pltpu.SemaphoreType.DMA((n_tp,)),
            pltpu.SemaphoreType.DMA((2,)),
            pltpu.SemaphoreType.DMA((4,)),
            pltpu.SemaphoreType.DMA((3,)),
        ],
        compiler_params=pltpu.CompilerParams(collective_id=1, has_side_effects=True, vmem_limit_bytes=40 * 2**20),
        cost_estimate=pl.CostEstimate(flops=6 * n_rows * width * local, bytes_accessed=2 * (n_rows * width + 3 * width * local), transcendentals=0),
    )(*map(in_hbm, (positions.reshape(n_rows // lanes, lanes), rope_table(slots, dim), q_gain, k_gain, hidden, w_q, w_k, w_v, w_o,
                    k_cache.reshape(flat), v_cache.reshape(flat))))


ROW_BLOCK = 256
INSERT_UNROLL = 16
GROUP = 8


def attend_kernel(slots, heads, q_ref, k_ref, posb_ref, kc_ref, vn_ref, o_ref, k_out, v_out, kn, k_sem, v_sem):
    n_rows = q_ref.shape[0]
    dim = q_ref.shape[1] // heads
    lines = slots * heads
    block = ROW_BLOCK
    v_copy = pltpu.make_async_copy(vn_ref, v_out, v_sem)
    v_copy.start()
    insert = inserter(slots, heads, dim)
    n_groups = block // GROUP
    wide = GROUP * lines
    m = lax.broadcasted_iota(jnp.int32, (heads * GROUP, wide), 0)
    n = lax.broadcasted_iota(jnp.int32, (heads * GROUP, wide), 1)
    own = (lax.rem(m, GROUP) == n // lines) & (m // GROUP == lax.rem(n, heads))
    slot = jnp.where(own, (lax.rem(n, lines) // heads).astype(jnp.float32), 1e9)

    def k_copy(i):
        at = pl.ds(pl.multiple_of(i * block * lines, block * lines), block * lines)
        return pltpu.make_async_copy(kn.at[at, :], k_out.at[at, :], k_sem.at[i])

    def fill(i, carry):
        for r in range(0, block, INSERT_UNROLL):
            insert(posb_ref, k_ref, i * block + r, INSERT_UNROLL, kc_ref, kn)
        k_copy(i).start()
        return carry

    lax.fori_loop(0, n_rows // block, fill, 0)

    def one(i, carry):
        scores = []
        for g in range(n_groups):
            rows = pl.ds(pl.multiple_of(i * block + g * GROUP, GROUP), GROUP)
            keys = kn[pl.ds(pl.multiple_of((i * n_groups + g) * wide, wide), wide), :]
            q = jnp.concatenate([q_ref[rows, h * dim:(h + 1) * dim] for h in range(heads)], axis=0)
            s = lax.dot_general(q, keys, (((1,), (1,)), ((), ())), preferred_element_type=jnp.float32) * dim ** -0.5
            at = jnp.concatenate([posb_ref[rows, :]] * heads, axis=0)
            at = jnp.concatenate([at] * (wide // at.shape[1]), axis=1)
            scores.append(jnp.where(slot <= at, s, -1e30))
        for g in range(n_groups):
            rows = pl.ds(pl.multiple_of(i * block + g * GROUP, GROUP), GROUP)
            values = vn_ref[pl.ds(pl.multiple_of((i * n_groups + g) * wide, wide), wide), :]
            s = scores[g]
            e = jnp.exp(s - jnp.max(s, axis=-1, keepdims=True))
            probs = (e / jnp.sum(e, axis=-1, keepdims=True)).astype(jnp.bfloat16)
            o = jnp.dot(probs, values, preferred_element_type=jnp.float32).astype(jnp.bfloat16)
            for h in range(heads):
                o_ref[rows, h * dim:(h + 1) * dim] = o[h * GROUP:(h + 1) * GROUP]
        return carry

    lax.fori_loop(0, n_rows // block, one, 0)
    for i in range(n_rows // block):
        k_copy(i).wait()
    v_copy.wait()


def attend_call(q, k, posb, k_cache, v_new, cache_shape):
    n_rows, slots, heads, dim = cache_shape
    flat = (n_rows * slots * heads, dim)
    vmem, hbm = pl.BlockSpec(memory_space=pltpu.VMEM), pl.BlockSpec(memory_space=pltpu.HBM)
    o, k_out, v_out = pl.pallas_call(
        functools.partial(attend_kernel, slots, heads),
        name="attend",
        out_shape=[pltpu.VMEM((n_rows, heads * dim), jnp.bfloat16),
                   pltpu.HBM(flat, jnp.bfloat16), pltpu.HBM(flat, jnp.bfloat16)],
        in_specs=[vmem] * 5,
        out_specs=[vmem, hbm, hbm],
        scratch_shapes=[pltpu.VMEM(flat, jnp.bfloat16), pltpu.SemaphoreType.DMA((n_rows // ROW_BLOCK,)), pltpu.SemaphoreType.DMA],
        compiler_params=pltpu.CompilerParams(vmem_limit_bytes=24 * 2**20),
    )(q, k, posb, k_cache, v_new)
    return o, k_out.reshape(cache_shape), v_out.reshape(cache_shape)


SUBS = 2
LAG = 0
RS_PLAN = 2
AG_PLAN = 0
SHARE_TILE = 4096


def rs_plan_of(far):
    if RS_PLAN == 0:
        return [[(t, "L")] + ([(t + 1, "S")] if t + 1 < far else []) for t in range(far)]
    if RS_PLAN == 1:
        return [[(0, "L")]] + [[(t, "F")] for t in range(1, far)]
    if RS_PLAN == 3:
        return [[(0, "L"), (1, "S")], [(1, "L")]] + [[(t, "F")] for t in range(2, far - 1)] + [[(far - 1, "L"), (far - 1, "S")]]
    return [[(0, "L"), (1, "S")], [(1, "L")]] + [[(t, "F")] for t in range(2, far)]


def ag_plan_of(far):
    if AG_PLAN == 0:
        return [[(t, "L")] + ([(t, "S")] if t + 1 < far else []) for t in range(far)]
    if AG_PLAN == 2:
        return [[(t, "F")] if t < far - 2 else [(t, "L")] + ([(t, "S")] if t + 1 < far else []) for t in range(far)]
    if AG_PLAN == 3:
        return [[(t, "F")] if t < 1 else [(t, "L")] + ([(t, "S")] if t + 1 < far else []) for t in range(far)]
    return [[(t, "F")] for t in range(far - 1)] + [[(far - 1, "L")]]


def finish_kernel(n_tp, o_ref, w_ref, w_in, hid_ref, gain_ref, out_ref,
                  o_in, lhs, lhs_in, hid, share, rs_in, rs_out,
                  x_send, x_recv, h_sem, rs_send, rs_recv, ag_send, ag_recv, d2d_send, d2d_recv):
    nz = n_tp // 2
    t = lax.axis_index("tp")
    z, k = t // 2, lax.rem(t, 2)
    up, down, mate = lax.rem(t + 2, n_tp), lax.rem(t + n_tp - 2, n_tp), z * 2 + 1 - k
    n_rows, width = out_ref.shape
    half_rows = n_rows // 2
    rows = half_rows // nz
    sub = rows // SUBS
    half = width // 2
    far = nz // 2
    chunk_of = lambda j: lax.rem(z + nz + j, nz)
    out_row = lambda j, s: pl.multiple_of(k * half_rows + chunk_of(j) * rows + s * sub, sub)
    cols = (pl.ds(0, half), pl.ds(half, half))
    target = (up, down)
    long_half = (0, 1)

    barrier = pltpu.get_barrier_semaphore()
    for peer in (up, down, mate):
        pl.semaphore_signal(barrier, inc=1, device_id={"tp": peer}, device_id_type=MESH)
    hid_copy = pltpu.make_async_copy(hid_ref.at[pl.ds(pl.multiple_of(k * half_rows + z * rows, rows), rows), :], hid, h_sem)
    hid_copy.start()
    pl.semaphore_wait(barrier, 3)

    o_copy = pltpu.make_async_remote_copy(
        o_ref.at[pl.ds(pl.multiple_of((1 - k) * half_rows, half_rows), half_rows), :], o_in,
        x_send, x_recv, device_id={"tp": mate}, device_id_type=MESH)
    o_copy.start()

    order = sorted(range(nz), key=lambda j: -min(j, nz - j))
    place = {j: i for i, j in enumerate(order)}
    def gather(first, last, ref, base, out):
        for j in order[first:last]:
            at = slice(place[j] * rows, (place[j] + 1) * rows)
            out[at, :] = ref[pl.ds(pl.multiple_of(base + chunk_of(j) * rows, rows), rows), :]

    def add_shares(first, last, lhs_ref, weight, fresh):
        def one(c, carry):
            at = pl.ds(pl.multiple_of(c * SHARE_TILE, SHARE_TILE), SHARE_TILE)
            part = jnp.dot(lhs_ref[first * rows:last * rows, :], weight[:, at], preferred_element_type=jnp.float32)
            if fresh:
                share[first * rows:last * rows, at] = part
            else:
                share[first * rows:last * rows, at] += part
            return carry

        lax.fori_loop(0, width // SHARE_TILE, one, 0)

    gather(0, nz, o_ref, k * half_rows, lhs)
    add_shares(0, 3, lhs, w_ref, True)
    o_copy.wait_recv()
    gather(0, 3, o_in, 0, lhs_in)

    def halves(d, kind):
        return {"L": (d,), "S": (1 - d,), "F": (0, 1)}[kind]

    def span(d, kind):
        return pl.ds(0, width) if kind == "F" else pl.ds(halves(d, kind)[0] * half, half)

    rs_plan, ag_plan = rs_plan_of(far), ag_plan_of(far)
    slots = {}
    for stage_list in rs_plan:
        for g, kind in stage_list:
            for d in range(2):
                for s in range(SUBS):
                    slots[d, g, kind, s] = len(slots)
    ag_slots = {}
    for stage_list in ag_plan:
        for g, kind in stage_list:
            for d in range(2):
                for s in range(SUBS):
                    ag_slots[d, g, kind, s] = len(ag_slots)

    def page(d, g, s):
        return (d * far + g) * SUBS + s

    def rs_message(d, g, kind, s):
        i = slots[d, g, kind, s]
        at = span(d, kind)
        return pltpu.make_async_remote_copy(
            rs_out.at[page(d, g, s), :, at], rs_in.at[page(d, g, s), :, at], rs_send.at[i], rs_recv.at[i],
            device_id={"tp": target[d]}, device_id_type=MESH)

    def piece(j, c, s):
        return share[place[j % nz] * rows + s * sub:place[j % nz] * rows + (s + 1) * sub, c * half:(c + 1) * half]

    arrived = set()

    def received(d, g, c, s):
        for kind in ("L", "S", "F"):
            if (d, g, kind, s) in slots and c in halves(d, kind) and (d, g, kind, s) not in arrived:
                rs_message(d, g, kind, s).wait_recv()
                arrived.add((d, g, kind, s))
        return rs_in[page(d, g, s), :, c * half:(c + 1) * half].astype(jnp.float32)

    def rs_step(d, g, kind, s):
        j = far - g if d == 0 else g - far
        for c in halves(d, kind):
            value = piece(j, c, s)
            if g > (0 if c == d else 1):
                value = value + received(d, g - 1, c, s)
            rs_out[page(d, g, s), :, c * half:(c + 1) * half] = value.astype(jnp.bfloat16)
        rs_message(d, g, kind, s).start()

    def ag_message(d, g, kind, s, behind):
        here = out_ref.at[pl.ds(out_row(-behind if d == 0 else behind, s), sub), span(d, kind)]
        i = ag_slots[d, g, kind, s]
        return pltpu.make_async_remote_copy(
            here, here, ag_send.at[i], ag_recv.at[i], device_id={"tp": target[d]}, device_id_type=MESH)

    d2d = []

    def d2d_start(j, at, s):
        here = out_ref.at[pl.ds(out_row(j, s), sub), at]
        i = len(d2d)
        copy = pltpu.make_async_remote_copy(here, here, d2d_send.at[i], d2d_recv.at[i], device_id={"tp": mate}, device_id_type=MESH)
        copy.start()
        d2d.append((j, at, s))

    def finish(s):
        total = []
        for c in range(2):
            acc = piece(0, c, s)
            for d in range(2):
                acc = acc + received(d, far - 1, c, s)
            share[place[0] * rows + s * sub:place[0] * rows + (s + 1) * sub, c * half:(c + 1) * half] = acc
            total.append(jnp.sum(acc * acc, axis=-1, keepdims=True))
        inv = lax.rsqrt((total[0] + total[1]) / width + NORM_EPS)
        for c in range(2):
            at = slice(c * half, (c + 1) * half)
            normed = piece(0, c, s) * inv * gain_ref[:, at]
            out_ref[pl.ds(out_row(0, s), sub), at] = (hid[s * sub:(s + 1) * sub, at].astype(jnp.float32) + normed).astype(jnp.bfloat16)
        for g, kind in ag_plan[0]:
            for d in range(2):
                ag_message(d, g, kind, s, 0).start()
        d2d_start(0, pl.ds(0, width), s)

    def ag_step(t, s):
        for g, kind in ag_plan[t - 1]:
            for d in range(2):
                ag_message(d, g, kind, s, g + 1).wait_recv()
                if t < len(ag_plan):
                    for g_next, kind_next in ag_plan[t]:
                        if set(halves(d, kind_next)) <= set(halves(d, kind)):
                            ag_message(d, g_next, kind_next, s, g + 1).start()
                d2d_start(-(g + 1) if d == 0 else g + 1, span(d, kind), s)

    def stage(t, s):
        if t < far:
            for g, kind in rs_plan[t]:
                for d in range(2):
                    rs_step(d, g, kind, s)
        elif t == far:
            if s == 0:
                hid_copy.wait()
            finish(s)
        else:
            ag_step(t - far, s)

    add_shares(0, 3, lhs_in, w_in, False)
    last_stage = far + len(ag_plan)
    for slot in range(last_stage + 1 + LAG * (SUBS - 1)):
        if slot == 1:
            gather(3, nz, o_in, 0, lhs_in)
            add_shares(3, nz, lhs, w_ref, True)
            add_shares(3, nz, lhs_in, w_in, False)
        for s in range(SUBS):
            t = slot - LAG * s
            if 0 <= t <= last_stage:
                stage(t, s)

    o_copy.wait_send()
    for d, g, kind, s in slots:
        rs_message(d, g, kind, s).wait_send()
    for d, g, kind, s in ag_slots:
        ag_message(d, g, kind, s, g).wait_send()
    for i, (j, at, s) in enumerate(d2d):
        here = out_ref.at[pl.ds(out_row(j, s), sub), at]
        there = out_ref.at[pl.ds(pl.multiple_of((1 - k) * half_rows + chunk_of(j) * rows + s * sub, sub), sub), at]
        copy = pltpu.make_async_remote_copy(here, there, d2d_send.at[i], d2d_recv.at[i], device_id={"tp": mate}, device_id_type=MESH)
        copy.wait_send()
        copy.wait_recv()


def finish_call(n_tp, attn, w_own, w_mate, hidden, gain):
    n_rows, width = hidden.shape
    depth = w_own.shape[0]
    nz = n_tp // 2
    half_rows, rows = n_rows // 2, n_rows // n_tp
    sub = rows // SUBS
    n_msg = 2 * SUBS * (nz - 1)
    vmem = pl.BlockSpec(memory_space=pltpu.VMEM)
    return pl.pallas_call(
        functools.partial(finish_kernel, n_tp),
        name="finish",
        out_shape=pltpu.VMEM((n_rows, width), jnp.bfloat16) if OUT_VMEM else jax.ShapeDtypeStruct((n_rows, width), jnp.bfloat16),
        in_specs=[vmem, vmem, vmem, pl.BlockSpec(memory_space=pltpu.HBM), vmem],
        out_specs=vmem,
        scratch_shapes=[
            pltpu.VMEM((half_rows, depth), jnp.bfloat16),
            pltpu.VMEM((half_rows, depth), jnp.bfloat16),
            pltpu.VMEM((half_rows, depth), jnp.bfloat16),
            pltpu.VMEM((rows, width), jnp.bfloat16),
            pltpu.VMEM((half_rows, width), jnp.float32),
            pltpu.VMEM((nz * SUBS, sub, width), jnp.bfloat16),
            pltpu.VMEM((nz * SUBS, sub, width), jnp.bfloat16),
            pltpu.SemaphoreType.DMA,
            pltpu.SemaphoreType.DMA,
            pltpu.SemaphoreType.DMA,
            pltpu.SemaphoreType.DMA((n_msg,)),
            pltpu.SemaphoreType.DMA((n_msg,)),
            pltpu.SemaphoreType.DMA((n_msg,)),
            pltpu.SemaphoreType.DMA((n_msg,)),
            pltpu.SemaphoreType.DMA((2 * SUBS * nz,)),
            pltpu.SemaphoreType.DMA((2 * SUBS * nz,)),
        ],
        compiler_params=pltpu.CompilerParams(collective_id=0, has_side_effects=True, vmem_limit_bytes=40 * 2**20),
    )(attn, w_own, w_mate, pltpu.with_memory_space_constraint(hidden, pltpu.HBM), gain)


def solution(mesh):
    def local_step(hidden, w_q, w_k, w_v, w_o, q_norm_w, k_norm_w, post_norm_w, k_cache, v_cache, positions):
        n_tp = mesh.shape["tp"]
        q_rot, k_rot, posb, w_own, w_mate, k_near, v_near = project_call(
            n_tp, hidden, w_q, w_k, w_v, w_o, q_norm_w[None, :], k_norm_w[None, :], positions, k_cache, v_cache)
        attn, k_new, v_new = attend_call(q_rot, k_rot, posb, k_near, v_near, k_cache.shape)
        hidden_out = finish_call(n_tp, attn, w_own, w_mate, hidden, post_norm_w[None, :])
        return hidden_out, k_new, v_new

    cache_spec = P('dp', None, 'tp', None)
    return jax.shard_map(local_step, mesh=mesh, in_specs=(P('dp', None), P(None, 'tp'), P(None, 'tp'), P(None, 'tp'), P('tp', None), P('tp'), P('tp'), P(None), cache_spec, cache_spec, P('dp')), out_specs=(P('dp', None), cache_spec, cache_spec), check_vma=False)
```

```python
import functools

import jax
import jax.numpy as jnp
import numpy as np
from jax import lax
from jax.experimental import pallas as pl
from jax.experimental.pallas import tpu as pltpu
from jax.sharding import PartitionSpec as P

NORM_EPS = 1e-6
ROPE_BASE = 500000.0
OUT_VMEM = True


MESH = pl.DeviceIdType.MESH
DEPTH_CUTS = 4
IN_FLIGHT = 4
TABLE_ROWS = 128


def rope_table(slots, dim):
    half = dim // 2
    inv_freq = np.float32(ROPE_BASE) ** (np.float32(-2.0) * np.arange(half, dtype=np.float32) / np.float32(dim))
    angles = (np.arange(slots, dtype=np.float32)[:, None] * inv_freq.astype(np.float32)[None, :]).astype(np.float64)
    cos_tab, sin_tab = np.cos(angles), np.sin(angles)
    rest = np.concatenate([cos_tab, cos_tab, -sin_tab, sin_tab], axis=1).astype(np.float32)
    out = np.zeros((TABLE_ROWS, 2 * dim), np.float32)
    for part in range(3):
        high = rest.astype(jnp.bfloat16).astype(np.float32)
        out[part * slots:(part + 1) * slots] = high
        rest = rest - high
    return jnp.asarray(out, dtype=jnp.bfloat16)


def inserter(slots, heads, dim):
    assert heads == 2
    part_lines = slots * heads // 2
    line = lax.broadcasted_iota(jnp.int32, (part_lines, dim), 0)
    first = lax.rem(line, heads) == 0
    slot_of = [(line // heads + part * (slots // 2)).astype(jnp.float32).astype(jnp.bfloat16) for part in range(2)]

    def insert(posb_ref, fresh_ref, start, count, old, new):
        rows = pl.ds(pl.multiple_of(start, count), count)
        lines = pl.ds(pl.multiple_of(start * 2 * part_lines, count * 2 * part_lines), count * 2 * part_lines)
        posb_ref, fresh_ref, old, new = posb_ref.at[rows, :], fresh_ref.at[:, rows, :], old.at[lines, :], new.at[lines, :]
        for r in range(count):
            p = jnp.broadcast_to(posb_ref[r:r + 1, :], (part_lines, dim)).astype(jnp.bfloat16)
            h0 = jnp.broadcast_to(fresh_ref[0, r:r + 1, :], (part_lines, dim))
            h1 = jnp.broadcast_to(fresh_ref[1, r:r + 1, :], (part_lines, dim))
            fresh = jnp.where(first, h0, h1).astype(jnp.bfloat16)
            for part in range(2):
                at = slice((2 * r + part) * part_lines, (2 * r + part + 1) * part_lines)
                new[at, :] = jnp.where(slot_of[part] == p, fresh, old[at, :])

    return insert


def project_kernel(n_tp, slots, dim, pos_hbm, table_hbm, qg_hbm, kg_hbm, hid_ref, wq_ref, wk_ref, wv_ref, wo_ref, kc_ref, vc_ref,
                   q_ref, k_ref, posb_ref, wo_own, wo_in, kc_out, vc_out,
                   pos_ref, table_ref, qg_ref, kg_ref, hid, wqk, wv, vc_in, acc, vacc, cosb, sinb, e_mine, e_in,
                   in_sem, v_sem, e_send, e_recv, w_sem, s_sem, c_sem):
    t = lax.axis_index("tp")
    mate = t + 1 - 2 * lax.rem(t, 2)
    n_rows, width = hid_ref.shape
    local = wq_ref.shape[1]
    heads = local // dim
    cut = width // DEPTH_CUTS
    barrier = pltpu.get_barrier_semaphore()
    for off in range(1, n_tp):
        pl.semaphore_signal(barrier, inc=1, device_id={"tp": lax.rem(t + off, n_tp)}, device_id_type=MESH)

    loads = []
    for c in range(DEPTH_CUTS):
        at = pl.ds(c * cut, cut)
        loads.append([
            pltpu.make_async_copy(hid_ref.at[:, at], hid.at[c], in_sem.at[c, 0]),
            pltpu.make_async_copy(wq_ref.at[at, :], wqk.at[c, :, pl.ds(0, local)], in_sem.at[c, 1]),
            pltpu.make_async_copy(wk_ref.at[at, :], wqk.at[c, :, pl.ds(local, local)], in_sem.at[c, 2])])
    v_loads = [pltpu.make_async_copy(wv_ref.at[pl.ds(c * cut, cut), :], wv.at[c], v_sem.at[c]) for c in range(DEPTH_CUTS)]
    small = [pltpu.make_async_copy(src, dst, s_sem.at[i]) for i, (src, dst) in enumerate(
        ((pos_hbm, pos_ref), (table_hbm, table_ref), (qg_hbm, qg_ref), (kg_hbm, kg_ref)))]
    caches = [pltpu.make_async_copy(src, dst, c_sem.at[i]) for i, (src, dst) in enumerate(((kc_ref, kc_out), (vc_ref, vc_in), (wo_ref, wo_own)))]
    queue = loads + [v_loads, small, [caches[2]], [caches[1]], [caches[0]]]

    def issue(count):
        for group in queue[:count]:
            for copy in group:
                copy.start()
        del queue[:count]

    issue(IN_FLIGHT)
    w_copy = pltpu.make_async_remote_copy(wo_own, wo_in, w_sem.at[0], w_sem.at[1], device_id={"tp": mate}, device_id_type=MESH)
    lanes = e_mine.shape[1]
    blocks = n_rows // lanes
    def tables():
        for copy in small:
            copy.wait()
        lane = lax.broadcasted_iota(jnp.int32, (lanes, TABLE_ROWS), 1)
        which = jnp.where(lane < 3 * slots, lax.rem(lane, slots), -1).astype(jnp.float32)
        for b in range(blocks):
            at = slice(b * lanes, (b + 1) * lanes)
            column = jnp.broadcast_to(pos_ref[b:b + 1, :].astype(jnp.float32), (lanes, lanes)).T
            posb_ref[at, :] = column
            hot = jnp.where(which == column, 1.0, 0.0).astype(jnp.bfloat16)
            factors = jnp.dot(hot, table_ref[...], preferred_element_type=jnp.float32)
            cosb[at, :] = factors[:, :dim]
            sinb[at, :] = factors[:, dim:]

    for c in range(DEPTH_CUTS):
        for copy in loads[c]:
            copy.wait()
        issue(1)
        part = jnp.dot(hid[c], wqk[c], preferred_element_type=jnp.float32)
        if c == 0:
            acc[...] = part
        else:
            acc[...] += part

    ones = jnp.ones((8, local), jnp.bfloat16)
    nt = (((1,), (1,)), ((), ()))
    for i in range(2):
        rounded = acc[:, i * local:(i + 1) * local].astype(jnp.bfloat16).astype(jnp.float32)
        square = rounded * rounded
        high = jnp.minimum(square, float(jnp.finfo(jnp.bfloat16).max)).astype(jnp.bfloat16)
        low = (square - high.astype(jnp.float32)).astype(jnp.bfloat16)
        energy = (lax.dot_general(ones, high, nt, preferred_element_type=jnp.float32)
                  + lax.dot_general(ones, low, nt, preferred_element_type=jnp.float32))
        for b in range(blocks):
            e_mine[i * blocks + b:i * blocks + b + 1, :] = energy[0:1, b * lanes:(b + 1) * lanes]
    issue(len(queue))
    pl.semaphore_wait(barrier, n_tp - 1)
    sends = [pltpu.make_async_remote_copy(
        e_mine, e_in.at[off], e_send.at[off], e_recv.at[off],
        device_id={"tp": lax.rem(t + off, n_tp)}, device_id_type=MESH) for off in range(1, n_tp)]
    for copy in sends:
        copy.start()
    caches[2].wait()
    w_copy.start()
    tables()

    for c in range(DEPTH_CUTS):
        v_loads[c].wait()
        part = jnp.dot(hid[c], wv[c], preferred_element_type=jnp.float32)
        for h in range(heads):
            if c == 0:
                vacc[h] = part[:, h * dim:(h + 1) * dim]
            else:
                vacc[h] += part[:, h * dim:(h + 1) * dim]
    caches[1].wait()
    insert = inserter(slots, heads, dim)

    def insert_rows(i, carry):
        insert(posb_ref, vacc, i * INSERT_UNROLL, INSERT_UNROLL, vc_in, vc_out)
        return carry

    lax.fori_loop(0, n_rows // INSERT_UNROLL, insert_rows, 0)

    total = e_mine[...]
    for i, copy in enumerate(sends):
        copy.wait_recv()
        total = total + e_in[i + 1]
    inv = lax.rsqrt(total / width + NORM_EPS)
    for b in range(blocks):
        at = slice(b * lanes, (b + 1) * lanes)
        for i, (gain, out) in enumerate(((qg_ref, q_ref), (kg_ref, k_ref))):
            scale = jnp.broadcast_to(inv[i * blocks + b:i * blocks + b + 1, :], (lanes, lanes)).T
            for h in range(heads):
                cols = slice(h * dim, (h + 1) * dim)
                x = acc[at, i * local + h * dim:i * local + (h + 1) * dim].astype(jnp.bfloat16).astype(jnp.float32)
                x = (x * scale * gain[:, cols]).astype(jnp.bfloat16).astype(jnp.float32)
                x = (x * cosb[at, :] + pltpu.roll(x, dim // 2, 1) * sinb[at, :]).astype(jnp.bfloat16)
                if i == 0:
                    out[at, cols] = x
                else:
                    out[h, at, :] = x.astype(jnp.float32)
    for copy in sends:
        copy.wait_send()
    w_copy.wait()
    caches[0].wait()


def project_call(n_tp, hidden, w_q, w_k, w_v, w_o, q_gain, k_gain, positions, k_cache, v_cache):
    n_rows, width = hidden.shape
    local = w_q.shape[1]
    slots, dim = k_cache.shape[1], k_cache.shape[3]
    lanes = 128
    flat = (k_cache.size // dim, dim)
    in_hbm = lambda x: pltpu.with_memory_space_constraint(x, pltpu.HBM)
    cut = width // DEPTH_CUTS
    vmem, hbm = pl.BlockSpec(memory_space=pltpu.VMEM), pl.BlockSpec(memory_space=pltpu.HBM)
    return pl.pallas_call(
        functools.partial(project_kernel, n_tp, slots, dim),
        name="project",
        out_shape=[pltpu.VMEM((n_rows, local), jnp.bfloat16), pltpu.VMEM((local // dim, n_rows, dim), jnp.float32)]
        + [pltpu.VMEM((n_rows, lanes), jnp.float32), pltpu.VMEM(w_o.shape, jnp.bfloat16), pltpu.VMEM(w_o.shape, jnp.bfloat16)] + [pltpu.VMEM(flat, jnp.bfloat16)] * 2,
        in_specs=[hbm] * 11,
        out_specs=[vmem] * 7,
        scratch_shapes=[
            pltpu.VMEM((n_rows // lanes, lanes), jnp.int32),
            pltpu.VMEM((TABLE_ROWS, 2 * dim), jnp.bfloat16),
            pltpu.VMEM((1, local), jnp.float32),
            pltpu.VMEM((1, local), jnp.float32),
            pltpu.VMEM((DEPTH_CUTS, n_rows, cut), jnp.bfloat16),
            pltpu.VMEM((DEPTH_CUTS, cut, 2 * local), jnp.bfloat16),
            pltpu.VMEM((DEPTH_CUTS, cut, local), jnp.bfloat16),
            pltpu.VMEM(flat, jnp.bfloat16),
            pltpu.VMEM((n_rows, 2 * local), jnp.float32),
            pltpu.VMEM((local // dim, n_rows, dim), jnp.float32),
            pltpu.VMEM((n_rows, dim), jnp.float32),
            pltpu.VMEM((n_rows, dim), jnp.float32),
            pltpu.VMEM((2 * n_rows // lanes, lanes), jnp.float32),
            pltpu.VMEM((n_tp, 2 * n_rows // lanes, lanes), jnp.float32),
            pltpu.SemaphoreType.DMA((DEPTH_CUTS, 3)),
            pltpu.SemaphoreType.DMA((DEPTH_CUTS,)),
            pltpu.SemaphoreType.DMA((n_tp,)),
            pltpu.SemaphoreType.DMA((n_tp,)),
            pltpu.SemaphoreType.DMA((2,)),
            pltpu.SemaphoreType.DMA((4,)),
            pltpu.SemaphoreType.DMA((3,)),
        ],
        compiler_params=pltpu.CompilerParams(collective_id=1, has_side_effects=True, vmem_limit_bytes=40 * 2**20),
        cost_estimate=pl.CostEstimate(flops=6 * n_rows * width * local, bytes_accessed=2 * (n_rows * width + 3 * width * local), transcendentals=0),
    )(*map(in_hbm, (positions.reshape(n_rows // lanes, lanes), rope_table(slots, dim), q_gain, k_gain, hidden, w_q, w_k, w_v, w_o,
                    k_cache.reshape(flat), v_cache.reshape(flat))))


ROW_BLOCK = 256
INSERT_UNROLL = 16
GROUP = 8


def attend_kernel(slots, heads, q_ref, k_ref, posb_ref, kc_ref, vn_ref, o_ref, k_out, v_out, kn, k_sem, v_sem):
    n_rows = q_ref.shape[0]
    dim = q_ref.shape[1] // heads
    lines = slots * heads
    block = ROW_BLOCK
    v_copy = pltpu.make_async_copy(vn_ref, v_out, v_sem)
    v_copy.start()
    insert = inserter(slots, heads, dim)
    n_groups = block // GROUP
    wide = GROUP * lines
    m = lax.broadcasted_iota(jnp.int32, (heads * GROUP, wide), 0)
    n = lax.broadcasted_iota(jnp.int32, (heads * GROUP, wide), 1)
    own = (lax.rem(m, GROUP) == n // lines) & (m // GROUP == lax.rem(n, heads))
    slot = jnp.where(own, (lax.rem(n, lines) // heads).astype(jnp.float32), 1e9)
    shut = jnp.where(own, -1e30, -jnp.inf)

    def k_copy(i):
        at = pl.ds(pl.multiple_of(i * block * lines, block * lines), block * lines)
        return pltpu.make_async_copy(kn.at[at, :], k_out.at[at, :], k_sem.at[i])

    def fill(i, carry):
        for r in range(0, block, INSERT_UNROLL):
            insert(posb_ref, k_ref, i * block + r, INSERT_UNROLL, kc_ref, kn)
        k_copy(i).start()
        return carry

    lax.fori_loop(0, n_rows // block, fill, 0)

    def one(i, carry):
        scores = []
        for g in range(n_groups):
            rows = pl.ds(pl.multiple_of(i * block + g * GROUP, GROUP), GROUP)
            keys = kn[pl.ds(pl.multiple_of((i * n_groups + g) * wide, wide), wide), :]
            q = jnp.concatenate([q_ref[rows, h * dim:(h + 1) * dim] for h in range(heads)], axis=0)
            s = lax.dot_general(q, keys, (((1,), (1,)), ((), ())), preferred_element_type=jnp.float32) * dim ** -0.5
            at = jnp.concatenate([posb_ref[rows, :]] * heads, axis=0)
            at = jnp.concatenate([at] * (wide // at.shape[1]), axis=1)
            scores.append(jnp.where(slot <= at, s, shut))
        for g in range(n_groups):
            rows = pl.ds(pl.multiple_of(i * block + g * GROUP, GROUP), GROUP)
            values = vn_ref[pl.ds(pl.multiple_of((i * n_groups + g) * wide, wide), wide), :]
            s = scores[g]
            e = jnp.exp(s - jnp.max(s, axis=-1, keepdims=True))
            probs = (e / jnp.sum(e, axis=-1, keepdims=True)).astype(jnp.bfloat16)
            o = jnp.dot(probs, values, preferred_element_type=jnp.float32).astype(jnp.bfloat16)
            for h in range(heads):
                o_ref[rows, h * dim:(h + 1) * dim] = o[h * GROUP:(h + 1) * GROUP]
        return carry

    lax.fori_loop(0, n_rows // block, one, 0)
    for i in range(n_rows // block):
        k_copy(i).wait()
    v_copy.wait()


def attend_call(q, k, posb, k_cache, v_new, cache_shape):
    n_rows, slots, heads, dim = cache_shape
    flat = (n_rows * slots * heads, dim)
    vmem, hbm = pl.BlockSpec(memory_space=pltpu.VMEM), pl.BlockSpec(memory_space=pltpu.HBM)
    o, k_out, v_out = pl.pallas_call(
        functools.partial(attend_kernel, slots, heads),
        name="attend",
        out_shape=[pltpu.VMEM((n_rows, heads * dim), jnp.bfloat16),
                   pltpu.HBM(flat, jnp.bfloat16), pltpu.HBM(flat, jnp.bfloat16)],
        in_specs=[vmem] * 5,
        out_specs=[vmem, hbm, hbm],
        scratch_shapes=[pltpu.VMEM(flat, jnp.bfloat16), pltpu.SemaphoreType.DMA((n_rows // ROW_BLOCK,)), pltpu.SemaphoreType.DMA],
        compiler_params=pltpu.CompilerParams(vmem_limit_bytes=24 * 2**20),
    )(q, k, posb, k_cache, v_new)
    return o, k_out.reshape(cache_shape), v_out.reshape(cache_shape)


SUBS = 2
LAG = 0
RS_PLAN = 2
AG_PLAN = 0
SHARE_TILE = 4096


def rs_plan_of(far):
    if RS_PLAN == 0:
        return [[(t, "L")] + ([(t + 1, "S")] if t + 1 < far else []) for t in range(far)]
    if RS_PLAN == 1:
        return [[(0, "L")]] + [[(t, "F")] for t in range(1, far)]
    if RS_PLAN == 3:
        return [[(0, "L"), (1, "S")], [(1, "L")]] + [[(t, "F")] for t in range(2, far - 1)] + [[(far - 1, "L"), (far - 1, "S")]]
    return [[(0, "L"), (1, "S")], [(1, "L")]] + [[(t, "F")] for t in range(2, far)]


def ag_plan_of(far):
    if AG_PLAN == 0:
        return [[(t, "L")] + ([(t, "S")] if t + 1 < far else []) for t in range(far)]
    if AG_PLAN == 2:
        return [[(t, "F")] if t < far - 2 else [(t, "L")] + ([(t, "S")] if t + 1 < far else []) for t in range(far)]
    if AG_PLAN == 3:
        return [[(t, "F")] if t < 1 else [(t, "L")] + ([(t, "S")] if t + 1 < far else []) for t in range(far)]
    return [[(t, "F")] for t in range(far - 1)] + [[(far - 1, "L")]]


def finish_kernel(n_tp, o_ref, w_ref, w_in, hid_ref, gain_ref, out_ref,
                  o_in, lhs, lhs_in, hid, share, rs_in, rs_out,
                  x_send, x_recv, h_sem, rs_send, rs_recv, ag_send, ag_recv, d2d_send, d2d_recv):
    nz = n_tp // 2
    t = lax.axis_index("tp")
    z, k = t // 2, lax.rem(t, 2)
    up, down, mate = lax.rem(t + 2, n_tp), lax.rem(t + n_tp - 2, n_tp), z * 2 + 1 - k
    n_rows, width = out_ref.shape
    half_rows = n_rows // 2
    rows = half_rows // nz
    sub = rows // SUBS
    half = width // 2
    far = nz // 2
    chunk_of = lambda j: lax.rem(z + nz + j, nz)
    out_row = lambda j, s: pl.multiple_of(k * half_rows + chunk_of(j) * rows + s * sub, sub)
    cols = (pl.ds(0, half), pl.ds(half, half))
    target = (up, down)
    long_half = (0, 1)

    barrier = pltpu.get_barrier_semaphore()
    for peer in (up, down, mate):
        pl.semaphore_signal(barrier, inc=1, device_id={"tp": peer}, device_id_type=MESH)
    hid_copy = pltpu.make_async_copy(hid_ref.at[pl.ds(pl.multiple_of(k * half_rows + z * rows, rows), rows), :], hid, h_sem)
    hid_copy.start()
    pl.semaphore_wait(barrier, 3)

    o_copy = pltpu.make_async_remote_copy(
        o_ref.at[pl.ds(pl.multiple_of((1 - k) * half_rows, half_rows), half_rows), :], o_in,
        x_send, x_recv, device_id={"tp": mate}, device_id_type=MESH)
    o_copy.start()

    order = sorted(range(nz), key=lambda j: -min(j, nz - j))
    place = {j: i for i, j in enumerate(order)}
    def gather(first, last, ref, base, out):
        for j in order[first:last]:
            at = slice(place[j] * rows, (place[j] + 1) * rows)
            out[at, :] = ref[pl.ds(pl.multiple_of(base + chunk_of(j) * rows, rows), rows), :]

    def add_shares(first, last, lhs_ref, weight, fresh):
        def one(c, carry):
            at = pl.ds(pl.multiple_of(c * SHARE_TILE, SHARE_TILE), SHARE_TILE)
            part = jnp.dot(lhs_ref[first * rows:last * rows, :], weight[:, at], preferred_element_type=jnp.float32)
            if fresh:
                share[first * rows:last * rows, at] = part
            else:
                share[first * rows:last * rows, at] += part
            return carry

        lax.fori_loop(0, width // SHARE_TILE, one, 0)

    gather(0, nz, o_ref, k * half_rows, lhs)
    add_shares(0, 3, lhs, w_ref, True)
    o_copy.wait_recv()
    gather(0, 3, o_in, 0, lhs_in)

    def halves(d, kind):
        return {"L": (d,), "S": (1 - d,), "F": (0, 1)}[kind]

    def span(d, kind):
        return pl.ds(0, width) if kind == "F" else pl.ds(halves(d, kind)[0] * half, half)

    rs_plan, ag_plan = rs_plan_of(far), ag_plan_of(far)
    slots = {}
    for stage_list in rs_plan:
        for g, kind in stage_list:
            for d in range(2):
                for s in range(SUBS):
                    slots[d, g, kind, s] = len(slots)
    ag_slots = {}
    for stage_list in ag_plan:
        for g, kind in stage_list:
            for d in range(2):
                for s in range(SUBS):
                    ag_slots[d, g, kind, s] = len(ag_slots)

    def page(d, g, s):
        return (d * far + g) * SUBS + s

    def rs_message(d, g, kind, s):
        i = slots[d, g, kind, s]
        at = span(d, kind)
        return pltpu.make_async_remote_copy(
            rs_out.at[page(d, g, s), :, at], rs_in.at[page(d, g, s), :, at], rs_send.at[i], rs_recv.at[i],
            device_id={"tp": target[d]}, device_id_type=MESH)

    def piece(j, c, s):
        return share[place[j % nz] * rows + s * sub:place[j % nz] * rows + (s + 1) * sub, c * half:(c + 1) * half]

    arrived = set()

    def received(d, g, c, s):
        for kind in ("L", "S", "F"):
            if (d, g, kind, s) in slots and c in halves(d, kind) and (d, g, kind, s) not in arrived:
                rs_message(d, g, kind, s).wait_recv()
                arrived.add((d, g, kind, s))
        return rs_in[page(d, g, s), :, c * half:(c + 1) * half].astype(jnp.float32)

    def rs_step(d, g, kind, s):
        j = far - g if d == 0 else g - far
        for c in halves(d, kind):
            value = piece(j, c, s)
            if g > (0 if c == d else 1):
                value = value + received(d, g - 1, c, s)
            rs_out[page(d, g, s), :, c * half:(c + 1) * half] = value.astype(jnp.bfloat16)
        rs_message(d, g, kind, s).start()

    def ag_message(d, g, kind, s, behind):
        here = out_ref.at[pl.ds(out_row(-behind if d == 0 else behind, s), sub), span(d, kind)]
        i = ag_slots[d, g, kind, s]
        return pltpu.make_async_remote_copy(
            here, here, ag_send.at[i], ag_recv.at[i], device_id={"tp": target[d]}, device_id_type=MESH)

    d2d = []

    def d2d_start(j, at, s):
        here = out_ref.at[pl.ds(out_row(j, s), sub), at]
        i = len(d2d)
        copy = pltpu.make_async_remote_copy(here, here, d2d_send.at[i], d2d_recv.at[i], device_id={"tp": mate}, device_id_type=MESH)
        copy.start()
        d2d.append((j, at, s))

    def finish(s):
        total = []
        for c in range(2):
            acc = piece(0, c, s)
            for d in range(2):
                acc = acc + received(d, far - 1, c, s)
            share[place[0] * rows + s * sub:place[0] * rows + (s + 1) * sub, c * half:(c + 1) * half] = acc
            total.append(jnp.sum(acc * acc, axis=-1, keepdims=True))
        inv = lax.rsqrt((total[0] + total[1]) / width + NORM_EPS)
        for c in range(2):
            at = slice(c * half, (c + 1) * half)
            normed = piece(0, c, s) * inv * gain_ref[:, at]
            out_ref[pl.ds(out_row(0, s), sub), at] = (hid[s * sub:(s + 1) * sub, at].astype(jnp.float32) + normed).astype(jnp.bfloat16)
        for g, kind in ag_plan[0]:
            for d in range(2):
                ag_message(d, g, kind, s, 0).start()
        d2d_start(0, pl.ds(0, width), s)

    def ag_step(t, s):
        for g, kind in ag_plan[t - 1]:
            for d in range(2):
                ag_message(d, g, kind, s, g + 1).wait_recv()
                if t < len(ag_plan):
                    for g_next, kind_next in ag_plan[t]:
                        if set(halves(d, kind_next)) <= set(halves(d, kind)):
                            ag_message(d, g_next, kind_next, s, g + 1).start()
                d2d_start(-(g + 1) if d == 0 else g + 1, span(d, kind), s)

    def stage(t, s):
        if t < far:
            for g, kind in rs_plan[t]:
                for d in range(2):
                    rs_step(d, g, kind, s)
        elif t == far:
            if s == 0:
                hid_copy.wait()
            finish(s)
        else:
            ag_step(t - far, s)

    add_shares(0, 3, lhs_in, w_in, False)
    last_stage = far + len(ag_plan)
    for slot in range(last_stage + 1 + LAG * (SUBS - 1)):
        if slot == 1:
            gather(3, nz, o_in, 0, lhs_in)
            add_shares(3, nz, lhs, w_ref, True)
            add_shares(3, nz, lhs_in, w_in, False)
        for s in range(SUBS):
            t = slot - LAG * s
            if 0 <= t <= last_stage:
                stage(t, s)

    o_copy.wait_send()
    for d, g, kind, s in slots:
        rs_message(d, g, kind, s).wait_send()
    for d, g, kind, s in ag_slots:
        ag_message(d, g, kind, s, g).wait_send()
    for i, (j, at, s) in enumerate(d2d):
        here = out_ref.at[pl.ds(out_row(j, s), sub), at]
        there = out_ref.at[pl.ds(pl.multiple_of((1 - k) * half_rows + chunk_of(j) * rows + s * sub, sub), sub), at]
        copy = pltpu.make_async_remote_copy(here, there, d2d_send.at[i], d2d_recv.at[i], device_id={"tp": mate}, device_id_type=MESH)
        copy.wait_send()
        copy.wait_recv()


def finish_call(n_tp, attn, w_own, w_mate, hidden, gain):
    n_rows, width = hidden.shape
    depth = w_own.shape[0]
    nz = n_tp // 2
    half_rows, rows = n_rows // 2, n_rows // n_tp
    sub = rows // SUBS
    n_msg = 2 * SUBS * (nz - 1)
    vmem = pl.BlockSpec(memory_space=pltpu.VMEM)
    return pl.pallas_call(
        functools.partial(finish_kernel, n_tp),
        name="finish",
        out_shape=pltpu.VMEM((n_rows, width), jnp.bfloat16) if OUT_VMEM else jax.ShapeDtypeStruct((n_rows, width), jnp.bfloat16),
        in_specs=[vmem, vmem, vmem, pl.BlockSpec(memory_space=pltpu.HBM), vmem],
        out_specs=vmem,
        scratch_shapes=[
            pltpu.VMEM((half_rows, depth), jnp.bfloat16),
            pltpu.VMEM((half_rows, depth), jnp.bfloat16),
            pltpu.VMEM((half_rows, depth), jnp.bfloat16),
            pltpu.VMEM((rows, width), jnp.bfloat16),
            pltpu.VMEM((half_rows, width), jnp.float32),
            pltpu.VMEM((nz * SUBS, sub, width), jnp.bfloat16),
            pltpu.VMEM((nz * SUBS, sub, width), jnp.bfloat16),
            pltpu.SemaphoreType.DMA,
            pltpu.SemaphoreType.DMA,
            pltpu.SemaphoreType.DMA,
            pltpu.SemaphoreType.DMA((n_msg,)),
            pltpu.SemaphoreType.DMA((n_msg,)),
            pltpu.SemaphoreType.DMA((n_msg,)),
            pltpu.SemaphoreType.DMA((n_msg,)),
            pltpu.SemaphoreType.DMA((2 * SUBS * nz,)),
            pltpu.SemaphoreType.DMA((2 * SUBS * nz,)),
        ],
        compiler_params=pltpu.CompilerParams(collective_id=0, has_side_effects=True, vmem_limit_bytes=40 * 2**20),
    )(attn, w_own, w_mate, pltpu.with_memory_space_constraint(hidden, pltpu.HBM), gain)


def solution(mesh):
    def local_step(hidden, w_q, w_k, w_v, w_o, q_norm_w, k_norm_w, post_norm_w, k_cache, v_cache, positions):
        n_tp = mesh.shape["tp"]
        q_rot, k_rot, posb, w_own, w_mate, k_near, v_near = project_call(
            n_tp, hidden, w_q, w_k, w_v, w_o, q_norm_w[None, :], k_norm_w[None, :], positions, k_cache, v_cache)
        attn, k_new, v_new = attend_call(q_rot, k_rot, posb, k_near, v_near, k_cache.shape)
        hidden_out = finish_call(n_tp, attn, w_own, w_mate, hidden, post_norm_w[None, :])
        return hidden_out, k_new, v_new

    cache_spec = P('dp', None, 'tp', None)
    return jax.shard_map(local_step, mesh=mesh, in_specs=(P('dp', None), P(None, 'tp'), P(None, 'tp'), P(None, 'tp'), P('tp', None), P('tp'), P('tp'), P(None), cache_spec, cache_spec, P('dp')), out_specs=(P('dp', None), cache_spec, cache_spec), check_vma=False)
```

```python
import functools

import jax
import jax.numpy as jnp
import numpy as np
from jax import lax
from jax.experimental import pallas as pl
from jax.experimental.pallas import tpu as pltpu
from jax.sharding import PartitionSpec as P

NORM_EPS = 1e-6
ROPE_BASE = 500000.0
OUT_VMEM = True


MESH = pl.DeviceIdType.MESH
DEPTH_CUTS = 4
IN_FLIGHT = 4
TABLE_ROWS = 128


def rope_table(slots, dim):
    half = dim // 2
    inv_freq = np.float32(ROPE_BASE) ** (np.float32(-2.0) * np.arange(half, dtype=np.float32) / np.float32(dim))
    angles = (np.arange(slots, dtype=np.float32)[:, None] * inv_freq.astype(np.float32)[None, :]).astype(np.float64)
    cos_tab, sin_tab = np.cos(angles), np.sin(angles)
    rest = np.concatenate([cos_tab, cos_tab, -sin_tab, sin_tab], axis=1).astype(np.float32)
    out = np.zeros((TABLE_ROWS, 2 * dim), np.float32)
    for part in range(3):
        high = rest.astype(jnp.bfloat16).astype(np.float32)
        out[part * slots:(part + 1) * slots] = high
        rest = rest - high
    return jnp.asarray(out, dtype=jnp.bfloat16)


def inserter(slots, heads, dim):
    assert heads == 2
    part_lines = slots * heads // 2
    line = lax.broadcasted_iota(jnp.int32, (part_lines, dim), 0)
    first = lax.rem(line, heads) == 0
    slot_of = [(line // heads + part * (slots // 2)).astype(jnp.float32).astype(jnp.bfloat16) for part in range(2)]

    def insert(posb_ref, fresh_ref, start, count, old, new):
        rows = pl.ds(pl.multiple_of(start, count), count)
        lines = pl.ds(pl.multiple_of(start * 2 * part_lines, count * 2 * part_lines), count * 2 * part_lines)
        posb_ref, fresh_ref, old, new = posb_ref.at[rows, :], fresh_ref.at[:, rows, :], old.at[lines, :], new.at[lines, :]
        for r in range(count):
            p = jnp.broadcast_to(posb_ref[r:r + 1, :], (part_lines, dim)).astype(jnp.bfloat16)
            h0 = jnp.broadcast_to(fresh_ref[0, r:r + 1, :], (part_lines, dim))
            h1 = jnp.broadcast_to(fresh_ref[1, r:r + 1, :], (part_lines, dim))
            fresh = jnp.where(first, h0, h1).astype(jnp.bfloat16)
            for part in range(2):
                at = slice((2 * r + part) * part_lines, (2 * r + part + 1) * part_lines)
                new[at, :] = jnp.where(slot_of[part] == p, fresh, old[at, :])

    return insert


def project_kernel(n_tp, slots, dim, pos_hbm, table_hbm, qg_hbm, kg_hbm, hid_ref, wq_ref, wk_ref, wv_ref, wo_ref, kc_ref, vc_ref,
                   q_ref, k_ref, posb_ref, wo_own, wo_in, kc_out, vc_out,
                   pos_ref, table_ref, qg_ref, kg_ref, hid, wqk, wv, vc_in, acc, vacc, cosb, sinb, e_mine, e_in,
                   in_sem, v_sem, e_send, e_recv, w_sem, s_sem, c_sem):
    t = lax.axis_index("tp")
    mate = t + 1 - 2 * lax.rem(t, 2)
    n_rows, width = hid_ref.shape
    local = wq_ref.shape[1]
    heads = local // dim
    cut = width // DEPTH_CUTS
    barrier = pltpu.get_barrier_semaphore()
    for off in range(1, n_tp):
        pl.semaphore_signal(barrier, inc=1, device_id={"tp": lax.rem(t + off, n_tp)}, device_id_type=MESH)

    loads = []
    for c in range(DEPTH_CUTS):
        at = pl.ds(c * cut, cut)
        loads.append([
            pltpu.make_async_copy(hid_ref.at[:, at], hid.at[c], in_sem.at[c, 0]),
            pltpu.make_async_copy(wq_ref.at[at, :], wqk.at[c, :, pl.ds(0, local)], in_sem.at[c, 1]),
            pltpu.make_async_copy(wk_ref.at[at, :], wqk.at[c, :, pl.ds(local, local)], in_sem.at[c, 2])])
    v_loads = [pltpu.make_async_copy(wv_ref.at[pl.ds(c * cut, cut), :], wv.at[c], v_sem.at[c]) for c in range(DEPTH_CUTS)]
    small = [pltpu.make_async_copy(src, dst, s_sem.at[i]) for i, (src, dst) in enumerate(
        ((pos_hbm, pos_ref), (table_hbm, table_ref), (qg_hbm, qg_ref), (kg_hbm, kg_ref)))]
    caches = [pltpu.make_async_copy(src, dst, c_sem.at[i]) for i, (src, dst) in enumerate(((kc_ref, kc_out), (vc_ref, vc_in), (wo_ref, wo_own)))]
    queue = loads + [v_loads, small, [caches[2]], [caches[1]], [caches[0]]]

    def issue(count):
        for group in queue[:count]:
            for copy in group:
                copy.start()
        del queue[:count]

    issue(IN_FLIGHT)
    w_copy = pltpu.make_async_remote_copy(wo_own, wo_in, w_sem.at[0], w_sem.at[1], device_id={"tp": mate}, device_id_type=MESH)
    lanes = e_mine.shape[1]
    blocks = n_rows // lanes
    def tables():
        for copy in small:
            copy.wait()
        lane = lax.broadcasted_iota(jnp.int32, (lanes, TABLE_ROWS), 1)
        which = jnp.where(lane < 3 * slots, lax.rem(lane, slots), -1).astype(jnp.float32)
        for b in range(blocks):
            at = slice(b * lanes, (b + 1) * lanes)
            column = jnp.broadcast_to(pos_ref[b:b + 1, :].astype(jnp.float32), (lanes, lanes)).T
            posb_ref[at, :] = column
            hot = jnp.where(which == column, 1.0, 0.0).astype(jnp.bfloat16)
            factors = jnp.dot(hot, table_ref[...], preferred_element_type=jnp.float32)
            cosb[at, :] = factors[:, :dim]
            sinb[at, :] = factors[:, dim:]

    for c in range(DEPTH_CUTS):
        for copy in loads[c]:
            copy.wait()
        issue(1)
        part = jnp.dot(hid[c], wqk[c], preferred_element_type=jnp.float32)
        if c == 0:
            acc[...] = part
        else:
            acc[...] += part

    ones = jnp.ones((8, local), jnp.bfloat16)
    nt = (((1,), (1,)), ((), ()))
    for i in range(2):
        rounded = acc[:, i * local:(i + 1) * local].astype(jnp.bfloat16).astype(jnp.float32)
        square = rounded * rounded
        high = jnp.minimum(square, float(jnp.finfo(jnp.bfloat16).max)).astype(jnp.bfloat16)
        low = (square - high.astype(jnp.float32)).astype(jnp.bfloat16)
        energy = (lax.dot_general(ones, high, nt, preferred_element_type=jnp.float32)
                  + lax.dot_general(ones, low, nt, preferred_element_type=jnp.float32))
        for b in range(blocks):
            e_mine[i * blocks + b:i * blocks + b + 1, :] = energy[0:1, b * lanes:(b + 1) * lanes]
    issue(len(queue))
    pl.semaphore_wait(barrier, n_tp - 1)
    sends = [pltpu.make_async_remote_copy(
        e_mine, e_in.at[off], e_send.at[off], e_recv.at[off],
        device_id={"tp": lax.rem(t + off, n_tp)}, device_id_type=MESH) for off in range(1, n_tp)]
    for copy in sends:
        copy.start()
    caches[2].wait()
    w_copy.start()
    tables()

    for c in range(DEPTH_CUTS):
        v_loads[c].wait()
        part = jnp.dot(hid[c], wv[c], preferred_element_type=jnp.float32)
        for h in range(heads):
            if c == 0:
                vacc[h] = part[:, h * dim:(h + 1) * dim]
            else:
                vacc[h] += part[:, h * dim:(h + 1) * dim]
    caches[1].wait()
    insert = inserter(slots, heads, dim)

    def insert_rows(i, carry):
        insert(posb_ref, vacc, i * INSERT_UNROLL, INSERT_UNROLL, vc_in, vc_out)
        return carry

    lax.fori_loop(0, n_rows // INSERT_UNROLL, insert_rows, 0)

    total = e_mine[...]
    for i, copy in enumerate(sends):
        copy.wait_recv()
        total = total + e_in[i + 1]
    inv = lax.rsqrt(total / width + NORM_EPS)
    for b in range(blocks):
        at = slice(b * lanes, (b + 1) * lanes)
        for i, (gain, out) in enumerate(((qg_ref, q_ref), (kg_ref, k_ref))):
            scale = jnp.broadcast_to(inv[i * blocks + b:i * blocks + b + 1, :], (lanes, lanes)).T
            for h in range(heads):
                cols = slice(h * dim, (h + 1) * dim)
                x = acc[at, i * local + h * dim:i * local + (h + 1) * dim].astype(jnp.bfloat16).astype(jnp.float32)
                x = (x * scale * gain[:, cols]).astype(jnp.bfloat16).astype(jnp.float32)
                x = (x * cosb[at, :] + pltpu.roll(x, dim // 2, 1) * sinb[at, :]).astype(jnp.bfloat16)
                if i == 0:
                    out[at, cols] = x
                else:
                    out[h, at, :] = x.astype(jnp.float32)
    for copy in sends:
        copy.wait_send()
    w_copy.wait()
    caches[0].wait()


def project_call(n_tp, hidden, w_q, w_k, w_v, w_o, q_gain, k_gain, positions, k_cache, v_cache):
    n_rows, width = hidden.shape
    local = w_q.shape[1]
    slots, dim = k_cache.shape[1], k_cache.shape[3]
    lanes = 128
    flat = (k_cache.size // dim, dim)
    in_hbm = lambda x: pltpu.with_memory_space_constraint(x, pltpu.HBM)
    cut = width // DEPTH_CUTS
    vmem, hbm = pl.BlockSpec(memory_space=pltpu.VMEM), pl.BlockSpec(memory_space=pltpu.HBM)
    return pl.pallas_call(
        functools.partial(project_kernel, n_tp, slots, dim),
        name="project",
        out_shape=[pltpu.VMEM((n_rows, local), jnp.bfloat16), pltpu.VMEM((local // dim, n_rows, dim), jnp.float32)]
        + [pltpu.VMEM((n_rows, lanes), jnp.float32), pltpu.VMEM(w_o.shape, jnp.bfloat16), pltpu.VMEM(w_o.shape, jnp.bfloat16)] + [pltpu.VMEM(flat, jnp.bfloat16)] * 2,
        in_specs=[hbm] * 11,
        out_specs=[vmem] * 7,
        scratch_shapes=[
            pltpu.VMEM((n_rows // lanes, lanes), jnp.int32),
            pltpu.VMEM((TABLE_ROWS, 2 * dim), jnp.bfloat16),
            pltpu.VMEM((1, local), jnp.float32),
            pltpu.VMEM((1, local), jnp.float32),
            pltpu.VMEM((DEPTH_CUTS, n_rows, cut), jnp.bfloat16),
            pltpu.VMEM((DEPTH_CUTS, cut, 2 * local), jnp.bfloat16),
            pltpu.VMEM((DEPTH_CUTS, cut, local), jnp.bfloat16),
            pltpu.VMEM(flat, jnp.bfloat16),
            pltpu.VMEM((n_rows, 2 * local), jnp.float32),
            pltpu.VMEM((local // dim, n_rows, dim), jnp.float32),
            pltpu.VMEM((n_rows, dim), jnp.float32),
            pltpu.VMEM((n_rows, dim), jnp.float32),
            pltpu.VMEM((2 * n_rows // lanes, lanes), jnp.float32),
            pltpu.VMEM((n_tp, 2 * n_rows // lanes, lanes), jnp.float32),
            pltpu.SemaphoreType.DMA((DEPTH_CUTS, 3)),
            pltpu.SemaphoreType.DMA((DEPTH_CUTS,)),
            pltpu.SemaphoreType.DMA((n_tp,)),
            pltpu.SemaphoreType.DMA((n_tp,)),
            pltpu.SemaphoreType.DMA((2,)),
            pltpu.SemaphoreType.DMA((4,)),
            pltpu.SemaphoreType.DMA((3,)),
        ],
        compiler_params=pltpu.CompilerParams(collective_id=1, has_side_effects=True, vmem_limit_bytes=40 * 2**20),
        cost_estimate=pl.CostEstimate(flops=6 * n_rows * width * local, bytes_accessed=2 * (n_rows * width + 3 * width * local), transcendentals=0),
    )(*map(in_hbm, (positions.reshape(n_rows // lanes, lanes), rope_table(slots, dim), q_gain, k_gain, hidden, w_q, w_k, w_v, w_o,
                    k_cache.reshape(flat), v_cache.reshape(flat))))


ROW_BLOCK = 256
INSERT_UNROLL = 16
GROUP = 8


def attend_kernel(slots, heads, q_ref, k_ref, posb_ref, kc_ref, vn_ref, o_ref, k_out, v_out, kn, k_sem, v_sem):
    n_rows = q_ref.shape[0]
    dim = q_ref.shape[1] // heads
    lines = slots * heads
    block = ROW_BLOCK
    v_copy = pltpu.make_async_copy(vn_ref, v_out, v_sem)
    v_copy.start()
    insert = inserter(slots, heads, dim)
    n_groups = block // GROUP
    wide = GROUP * lines
    m = lax.broadcasted_iota(jnp.int32, (heads * GROUP, wide), 0)
    n = lax.broadcasted_iota(jnp.int32, (heads * GROUP, wide), 1)
    own = (lax.rem(m, GROUP) == n // lines) & (m // GROUP == lax.rem(n, heads))
    slot = jnp.where(own, (lax.rem(n, lines) // heads).astype(jnp.float32), 1e9)
    shut = jnp.where(own, -1e30, -jnp.inf)

    def k_copy(i):
        at = pl.ds(pl.multiple_of(i * block * lines, block * lines), block * lines)
        return pltpu.make_async_copy(kn.at[at, :], k_out.at[at, :], k_sem.at[i])

    def fill(i, carry):
        for r in range(0, block, INSERT_UNROLL):
            insert(posb_ref, k_ref, i * block + r, INSERT_UNROLL, kc_ref, kn)
        k_copy(i).start()
        return carry

    lax.fori_loop(0, n_rows // block, fill, 0)

    def one(i, carry):
        scores = []
        for g in range(n_groups):
            rows = pl.ds(pl.multiple_of(i * block + g * GROUP, GROUP), GROUP)
            keys = kn[pl.ds(pl.multiple_of((i * n_groups + g) * wide, wide), wide), :]
            q = jnp.concatenate([q_ref[rows, h * dim:(h + 1) * dim] for h in range(heads)], axis=0)
            s = lax.dot_general(q, keys, (((1,), (1,)), ((), ())), preferred_element_type=jnp.float32) * dim ** -0.5
            at = jnp.concatenate([posb_ref[rows, :]] * heads, axis=0)
            at = jnp.concatenate([at] * (wide // at.shape[1]), axis=1)
            scores.append(jnp.where(slot <= at, s, shut))
        for g in range(n_groups):
            rows = pl.ds(pl.multiple_of(i * block + g * GROUP, GROUP), GROUP)
            values = vn_ref[pl.ds(pl.multiple_of((i * n_groups + g) * wide, wide), wide), :]
            s = scores[g]
            e = jnp.exp(s - jnp.max(s, axis=-1, keepdims=True))
            probs = (e / jnp.sum(e, axis=-1, keepdims=True)).astype(jnp.bfloat16)
            o = jnp.dot(probs, values, preferred_element_type=jnp.float32).astype(jnp.bfloat16)
            for h in range(heads):
                o_ref[rows, h * dim:(h + 1) * dim] = o[h * GROUP:(h + 1) * GROUP]
        return carry

    lax.fori_loop(0, n_rows // block, one, 0)
    for i in range(n_rows // block):
        k_copy(i).wait()
    v_copy.wait()


def attend_call(q, k, posb, k_cache, v_new, cache_shape):
    n_rows, slots, heads, dim = cache_shape
    flat = (n_rows * slots * heads, dim)
    vmem, hbm = pl.BlockSpec(memory_space=pltpu.VMEM), pl.BlockSpec(memory_space=pltpu.HBM)
    o, k_out, v_out = pl.pallas_call(
        functools.partial(attend_kernel, slots, heads),
        name="attend",
        out_shape=[pltpu.VMEM((n_rows, heads * dim), jnp.bfloat16),
                   pltpu.HBM(flat, jnp.bfloat16), pltpu.HBM(flat, jnp.bfloat16)],
        in_specs=[vmem] * 5,
        out_specs=[vmem, hbm, hbm],
        scratch_shapes=[pltpu.VMEM(flat, jnp.bfloat16), pltpu.SemaphoreType.DMA((n_rows // ROW_BLOCK,)), pltpu.SemaphoreType.DMA],
        compiler_params=pltpu.CompilerParams(vmem_limit_bytes=24 * 2**20),
    )(q, k, posb, k_cache, v_new)
    return o, k_out.reshape(cache_shape), v_out.reshape(cache_shape)


SUBS = 2
LAG = 0
RS_PLAN = 4
AG_PLAN = 0
SHARE_TILE = 4096


def rs_plan_of(far):
    if RS_PLAN == 0:
        return [[(t, "L")] + ([(t + 1, "S")] if t + 1 < far else []) for t in range(far)]
    if RS_PLAN == 1:
        return [[(0, "L")]] + [[(t, "F")] for t in range(1, far)]
    if RS_PLAN == 3:
        return [[(0, "L"), (1, "S")], [(1, "L")]] + [[(t, "F")] for t in range(2, far - 1)] + [[(far - 1, "L"), (far - 1, "S")]]
    if RS_PLAN == 4:
        return [[(0, "L")], [(1, "S"), (1, "L")]] + [[(t, "F")] for t in range(2, far)]
    return [[(0, "L"), (1, "S")], [(1, "L")]] + [[(t, "F")] for t in range(2, far)]


def ag_plan_of(far):
    if AG_PLAN == 0:
        return [[(t, "L")] + ([(t, "S")] if t + 1 < far else []) for t in range(far)]
    if AG_PLAN == 2:
        return [[(t, "F")] if t < far - 2 else [(t, "L")] + ([(t, "S")] if t + 1 < far else []) for t in range(far)]
    if AG_PLAN == 3:
        return [[(t, "F")] if t < 1 else [(t, "L")] + ([(t, "S")] if t + 1 < far else []) for t in range(far)]
    return [[(t, "F")] for t in range(far - 1)] + [[(far - 1, "L")]]


def finish_kernel(n_tp, o_ref, w_ref, w_in, hid_ref, gain_ref, out_ref,
                  o_in, lhs, lhs_in, hid, share, rs_in, rs_out,
                  x_send, x_recv, h_sem, rs_send, rs_recv, ag_send, ag_recv, d2d_send, d2d_recv):
    nz = n_tp // 2
    t = lax.axis_index("tp")
    z, k = t // 2, lax.rem(t, 2)
    up, down, mate = lax.rem(t + 2, n_tp), lax.rem(t + n_tp - 2, n_tp), z * 2 + 1 - k
    n_rows, width = out_ref.shape
    half_rows = n_rows // 2
    rows = half_rows // nz
    sub = rows // SUBS
    half = width // 2
    far = nz // 2
    chunk_of = lambda j: lax.rem(z + nz + j, nz)
    out_row = lambda j, s: pl.multiple_of(k * half_rows + chunk_of(j) * rows + s * sub, sub)
    cols = (pl.ds(0, half), pl.ds(half, half))
    target = (up, down)
    long_half = (0, 1)

    barrier = pltpu.get_barrier_semaphore()
    for peer in (up, down, mate):
        pl.semaphore_signal(barrier, inc=1, device_id={"tp": peer}, device_id_type=MESH)
    hid_copy = pltpu.make_async_copy(hid_ref.at[pl.ds(pl.multiple_of(k * half_rows + z * rows, rows), rows), :], hid, h_sem)
    hid_copy.start()
    pl.semaphore_wait(barrier, 3)

    o_copy = pltpu.make_async_remote_copy(
        o_ref.at[pl.ds(pl.multiple_of((1 - k) * half_rows, half_rows), half_rows), :], o_in,
        x_send, x_recv, device_id={"tp": mate}, device_id_type=MESH)
    o_copy.start()

    order = sorted(range(nz), key=lambda j: -min(j, nz - j))
    place = {j: i for i, j in enumerate(order)}
    def gather(first, last, ref, base, out):
        for j in order[first:last]:
            at = slice(place[j] * rows, (place[j] + 1) * rows)
            out[at, :] = ref[pl.ds(pl.multiple_of(base + chunk_of(j) * rows, rows), rows), :]

    def add_shares(first, last, lhs_ref, weight, fresh):
        def one(c, carry):
            at = pl.ds(pl.multiple_of(c * SHARE_TILE, SHARE_TILE), SHARE_TILE)
            part = jnp.dot(lhs_ref[first * rows:last * rows, :], weight[:, at], preferred_element_type=jnp.float32)
            if fresh:
                share[first * rows:last * rows, at] = part
            else:
                share[first * rows:last * rows, at] += part
            return carry

        lax.fori_loop(0, width // SHARE_TILE, one, 0)

    gather(0, nz, o_ref, k * half_rows, lhs)
    add_shares(0, 3, lhs, w_ref, True)
    o_copy.wait_recv()
    gather(0, 3, o_in, 0, lhs_in)

    def halves(d, kind):
        return {"L": (d,), "S": (1 - d,), "F": (0, 1)}[kind]

    def span(d, kind):
        return pl.ds(0, width) if kind == "F" else pl.ds(halves(d, kind)[0] * half, half)

    rs_plan, ag_plan = rs_plan_of(far), ag_plan_of(far)
    slots = {}
    for stage_list in rs_plan:
        for g, kind in stage_list:
            for d in range(2):
                for s in range(SUBS):
                    slots[d, g, kind, s] = len(slots)
    ag_slots = {}
    for stage_list in ag_plan:
        for g, kind in stage_list:
            for d in range(2):
                for s in range(SUBS):
                    ag_slots[d, g, kind, s] = len(ag_slots)

    def page(d, g, s):
        return (d * far + g) * SUBS + s

    def rs_message(d, g, kind, s):
        i = slots[d, g, kind, s]
        at = span(d, kind)
        return pltpu.make_async_remote_copy(
            rs_out.at[page(d, g, s), :, at], rs_in.at[page(d, g, s), :, at], rs_send.at[i], rs_recv.at[i],
            device_id={"tp": target[d]}, device_id_type=MESH)

    def piece(j, c, s):
        return share[place[j % nz] * rows + s * sub:place[j % nz] * rows + (s + 1) * sub, c * half:(c + 1) * half]

    arrived = set()

    def received(d, g, c, s):
        for kind in ("L", "S", "F"):
            if (d, g, kind, s) in slots and c in halves(d, kind) and (d, g, kind, s) not in arrived:
                rs_message(d, g, kind, s).wait_recv()
                arrived.add((d, g, kind, s))
        return rs_in[page(d, g, s), :, c * half:(c + 1) * half].astype(jnp.float32)

    def rs_step(d, g, kind, s):
        j = far - g if d == 0 else g - far
        for c in halves(d, kind):
            value = piece(j, c, s)
            if g > (0 if c == d else 1):
                value = value + received(d, g - 1, c, s)
            rs_out[page(d, g, s), :, c * half:(c + 1) * half] = value.astype(jnp.bfloat16)
        rs_message(d, g, kind, s).start()

    def ag_message(d, g, kind, s, behind):
        here = out_ref.at[pl.ds(out_row(-behind if d == 0 else behind, s), sub), span(d, kind)]
        i = ag_slots[d, g, kind, s]
        return pltpu.make_async_remote_copy(
            here, here, ag_send.at[i], ag_recv.at[i], device_id={"tp": target[d]}, device_id_type=MESH)

    d2d = []

    def d2d_start(j, at, s):
        here = out_ref.at[pl.ds(out_row(j, s), sub), at]
        i = len(d2d)
        copy = pltpu.make_async_remote_copy(here, here, d2d_send.at[i], d2d_recv.at[i], device_id={"tp": mate}, device_id_type=MESH)
        copy.start()
        d2d.append((j, at, s))

    def finish(s):
        total = []
        for c in range(2):
            acc = piece(0, c, s)
            for d in range(2):
                acc = acc + received(d, far - 1, c, s)
            share[place[0] * rows + s * sub:place[0] * rows + (s + 1) * sub, c * half:(c + 1) * half] = acc
            total.append(jnp.sum(acc * acc, axis=-1, keepdims=True))
        inv = lax.rsqrt((total[0] + total[1]) / width + NORM_EPS)
        for c in range(2):
            at = slice(c * half, (c + 1) * half)
            normed = piece(0, c, s) * inv * gain_ref[:, at]
            out_ref[pl.ds(out_row(0, s), sub), at] = (hid[s * sub:(s + 1) * sub, at].astype(jnp.float32) + normed).astype(jnp.bfloat16)
        for g, kind in ag_plan[0]:
            for d in range(2):
                ag_message(d, g, kind, s, 0).start()
        d2d_start(0, pl.ds(0, width), s)

    def ag_step(t, s):
        for g, kind in ag_plan[t - 1]:
            for d in range(2):
                ag_message(d, g, kind, s, g + 1).wait_recv()
                if t < len(ag_plan):
                    for g_next, kind_next in ag_plan[t]:
                        if set(halves(d, kind_next)) <= set(halves(d, kind)):
                            ag_message(d, g_next, kind_next, s, g + 1).start()
                d2d_start(-(g + 1) if d == 0 else g + 1, span(d, kind), s)

    def stage(t, s):
        if t < far:
            for g, kind in rs_plan[t]:
                for d in range(2):
                    rs_step(d, g, kind, s)
        elif t == far:
            if s == 0:
                hid_copy.wait()
            finish(s)
        else:
            ag_step(t - far, s)

    add_shares(0, 3, lhs_in, w_in, False)
    last_stage = far + len(ag_plan)
    for slot in range(last_stage + 1 + LAG * (SUBS - 1)):
        if slot == 1:
            gather(3, nz, o_in, 0, lhs_in)
            add_shares(3, nz, lhs, w_ref, True)
            add_shares(3, nz, lhs_in, w_in, False)
        for s in range(SUBS):
            t = slot - LAG * s
            if 0 <= t <= last_stage:
                stage(t, s)

    o_copy.wait_send()
    for d, g, kind, s in slots:
        rs_message(d, g, kind, s).wait_send()
    for d, g, kind, s in ag_slots:
        ag_message(d, g, kind, s, g).wait_send()
    for i, (j, at, s) in enumerate(d2d):
        here = out_ref.at[pl.ds(out_row(j, s), sub), at]
        there = out_ref.at[pl.ds(pl.multiple_of((1 - k) * half_rows + chunk_of(j) * rows + s * sub, sub), sub), at]
        copy = pltpu.make_async_remote_copy(here, there, d2d_send.at[i], d2d_recv.at[i], device_id={"tp": mate}, device_id_type=MESH)
        copy.wait_send()
        copy.wait_recv()


def finish_call(n_tp, attn, w_own, w_mate, hidden, gain):
    n_rows, width = hidden.shape
    depth = w_own.shape[0]
    nz = n_tp // 2
    half_rows, rows = n_rows // 2, n_rows // n_tp
    sub = rows // SUBS
    n_msg = 2 * SUBS * (nz - 1)
    vmem = pl.BlockSpec(memory_space=pltpu.VMEM)
    return pl.pallas_call(
        functools.partial(finish_kernel, n_tp),
        name="finish",
        out_shape=pltpu.VMEM((n_rows, width), jnp.bfloat16) if OUT_VMEM else jax.ShapeDtypeStruct((n_rows, width), jnp.bfloat16),
        in_specs=[vmem, vmem, vmem, pl.BlockSpec(memory_space=pltpu.HBM), vmem],
        out_specs=vmem,
        scratch_shapes=[
            pltpu.VMEM((half_rows, depth), jnp.bfloat16),
            pltpu.VMEM((half_rows, depth), jnp.bfloat16),
            pltpu.VMEM((half_rows, depth), jnp.bfloat16),
            pltpu.VMEM((rows, width), jnp.bfloat16),
            pltpu.VMEM((half_rows, width), jnp.float32),
            pltpu.VMEM((nz * SUBS, sub, width), jnp.bfloat16),
            pltpu.VMEM((nz * SUBS, sub, width), jnp.bfloat16),
            pltpu.SemaphoreType.DMA,
            pltpu.SemaphoreType.DMA,
            pltpu.SemaphoreType.DMA,
            pltpu.SemaphoreType.DMA((n_msg,)),
            pltpu.SemaphoreType.DMA((n_msg,)),
            pltpu.SemaphoreType.DMA((n_msg,)),
            pltpu.SemaphoreType.DMA((n_msg,)),
            pltpu.SemaphoreType.DMA((2 * SUBS * nz,)),
            pltpu.SemaphoreType.DMA((2 * SUBS * nz,)),
        ],
        compiler_params=pltpu.CompilerParams(collective_id=0, has_side_effects=True, vmem_limit_bytes=40 * 2**20),
    )(attn, w_own, w_mate, pltpu.with_memory_space_constraint(hidden, pltpu.HBM), gain)


def solution(mesh):
    def local_step(hidden, w_q, w_k, w_v, w_o, q_norm_w, k_norm_w, post_norm_w, k_cache, v_cache, positions):
        n_tp = mesh.shape["tp"]
        q_rot, k_rot, posb, w_own, w_mate, k_near, v_near = project_call(
            n_tp, hidden, w_q, w_k, w_v, w_o, q_norm_w[None, :], k_norm_w[None, :], positions, k_cache, v_cache)
        attn, k_new, v_new = attend_call(q_rot, k_rot, posb, k_near, v_near, k_cache.shape)
        hidden_out = finish_call(n_tp, attn, w_own, w_mate, hidden, post_norm_w[None, :])
        return hidden_out, k_new, v_new

    cache_spec = P('dp', None, 'tp', None)
    return jax.shard_map(local_step, mesh=mesh, in_specs=(P('dp', None), P(None, 'tp'), P(None, 'tp'), P(None, 'tp'), P('tp', None), P('tp'), P('tp'), P(None), cache_spec, cache_spec, P('dp')), out_specs=(P('dp', None), cache_spec, cache_spec), check_vma=False)
```
